32 devices in a mesh: cells: 16 (over z, y, core), genes: 2 (over x).
Axes of the slice: x: 2, y: 2, z: 4, core: 2. Of those that a mesh axis runs over, the one named last changes fastest.
Arguments:
- counts: int32 [2048, 33280], P('cells', 'genes'), may hold values from 0 to 64, as said below
- live_rows: int32 [16], P('cells'), may hold values from 64 to 128, as said below
- left_basis: float32 [32, 2048], P(None, 'cells'), may hold values from -0.125 to 0.125
- right_basis: float32 [32, 33280], P(None, 'genes'), may hold values from -0.03125 to 0.03125
- right_start: float32 [16, 33280], P(None, 'genes'), may hold values from -0.03125 to 0.03125
Outputs:
- left_vectors: float32 [48, 2048], P(None, 'cells')
- right_vectors: float32 [48, 33280], P(None, 'genes')
- diag_blocks: float32 [3, 16, 16], replicated
- couple_blocks: float32 [3, 16, 16], replicated
The draws below stay inside these ranges and needn't reach their ends.
Inputs may be any that keep to these rules, and one draw needn't show every extreme that they name: `counts`: rows of a cell block at or beyond its live count are padding and are not part of the matrix. `live_rows`: entry b is the number of live rows, the first ones, of cell block b; some block is full in every draw.
All inputs are finite; a program needn't handle non-finite values.
Results may differ from the reference program's by a relative error of at most 0.0003.
Values sent between devices are 32-bit elements; how exact they have to be, the bound alone decides.
A program may use at most 64 MiB of HBM per device.

```python
import jax
import jax.numpy as jnp
from jax import lax

CELL_DEV = 128
GENES = 33280
BASIS = 32
BLOCK = 16
STEPS = 3
CELL_BLOCKS = 16
CELLS = 2048


def draw_counts(key, part):
    first = jax.random.fold_in(key, 11)
    second = jax.random.fold_in(key, 12)
    third = jax.random.fold_in(key, 13)
    powers = jax.random.randint(first, (1, GENES), 0, 7)
    ceiling = jnp.left_shift(jnp.ones((1, GENES), jnp.int32), powers)
    values = jax.random.randint(second, (CELLS, GENES), 0, ceiling + 1)
    present = jax.random.randint(third, (CELLS, GENES), 0, 5) < 2
    return jnp.where(present, values, 0).astype(jnp.int32)


def draw_live_rows(key, part):
    first = jax.random.fold_in(key, 21)
    second = jax.random.fold_in(key, 22)
    lengths = jax.random.randint(first, (CELL_BLOCKS,), CELL_DEV // 2, CELL_DEV + 1)
    chosen = jax.random.randint(second, (), 0, CELL_BLOCKS)
    places = jnp.arange(CELL_BLOCKS, dtype=jnp.int32)
    return jnp.where(places == chosen, CELL_DEV, lengths).astype(jnp.int32)


def shard_levels(rng, shape, pieces, least, largest):
    def one(axis_at, parts):
        draws = jax.random.uniform(jax.random.fold_in(jax.random.fold_in(rng, 6), axis_at), (parts,), jnp.float32, least / len(pieces), largest / len(pieces))
        return jnp.repeat(jnp.exp(draws), shape[axis_at] // parts).reshape((-1,) + (1,) * (len(shape) - axis_at - 1))

    loudness = one(*pieces[0])
    for cut in pieces[1:]:
        loudness = loudness * one(*cut)
    return loudness


def centred(rng, shape, scale, reach, shards=(), kind=jnp.bfloat16):
    loudness = shard_levels(rng, shape, shards, -0.22, 0.18) if shards else 1.0
    drawn = jax.random.normal(rng, shape, jnp.float32) * scale * loudness
    return jnp.minimum(jnp.maximum(drawn, -reach), reach).astype(kind)


def setup_inputs(seed: int = 0) -> dict:
    keys = jax.random.split(jax.random.key(seed), 6)
    counts = draw_counts(jax.random.fold_in(keys[5], 71), 0)
    live_rows = draw_live_rows(jax.random.fold_in(keys[5], 71), 0)
    left_basis = centred(keys[2], (BASIS, CELLS), CELLS ** -0.5, 0.125, ((1, 16),), jnp.float32)
    right_basis = centred(keys[3], (BASIS, GENES), GENES ** -0.5, 0.03125, ((1, 2),), jnp.float32)
    right_start = centred(keys[4], (BLOCK, GENES), GENES ** -0.5, 0.03125, ((1, 2),), jnp.float32)
    return {"counts": counts, "live_rows": live_rows, "left_basis": left_basis, "right_basis": right_basis, "right_start": right_start}


HIGHEST = lax.Precision.HIGHEST

def matmul(lhs, rhs):
    return jnp.dot(lhs.astype(jnp.float32), rhs.astype(jnp.float32), precision=HIGHEST, preferred_element_type=jnp.float32)

def outer_rows(lhs, rhs):
    return lax.dot_general(lhs.astype(jnp.float32), rhs.astype(jnp.float32), (((1,), (1,)), ((), ())), precision=HIGHEST, preferred_element_type=jnp.float32)

def orthonormal_block(vectors, spanning):
    coeffs = outer_rows(vectors, spanning)
    cleaned = vectors - matmul(coeffs, spanning)
    coeffs = outer_rows(cleaned, spanning)
    cleaned = cleaned - matmul(coeffs, spanning)
    squares = outer_rows(cleaned, cleaned)
    factor = jnp.linalg.cholesky(squares)
    result = lax.linalg.triangular_solve(factor, cleaned, left_side=True, lower=True)
    return (result, factor)

def reference(counts, live_rows, left_basis, right_basis, right_start):
    within = jnp.arange(CELL_DEV, dtype=jnp.int32)[None, :] < live_rows[:, None]
    weights = within.reshape(CELLS).astype(jnp.float32)
    logged = jnp.where(weights[:, None] > 0, jnp.log1p(counts.astype(jnp.float32)), 0.0)
    live_total = jnp.sum(live_rows).astype(jnp.float32)
    column_mean = lax.optimization_barrier(jnp.sum(logged, axis=0)) / live_total
    factor_scale = lax.rsqrt(live_total)
    slots_left = jnp.concatenate([left_basis * weights[None, :], jnp.zeros((STEPS * BLOCK, CELLS), jnp.float32)], axis=0)
    slots_right = jnp.concatenate([right_basis, right_start, jnp.zeros(((STEPS - 1) * BLOCK, GENES), jnp.float32)], axis=0)
    current = right_start
    left_blocks, right_blocks, diag_list, couple_list = ([], [], [], [])
    for iteration in range(STEPS):
        projected = (outer_rows(current, logged) - matmul(current, column_mean)[:, None] * weights[None, :]) * factor_scale
        leftvec, diag_factor = orthonormal_block(projected, slots_left)
        position = BASIS + iteration * BLOCK
        slots_left = slots_left.at[position:position + BLOCK].set(leftvec)
        projected = (matmul(leftvec, logged) - lax.optimization_barrier(jnp.sum(leftvec, axis=1))[:, None] * column_mean[None, :]) * factor_scale
        current, side_factor = orthonormal_block(projected, slots_right)
        if iteration + 1 < STEPS:
            slots_right = slots_right.at[position + BLOCK:position + 2 * BLOCK].set(current)
        left_blocks.append(leftvec)
        right_blocks.append(current)
        diag_list.append(diag_factor)
        couple_list.append(side_factor)
    left_vectors = jnp.concatenate(left_blocks, axis=0) * jnp.sqrt(jnp.float32(CELLS))
    right_vectors = jnp.concatenate(right_blocks, axis=0) * jnp.sqrt(jnp.float32(GENES))
    return (left_vectors, right_vectors, jnp.stack(diag_list), jnp.stack(couple_list))
```

```python
import functools
import math

import jax
import jax.numpy as jnp
from jax import lax
from jax.experimental import pallas as pl
from jax.experimental.pallas import tpu as pltpu
from jax.sharding import PartitionSpec as P

BASIS = 32
BLOCK = 16
STEPS = 3
SLOTS = BASIS + STEPS * BLOCK
WEIGHT = SLOTS + BLOCK
LANES = 128
F32 = jnp.float32
BF16 = jnp.bfloat16
HIGHEST = lax.Precision.HIGHEST
MESH = pl.DeviceIdType.MESH


def exact(lhs, rhs):
    return jnp.dot(lhs, rhs, precision=HIGHEST, preferred_element_type=F32)


def exact_rows(lhs, rhs):
    return lax.dot_general(
        lhs, rhs, (((1,), (1,)), ((), ())), precision=HIGHEST, preferred_element_type=F32
    )


def split(values):
    high = values.astype(BF16)
    return high, (values - high.astype(F32)).astype(BF16)


def product(high, both, rhs_high, rhs_low, dims):
    rows = high.shape[0]
    first = lax.dot_general(both, rhs_high, (dims, ((), ())), preferred_element_type=F32)
    second = lax.dot_general(high, rhs_low, (dims, ((), ())), preferred_element_type=F32)
    return first[:rows] + (first[rows:] + second)


ALONG = ((1,), (0,))
ROWS = ((1,), (1,))


def loop(start, stop, step):
    def one(k, carry):
        step(k)
        return carry

    lax.fori_loop(start, stop, one, 0)


def orthonormal(gram, near, lower, spanning, vectors):
    lane = lax.broadcasted_iota(jnp.int32, (BLOCK, LANES), 1)
    row = lax.broadcasted_iota(jnp.int32, (BLOCK, LANES), 0)
    coeffs = jnp.where(lane < SLOTS, gram, 0.0)
    squares = gram[:, SLOTS : SLOTS + BLOCK]
    combined = coeffs + coeffs - (exact(coeffs, near) + exact_rows(coeffs, lower))
    residue = coeffs - (exact(combined, near) + exact_rows(combined, lower))
    squares = squares - exact_rows(combined, coeffs) - exact_rows(residue, combined)
    cleaned = vectors - exact(combined, spanning)
    change = jnp.where(lane == row + SLOTS, 1.0, -combined)
    parts = [squares, cleaned, residue, change]
    for k in range(BLOCK):
        pivot = parts[0][k : k + 1, k : k + 1]
        root = lax.rsqrt(pivot)
        root = root * (1.5 - 0.5 * pivot * root * root)
        column = parts[0][:, k : k + 1] * root
        after = []
        for part in parts:
            scaled = part[k : k + 1, :] * root
            places = lax.broadcasted_iota(jnp.int32, part.shape, 0)
            after.append(
                jnp.where(places > k, part - column * scaled, jnp.where(places == k, scaled, part))
            )
        parts = after
    spot = lax.broadcasted_iota(jnp.int32, (BLOCK, BLOCK), 0)
    other = lax.broadcasted_iota(jnp.int32, (BLOCK, BLOCK), 1)
    upper = jnp.where(other >= spot, parts[0], 0.0)
    factor = exact_rows(jnp.where(other == spot, 1.0, 0.0).astype(F32), upper)
    return parts[1], factor, parts[2], parts[3]


def kernel(
    n, g, width, scales,
    live, counts, left_basis, right_basis, right_start,
    left_out, right_out, diag_out, couple_out,
    cnt, logged, bhi, blo, rb, sl, mr, el, tl, er, tr,
    w, ra, rt, rz, pb, mu, wsum, chg, gram0, gram, xg0, xg,
    in_sem, as_sem, ar_sem, bs_sem, br_sem, cs_sem, cr_sem, ds_sem, fs_sem, zs_sem, zr_sem,
    ms_sem, mr_sem, g0s_sem, g0r_sem, gs_sem, gr_sem, x0s_sem, x0r_sem, xs_sem, xr_sem,
):
    cells, genes = counts.shape
    me = lax.axis_index("cells")
    mine = lax.axis_index("genes")
    core = lax.rem(me, 2)
    chip = me // 2
    h = n // 2
    b = 1 << ((h.bit_length() - 1) // 2)
    b = b if h % b == 0 else 1
    a = h // b
    zi, yi = chip // b, lax.rem(chip, b)
    sibling = me + 1 - 2 * core

    def along_cells(src, dst, send, recv, peer):
        return pltpu.make_async_remote_copy(
            src_ref=src, dst_ref=dst, send_sem=send, recv_sem=recv,
            device_id=(peer, mine), device_id_type=MESH,
        )

    def along_genes(src, dst, send, recv, peer):
        return pltpu.make_async_remote_copy(
            src_ref=src, dst_ref=dst, send_sem=send, recv_sem=recv,
            device_id=(me, peer), device_id_type=MESH,
        )

    loads = []
    for d in range(n):
        cols = max(0, min(width, genes - d * width))
        if cols:
            here = pl.ds(d * width, cols)
            loads.append((d, [
                pltpu.make_async_copy(counts.at[:, here], cnt.at[d, :, pl.ds(0, cols)], in_sem.at[d, 0]),
                pltpu.make_async_copy(right_basis.at[:, here], rb.at[d, pl.ds(0, BASIS), pl.ds(0, cols)], in_sem.at[d, 1]),
                pltpu.make_async_copy(right_start.at[:, here], rb.at[d, pl.ds(BASIS, BLOCK), pl.ds(0, cols)], in_sem.at[d, 2]),
            ]))
        if cols < width:
            cnt[d, :, cols:] = jnp.zeros((cells, width - cols), jnp.int32)
            rb[d, :, cols:] = jnp.zeros((BASIS + BLOCK, width - cols), F32)
    for _, trio in loads:
        trio[0].start()
    for _, trio in loads:
        trio[1].start()
        trio[2].start()

    barrier = pltpu.get_barrier_semaphore()

    def greet_cells(k):
        pl.semaphore_signal(barrier, inc=1, device_id=(lax.rem(me + k, n), mine), device_id_type=MESH)

    def greet_genes(k):
        pl.semaphore_signal(barrier, inc=1, device_id=(me, lax.rem(mine + k, g)), device_id_type=MESH)

    loop(1, n, greet_cells)
    loop(1, g, greet_genes)

    def spread(copy, buf, at, size, send, recv):
        def go(k):
            copy(buf.at[at], buf.at[at], send.at[k], recv.at[at], lax.rem(at + k, size)).start()

        loop(1, size, go)

    def waited(copy, buf, at, size, send, recv):
        def end(k):
            source = lax.rem(at + size - k, size)
            item = copy(buf.at[source], buf.at[source], send.at[k], recv.at[source], lax.rem(at + k, size))
            item.wait_send()
            item.wait_recv()

        loop(1, size, end)

    def gathered(copy, buf, at, size, send, recv):
        waited(copy, buf, at, size, send, recv)
        return lax.fori_loop(
            1, size, lambda k, total: total + buf[k], buf[0]
        )

    def order(k):
        return lax.rem(zi + 1 + lax.rem(k, a), a), lax.rem(yi + 1 + k // a, b)

    def reduce_scatter(produce, part, fromcore, fromy, fromz, result):
        def first(k):
            z, y = order(k)
            t = z * b + y
            d = 2 * t + 1 - core
            produce(d)
            along_cells(part.at[d], fromcore.at[t], as_sem.at[t], ar_sem.at[t], sibling).start()

        loop(0, h, first)

        def join(t):
            d = 2 * t + core
            produce(d)
            along_cells(part.at[d], fromcore.at[t], as_sem.at[t], ar_sem.at[t], sibling).wait_recv()
            part[d] = part[d] + fromcore[t]
            return d

        def second(k):
            z, y = order(k)
            t = z * b + y
            d = join(t)
            to = z * b + yi
            along_cells(part.at[d], fromy.at[to], bs_sem.at[t], br_sem.at[to], 2 * (zi * b + y) + core).start()

        loop(0, h - a, second)

        def complete(z):
            d = join(z * b + yi)

            def add(k):
                source = z * b + lax.rem(yi + k, b)
                along_cells(part.at[d], fromy.at[source], bs_sem.at[source], br_sem.at[source], sibling).wait_recv()
                part[d] = part[d] + fromy[source]

            loop(1, b, add)
            return d

        def third(k):
            z = lax.rem(zi + k, a)
            d = complete(z)
            along_cells(part.at[d], fromz.at[zi], zs_sem.at[z], zr_sem.at[zi], d).start()

        loop(1, a, third)
        complete(zi)
        result[me] = part[me]

        def fourth(k):
            z = lax.rem(zi + a - k, a)
            along_cells(part.at[me], fromz.at[z], zs_sem.at[z], zr_sem.at[z], sibling).wait_recv()
            result[me] = result[me] + fromz[z]

        loop(1, a, fourth)

    def all_gather(part, fromcore, fromy, fromz, result, consume):
        def relay(z):
            t = z * b + yi
            d = 2 * t + core

            def to_y(k):
                y = lax.rem(yi + k, b)
                along_cells(result.at[d], result.at[d], fs_sem.at[z * b + y], cr_sem.at[d], 2 * (zi * b + y) + core).start()

            loop(1, b, to_y)
            along_cells(result.at[d], result.at[d], ds_sem.at[t], cr_sem.at[d], sibling).start()

        def arrived(d):
            along_cells(result.at[d], result.at[d], ds_sem.at[0], cr_sem.at[d], sibling).wait_recv()

        def go(k):
            z = lax.rem(zi + k, a)
            along_cells(result.at[me], result.at[me], cs_sem.at[z], cr_sem.at[me], 2 * (z * b + yi) + core).start()

        loop(1, a, go)
        relay(zi)
        consume(me)

        def pass_z(k):
            z = lax.rem(zi + a - k, a)
            d = 2 * (z * b + yi) + core
            arrived(d)
            relay(z)

        loop(1, a, pass_z)
        loop(1, a, lambda k: consume(2 * (lax.rem(zi + a - k, a) * b + yi) + core))

        def pass_y(k):
            z = lax.rem(zi + a - lax.rem(k, a), a)
            t = z * b + lax.rem(yi + 1 + k // a, b)
            d = 2 * t + core
            arrived(d)
            along_cells(result.at[d], result.at[d], ds_sem.at[t], cr_sem.at[d], sibling).start()
            consume(d)

        loop(0, h - a, pass_y)

        def rest(k):
            z = lax.rem(zi + a - lax.rem(k, a), a)
            t = z * b + lax.rem(yi + k // a, b)
            d = 2 * t + 1 - core
            arrived(d)
            consume(d)

        loop(0, h, rest)

        def ended(t):
            along_cells(part.at[t], fromcore.at[t], as_sem.at[t], ar_sem.at[t], sibling).wait_send()
            along_cells(result.at[t], result.at[t], ds_sem.at[t], cr_sem.at[t], sibling).wait_send()

        loop(0, h, ended)

        def ended_y(k):
            z, y = order(k)
            t = z * b + y
            along_cells(part.at[t], fromy.at[t], bs_sem.at[t], br_sem.at[t], sibling).wait_send()
            along_cells(result.at[t], result.at[t], fs_sem.at[t], cr_sem.at[t], sibling).wait_send()

        loop(0, h - a, ended_y)

        def ended_z(k):
            z = lax.rem(zi + k, a)
            along_cells(part.at[z], fromz.at[z], zs_sem.at[z], zr_sem.at[z], sibling).wait_send()
            along_cells(result.at[z], result.at[z], cs_sem.at[z], cr_sem.at[z], sibling).wait_send()

        loop(1, a, ended_z)

    live_here = live[0]
    weights_row = jnp.where(
        lax.broadcasted_iota(jnp.int32, (1, cells), 1) < live_here, 1.0, 0.0
    ).astype(F32)
    weights = jnp.where(
        lax.broadcasted_iota(jnp.int32, (cells, LANES), 0) < live_here, 1.0, 0.0
    ).astype(F32)
    for table in (sl, mr, tl, tr):
        table[...] = jnp.zeros_like(table)
    same = jnp.where(
        lax.broadcasted_iota(jnp.int32, (LANES, LANES), 0)
        == lax.broadcasted_iota(jnp.int32, (LANES, LANES), 1),
        1.0, 0.0,
    ).astype(F32)
    el[...] = same
    er[...] = same
    sl[0:BASIS] = left_basis[...] * weights_row
    sl[WEIGHT : WEIGHT + 8] = jnp.where(
        lax.broadcasted_iota(jnp.int32, (8, cells), 0) == 0, weights_row, 0.0
    )
    tiles = width // LANES

    def take_log(d):
        for i in range(tiles):
            here = slice(i * LANES, (i + 1) * LANES)
            logged[d, :, here] = jnp.log(1.0 + cnt[d, :, here].astype(F32)) * weights

    for _, trio in loads:
        trio[0].wait()
    take_log(me)
    portion = 1.0 / jnp.maximum(live_here, 1).astype(F32)
    for i in range(tiles):
        here = slice(i * LANES, (i + 1) * LANES)
        mu[me, :, here] = jnp.sum(logged[me, :, here], axis=0, keepdims=True) * portion
    gram0[me, 0:BASIS] = exact_rows(sl[0:BASIS], sl[...])
    gram0[me, BASIS:] = exact_rows(sl[WEIGHT : WEIGHT + 8], sl[...])
    pl.semaphore_wait(barrier, n - 1 + g - 1)
    spread(along_cells, mu, me, n, ms_sem, mr_sem)
    spread(along_cells, gram0, me, n, g0s_sem, g0r_sem)
    loop(1, n, lambda k: take_log(lax.rem(me + k, n)))

    for _, trio in loads:
        trio[1].wait()
        trio[2].wait()
    xg0[mine] = jnp.zeros((BASIS + BLOCK, 2 * LANES), F32)

    def fill(d):
        high, low = split(rb[d])
        bhi[d, cells : cells + BASIS + BLOCK] = high
        blo[d, cells : cells + BASIS + BLOCK] = low
        blank = jnp.zeros((LANES - BASIS - BLOCK, width), BF16)
        bhi[d, cells + BASIS + BLOCK :] = blank
        blo[d, cells + BASIS + BLOCK :] = blank
        both = jnp.concatenate([high, low], axis=0)
        xg0[mine, :, cells:] = xg0[mine, :, cells:] + product(high, both, bhi[d, cells:], blo[d, cells:], ROWS)

    loop(0, n, fill)
    waited(along_cells, mu, me, n, ms_sem, mr_sem)

    def center(d):
        for i in range(tiles):
            here = slice(i * LANES, (i + 1) * LANES)
            high, low = split(logged[d, :, here] - weights * mu[d, :, here])
            bhi[d, 0:cells, here] = high
            blo[d, 0:cells, here] = low
        high = bhi[d, cells : cells + BASIS + BLOCK]
        both = jnp.concatenate([high, blo[d, cells : cells + BASIS + BLOCK]], axis=0)
        xg0[mine, :, :cells] = xg0[mine, :, :cells] + product(high, both, bhi[d, 0:cells], blo[d, 0:cells], ROWS)

    loop(0, n, center)
    spread(along_genes, xg0, mine, g, x0s_sem, x0r_sem)
    near = gathered(along_cells, gram0, me, n, g0s_sem, g0r_sem)
    corner = lax.broadcasted_iota(jnp.int32, (LANES, LANES), 0)
    across = lax.broadcasted_iota(jnp.int32, (BASIS, LANES), 1)
    el[...] = jnp.where((same > 0) & (corner >= BASIS), 1.0, 0.0)
    el[0:BASIS] = jnp.where(across < SLOTS, near[0:BASIS], 0.0)
    wsum[...] = near[BASIS:]
    live_total = near[BASIS : BASIS + 1, WEIGHT : WEIGHT + 1]
    inverse = 1.0 / live_total
    factor_scale = lax.rsqrt(live_total)
    factor_scale = factor_scale * (1.5 - 0.5 * live_total * factor_scale * factor_scale)
    cross = gathered(along_genes, xg0, mine, g, x0s_sem, x0r_sem)
    mr[0 : BASIS + BLOCK] = cross[:, :cells]
    er[0 : BASIS + BLOCK] = cross[:, cells:]
    whole = genes // width
    lane = lax.broadcasted_iota(jnp.int32, (BLOCK, LANES), 1)
    row = lax.broadcasted_iota(jnp.int32, (BLOCK, LANES), 0)

    def turned(column, start):
        return jnp.sum(jnp.where(lane == row + start, column, 0.0), axis=0, keepdims=True)

    def update(j):
        later = cells + BASIS + (j + 1) * BLOCK
        later = later if isinstance(j, int) else pl.multiple_of(later, BLOCK)
        chigh, clow = split(chg[...])
        cboth = jnp.concatenate([chigh, clow], axis=0)

        def right(d):
            fresh = product(chigh, cboth, bhi[d, cells:], blo[d, cells:], ALONG)
            vhigh, vlow = split(fresh)
            bhi[d, pl.ds(later, BLOCK)] = vhigh
            blo[d, pl.ds(later, BLOCK)] = vlow
            return fresh * scales[1]

        rows = pl.ds(j * BLOCK if isinstance(j, int) else pl.multiple_of(j * BLOCK, BLOCK), BLOCK)

        def emit(d):
            right_out[rows, pl.ds(pl.multiple_of(d * width, LANES), width)] = right(d)

        loop(0, whole, emit)
        if genes % width:
            right_out[rows, whole * width : genes] = right(whole)[:, : genes % width]

    def step(j):
        position = pl.multiple_of(BASIS + j * BLOCK, BLOCK)
        vectors = mr[pl.ds(position, BLOCK)]
        sl[SLOTS : SLOTS + BLOCK] = vectors
        gram[me] = exact_rows(vectors, sl[...])
        spread(along_cells, gram, me, n, gs_sem, gr_sem)
        pl.when(j > 0)(lambda: update(j - 1))
        total = gathered(along_cells, gram, me, n, gs_sem, gr_sem)
        held = total[:, WEIGHT : WEIGHT + 1] * inverse
        weighed = wsum[0:1] + turned(total[:, WEIGHT : WEIGHT + 1], SLOTS)
        scale = jnp.where(lane < SLOTS, factor_scale, factor_scale * factor_scale)
        leftvec, factor, against, change = orthonormal(
            (total - held * weighed) * scale, el[...], tl[...], sl[...],
            (vectors - held * weights_row) * factor_scale,
        )
        diag_out[j] = factor
        tilt = jnp.sum(jnp.where(lane < SLOTS, change * wsum[0:1], 0.0), axis=1, keepdims=True)
        wsum[0:1] = wsum[0:1] + turned(tilt, position)
        sl[pl.ds(position, BLOCK)] = leftvec
        el[pl.ds(position, BLOCK)] = el[pl.ds(position, BLOCK)] + against
        tl[pl.ds(position, BLOCK)] = against
        left_out[pl.ds(position - BASIS, BLOCK)] = leftvec * scales[0]
        high, low = split((leftvec - tilt * inverse * weights_row) * factor_scale)
        both = jnp.concatenate([high, low], axis=0)

        def produce(d):
            w[d] = product(high, both, bhi[d, 0:cells], blo[d, 0:cells], ALONG)

        reduce_scatter(produce, w, ra, rt, rz, pb)
        xg[j, mine] = jnp.zeros((BLOCK, 2 * LANES), F32)

        def consume(d):
            phigh, plow = split(pb[d])
            bhi[d, cells + SLOTS : cells + SLOTS + BLOCK] = phigh
            blo[d, cells + SLOTS : cells + SLOTS + BLOCK] = plow
            pboth = jnp.concatenate([phigh, plow], axis=0)
            xg[j, mine] = xg[j, mine] + product(phigh, pboth, bhi[d], blo[d], ROWS)

        all_gather(w, ra, rt, rz, pb, consume)
        box = xg.at[j]
        spread(along_genes, box, mine, g, xs_sem.at[j], xr_sem.at[j])
        total = gathered(along_genes, box, mine, g, xs_sem.at[j], xr_sem.at[j])
        projected, factor, against, change = orthonormal(
            total[:, cells:], er[...], tr[...], mr[...], total[:, :cells]
        )
        couple_out[j] = factor
        later = pl.multiple_of(position + BLOCK, BLOCK)
        mr[pl.ds(later, BLOCK)] = projected
        er[pl.ds(later, BLOCK)] = er[pl.ds(later, BLOCK)] + against
        tr[pl.ds(later, BLOCK)] = against
        chg[...] = change

    loop(0, STEPS, step)
    update(STEPS - 1)


def body(counts, live_rows, left_basis, right_basis, right_start):
    cells, genes = counts.shape
    n = lax.axis_size("cells")
    g = lax.axis_size("genes")
    h = n // 2
    width = -(-(genes // LANES) // n) * LANES
    scales = (math.sqrt(float(cells * n)), math.sqrt(float(genes * g)))
    vmem = pl.BlockSpec(memory_space=pltpu.VMEM)
    anywhere = pl.BlockSpec(memory_space=pl.ANY)
    square = pltpu.VMEM((LANES, LANES), F32)
    dma = lambda *shape: pltpu.SemaphoreType.DMA(shape)
    out_shape = (
        jax.ShapeDtypeStruct((STEPS * BLOCK, cells), F32),
        jax.ShapeDtypeStruct((STEPS * BLOCK, genes), F32),
        jax.ShapeDtypeStruct((STEPS, BLOCK, BLOCK), F32),
        jax.ShapeDtypeStruct((STEPS, BLOCK, BLOCK), F32),
    )
    buffers = lambda rows: [
        pltpu.VMEM((n, rows, width), F32),
        pltpu.VMEM((h, rows, width), F32),
        pltpu.VMEM((h, rows, width), F32),
        pltpu.VMEM((h, rows, width), F32),
        pltpu.VMEM((n, rows, width), F32),
    ]
    scratch = [
        pltpu.VMEM((n, cells, width), jnp.int32),
        pltpu.VMEM((n, cells, width), F32),
        pltpu.VMEM((n, cells + LANES, width), BF16),
        pltpu.VMEM((n, cells + LANES, width), BF16),
        pltpu.VMEM((n, BASIS + BLOCK, width), F32),
        square, square, square, square, square, square,
        *buffers(BLOCK),
        pltpu.VMEM((n, 1, width), F32),
        pltpu.VMEM((8, LANES), F32),
        pltpu.VMEM((BLOCK, LANES), F32),
        pltpu.VMEM((n, BASIS + 8, LANES), F32),
        pltpu.VMEM((n, BLOCK, LANES), F32),
        pltpu.VMEM((g, BASIS + BLOCK, 2 * LANES), F32),
        pltpu.VMEM((STEPS, g, BLOCK, 2 * LANES), F32),
        dma(n, 3),
        dma(h), dma(h), dma(h), dma(h), dma(h), dma(n), dma(h), dma(h), dma(h), dma(h),
        dma(n), dma(n), dma(n), dma(n), dma(n), dma(n),
        dma(g), dma(g), dma(STEPS, g), dma(STEPS, g),
    ]
    return pl.pallas_call(
        functools.partial(kernel, n, g, width, scales),
        out_shape=out_shape,
        in_specs=[pl.BlockSpec(memory_space=pltpu.SMEM), anywhere, vmem, anywhere, anywhere],
        out_specs=(vmem, vmem, vmem, vmem),
        scratch_shapes=scratch,
        compiler_params=pltpu.CompilerParams(
            collective_id=0, has_side_effects=True, vmem_limit_bytes=66 * 1000 * 1000
        ),
    )(live_rows, counts, left_basis, right_basis, right_start)


def solution(mesh):
    in_specs = (
        P("cells", "genes"),
        P("cells"),
        P(None, "cells"),
        P(None, "genes"),
        P(None, "genes"),
    )
    out_specs = (P(None, "cells"), P(None, "genes"), P(), P())
    return jax.shard_map(body, mesh=mesh, in_specs=in_specs, out_specs=out_specs, check_vma=False)
```

```python
import functools
import math

import jax
import jax.numpy as jnp
from jax import lax
from jax.experimental import pallas as pl
from jax.experimental.pallas import tpu as pltpu
from jax.sharding import PartitionSpec as P

BASIS = 32
BLOCK = 16
STEPS = 3
SLOTS = BASIS + STEPS * BLOCK
WEIGHT = SLOTS + BLOCK
LANES = 128
F32 = jnp.float32
BF16 = jnp.bfloat16
HIGHEST = lax.Precision.HIGHEST
MESH = pl.DeviceIdType.MESH


def exact(lhs, rhs):
    return jnp.dot(lhs, rhs, precision=HIGHEST, preferred_element_type=F32)


def exact_rows(lhs, rhs):
    return lax.dot_general(
        lhs, rhs, (((1,), (1,)), ((), ())), precision=HIGHEST, preferred_element_type=F32
    )


def split(values):
    high = values.astype(BF16)
    return high, (values - high.astype(F32)).astype(BF16)


def product(high, both, rhs_high, rhs_low, dims):
    rows = high.shape[0]
    first = lax.dot_general(both, rhs_high, (dims, ((), ())), preferred_element_type=F32)
    second = lax.dot_general(high, rhs_low, (dims, ((), ())), preferred_element_type=F32)
    return first[:rows] + (first[rows:] + second)


ALONG = ((1,), (0,))
ROWS = ((1,), (1,))


def loop(start, stop, step):
    def one(k, carry):
        step(k)
        return carry

    lax.fori_loop(start, stop, one, 0)


def orthonormal(gram, near, lower):
    lane = lax.broadcasted_iota(jnp.int32, (BLOCK, LANES), 1)
    row = lax.broadcasted_iota(jnp.int32, (BLOCK, LANES), 0)
    coeffs = jnp.where(lane < SLOTS, gram, 0.0)
    squares = gram[:, SLOTS : SLOTS + BLOCK]
    combined = coeffs + coeffs - (exact(coeffs, near) + exact_rows(coeffs, lower))
    residue = coeffs - (exact(combined, near) + exact_rows(combined, lower))
    squares = squares - exact_rows(combined, coeffs) - exact_rows(residue, combined)
    change = jnp.where(lane == row + SLOTS, 1.0, -combined)
    parts = [squares, residue, change]
    for k in range(BLOCK):
        pivot = parts[0][k : k + 1, k : k + 1]
        root = lax.rsqrt(pivot)
        root = root * (1.5 - 0.5 * pivot * root * root)
        column = parts[0][:, k : k + 1] * root
        after = []
        for part in parts:
            scaled = part[k : k + 1, :] * root
            places = lax.broadcasted_iota(jnp.int32, part.shape, 0)
            after.append(
                jnp.where(places > k, part - column * scaled, jnp.where(places == k, scaled, part))
            )
        parts = after
    spot = lax.broadcasted_iota(jnp.int32, (BLOCK, BLOCK), 0)
    other = lax.broadcasted_iota(jnp.int32, (BLOCK, BLOCK), 1)
    upper = jnp.where(other >= spot, parts[0], 0.0)
    factor = exact_rows(jnp.where(other == spot, 1.0, 0.0).astype(F32), upper)
    return factor, parts[1], parts[2]


def kernel(
    n, g, width, scales,
    live, counts, left_basis, right_basis, right_start,
    left_out, right_out, diag_out, couple_out,
    cnt, logged, bhi, blo, rb, sl, mr, el, tl, er, tr,
    w, ra, rt, rz, wb, rab, rtb, rzb, pb, stack, ground, tpart, tfrom,
    mu, wsum, chg, gram0, gram, xs0, xb0, xg, gx, gy, gz,
    in_sem, as_sem, ar_sem, bs_sem, br_sem, zs_sem, zr_sem,
    bas_sem, bar_sem, bbs_sem, bbr_sem, bzs_sem, bzr_sem,
    cs_sem, cr_sem, ds_sem, fs_sem, ts_sem, tr_sem,
    ms_sem, mr_sem, g0s_sem, g0r_sem, gs_sem, gr_sem, s0s_sem, s0r_sem, b0s_sem, b0r_sem,
    xs_sem, xr_sem, gxs_sem, gxr_sem, gys_sem, gyr_sem, gzs_sem, gzr_sem,
):
    cells, genes = counts.shape
    me = lax.axis_index("cells")
    mine = lax.axis_index("genes")
    core = lax.rem(me, 2)
    chip = me // 2
    h = n // 2
    b = 1 << ((h.bit_length() - 1) // 2)
    b = b if h % b == 0 else 1
    a = h // b
    zi, yi = chip // b, lax.rem(chip, b)
    sibling = me + 1 - 2 * core
    tiles = width // LANES
    whole, spare = genes // width, genes % width
    lane = lax.broadcasted_iota(jnp.int32, (BLOCK, LANES), 1)
    row = lax.broadcasted_iota(jnp.int32, (BLOCK, LANES), 0)

    def along_cells(src, dst, send, recv, peer):
        return pltpu.make_async_remote_copy(
            src_ref=src, dst_ref=dst, send_sem=send, recv_sem=recv,
            device_id=(peer, mine), device_id_type=MESH,
        )

    def along_genes(src, dst, send, recv, peer):
        return pltpu.make_async_remote_copy(
            src_ref=src, dst_ref=dst, send_sem=send, recv_sem=recv,
            device_id=(me, peer), device_id_type=MESH,
        )

    def along_plane(src, dst, send, recv, peer):
        return along_cells(src, dst, send, recv, 2 * b * zi + peer)

    def along_column(src, dst, send, recv, peer):
        return along_cells(src, dst, send, recv, 2 * (peer * b + yi) + core)

    loads = []
    for d in range(n):
        cols = max(0, min(width, genes - d * width))
        if cols:
            here = pl.ds(d * width, cols)
            loads.append((d, [
                pltpu.make_async_copy(counts.at[:, here], cnt.at[d, :, pl.ds(0, cols)], in_sem.at[d, 0]),
                pltpu.make_async_copy(right_basis.at[:, here], rb.at[d, pl.ds(0, BASIS), pl.ds(0, cols)], in_sem.at[d, 1]),
                pltpu.make_async_copy(right_start.at[:, here], rb.at[d, pl.ds(BASIS, BLOCK), pl.ds(0, cols)], in_sem.at[d, 2]),
            ]))
        if cols < width:
            cnt[d, :, cols:] = jnp.zeros((cells, width - cols), jnp.int32)
            rb[d, :, cols:] = jnp.zeros((BASIS + BLOCK, width - cols), F32)
    for _, trio in loads:
        trio[0].start()
    for _, trio in loads:
        trio[1].start()
        trio[2].start()

    barrier = pltpu.get_barrier_semaphore()

    def greet_cells(k):
        pl.semaphore_signal(barrier, inc=1, device_id=(lax.rem(me + k, n), mine), device_id_type=MESH)

    def greet_genes(k):
        pl.semaphore_signal(barrier, inc=1, device_id=(me, lax.rem(mine + k, g)), device_id_type=MESH)

    loop(1, n, greet_cells)
    loop(1, g, greet_genes)

    def spread(copy, buf, at, size, send, recv):
        def go(k):
            copy(buf.at[at], buf.at[at], send.at[k], recv.at[at], lax.rem(at + k, size)).start()

        loop(1, size, go)

    def waited(copy, buf, at, size, send, recv):
        def end(k):
            source = lax.rem(at + size - k, size)
            item = copy(buf.at[source], buf.at[source], send.at[k], recv.at[source], lax.rem(at + k, size))
            item.wait_send()
            item.wait_recv()

        loop(1, size, end)

    def gathered(copy, buf, at, size, send, recv):
        waited(copy, buf, at, size, send, recv)
        return lax.fori_loop(
            1, size, lambda k, total: total + buf[k], buf[0]
        )

    def order(k):
        return lax.rem(zi + 1 + lax.rem(k, a), a), lax.rem(yi + 1 + k // a, b)

    class Scatter:
        def __init__(self, part, fromcore, fromy, fromz, sems):
            self.part, self.fromcore, self.fromy, self.fromz = part, fromcore, fromy, fromz
            self.cs, self.cr, self.ys, self.yr, self.zs, self.zr = sems

        def over(self, d, t):
            return along_cells(self.part.at[d], self.fromcore.at[t], self.cs.at[t], self.cr.at[t], sibling)

        def first(self, produce):
            def one(k):
                z, y = order(k)
                t = z * b + y
                d = 2 * t + 1 - core
                produce(d)
                self.over(d, t).start()

            loop(0, h, one)

        def second(self, produce):
            def one(k, send):
                z, y = order(k)
                t = z * b + y
                d = 2 * t + core
                produce(d)
                self.over(d, t).wait_recv()
                self.part[d] = self.part[d] + self.fromcore[t]
                if send:
                    to = z * b + yi
                    along_cells(
                        self.part.at[d], self.fromy.at[to], self.ys.at[t], self.yr.at[to],
                        2 * (zi * b + y) + core,
                    ).start()

            loop(0, h - a, lambda k: one(k, True))
            loop(h - a, h, lambda k: one(k, False))

        def complete(self, z):
            d = 2 * (z * b + yi) + core

            def add(k):
                source = z * b + lax.rem(yi + k, b)
                along_cells(self.part.at[d], self.fromy.at[source], self.ys.at[source], self.yr.at[source], sibling).wait_recv()
                self.part[d] = self.part[d] + self.fromy[source]

            loop(1, b, add)
            return d

        def third(self):
            def one(k):
                z = lax.rem(zi + k, a)
                d = self.complete(z)
                along_cells(self.part.at[d], self.fromz.at[zi], self.zs.at[z], self.zr.at[zi], d).start()

            loop(1, a, one)
            self.complete(zi)

        def fourth(self, result, rows):
            result[rows] = self.part[me]

            def one(k):
                z = lax.rem(zi + a - k, a)
                along_cells(self.part.at[me], self.fromz.at[z], self.zs.at[z], self.zr.at[z], sibling).wait_recv()
                result[rows] = result[rows] + self.fromz[z]

            loop(1, a, one)

        def ended(self):
            loop(0, h, lambda t: self.over(t, t).wait_send())

            def sent_y(k):
                z, y = order(k)
                t = z * b + y
                along_cells(self.part.at[t], self.fromy.at[t], self.ys.at[t], self.yr.at[t], sibling).wait_send()

            loop(0, h - a, sent_y)

            def sent_z(k):
                z = lax.rem(zi + k, a)
                along_cells(self.part.at[z], self.fromz.at[z], self.zs.at[z], self.zr.at[z], sibling).wait_send()

            loop(1, a, sent_z)

    walk = Scatter(w, ra, rt, rz, (as_sem, ar_sem, bs_sem, br_sem, zs_sem, zr_sem))
    base = Scatter(wb, rab, rtb, rzb, (bas_sem, bar_sem, bbs_sem, bbr_sem, bzs_sem, bzr_sem))

    live_here = live[0]
    weights_row = jnp.where(
        lax.broadcasted_iota(jnp.int32, (1, cells), 1) < live_here, 1.0, 0.0
    ).astype(F32)
    weights = jnp.where(
        lax.broadcasted_iota(jnp.int32, (cells, LANES), 0) < live_here, 1.0, 0.0
    ).astype(F32)
    for table in (sl, mr, tl, tr, stack):
        table[...] = jnp.zeros_like(table)
    same = jnp.where(
        lax.broadcasted_iota(jnp.int32, (LANES, LANES), 0)
        == lax.broadcasted_iota(jnp.int32, (LANES, LANES), 1),
        1.0, 0.0,
    ).astype(F32)
    er[...] = same
    chg[...] = jnp.where(lane == row + SLOTS, 1.0, 0.0)
    sl[0:BASIS] = left_basis[...] * weights_row
    sl[WEIGHT : WEIGHT + 8] = jnp.where(
        lax.broadcasted_iota(jnp.int32, (8, cells), 0) == 0, weights_row, 0.0
    )
    gram0[me, 0:BASIS] = exact_rows(sl[0:BASIS], sl[...])
    gram0[me, BASIS:] = exact_rows(sl[WEIGHT : WEIGHT + 8], sl[...])

    def take_log(d):
        for i in range(tiles):
            here = slice(i * LANES, (i + 1) * LANES)
            logged[d, :, here] = jnp.log(1.0 + cnt[d, :, here].astype(F32)) * weights

    for _, trio in loads:
        trio[0].wait()
    take_log(me)
    portion = 1.0 / jnp.maximum(live_here, 1).astype(F32)
    for i in range(tiles):
        here = slice(i * LANES, (i + 1) * LANES)
        mu[me, :, here] = jnp.sum(logged[me, :, here], axis=0, keepdims=True) * portion
    pl.semaphore_wait(barrier, n - 1 + g - 1)
    spread(along_cells, mu, me, n, ms_sem, mr_sem)
    spread(along_cells, gram0, me, n, g0s_sem, g0r_sem)
    loop(1, n, lambda k: take_log(lax.rem(me + k, n)))

    for _, trio in loads:
        trio[1].wait()
        trio[2].wait()
    xs0[mine] = jnp.zeros((BASIS + BLOCK, LANES), F32)
    xb0[mine] = jnp.zeros((BASIS, LANES), F32)
    xg[0, mine] = jnp.zeros((BLOCK, LANES), F32)

    def fill(d):
        high, low = split(rb[d])
        bhi[d, cells : cells + BASIS + BLOCK] = high
        blo[d, cells : cells + BASIS + BLOCK] = low
        blank = jnp.zeros((LANES - BASIS - BLOCK, width), BF16)
        bhi[d, cells + BASIS + BLOCK :] = blank
        blo[d, cells + BASIS + BLOCK :] = blank
        both = jnp.concatenate([high, low], axis=0)
        xs0[mine] = xs0[mine] + product(high, both, bhi[d, cells:], blo[d, cells:], ROWS)

    loop(0, n, fill)
    spread(along_genes, xs0, mine, g, s0s_sem, s0r_sem)
    waited(along_cells, mu, me, n, ms_sem, mr_sem)

    bhigh, blow = split(jnp.concatenate(
        [sl[0:BASIS], sl[WEIGHT : WEIGHT + 8], jnp.zeros((8, cells), F32)], axis=0
    ))
    bboth = jnp.concatenate([bhigh, blow], axis=0)

    def center(d):
        for i in range(tiles):
            here = slice(i * LANES, (i + 1) * LANES)
            high, low = split(logged[d, :, here] - weights * mu[d, :, here])
            bhi[d, 0:cells, here] = high
            blo[d, 0:cells, here] = low
        high = bhi[d, cells : cells + BASIS + BLOCK]
        both = jnp.concatenate([high, blo[d, cells : cells + BASIS + BLOCK]], axis=0)
        met = product(high, both, bhi[d, 0:cells], blo[d, 0:cells], ROWS)
        xb0[mine] = xb0[mine] + met[0:BASIS]
        xg[0, mine] = xg[0, mine] + met[BASIS:]
        made = product(bhigh, bboth, bhi[d, 0:cells], blo[d, 0:cells], ALONG)
        wb[d] = made[0:BASIS]
        tpart[d] = made[BASIS : BASIS + 1]

    base.first(center)
    base.second(center)
    spread(along_genes, xg.at[0], mine, g, xs_sem.at[0], xr_sem.at[0])
    spread(along_genes, xb0, mine, g, b0s_sem, b0r_sem)

    def give(k):
        d = lax.rem(me + k, n)
        along_cells(tpart.at[d], tfrom.at[me], ts_sem.at[k], tr_sem.at[me], d).start()

    loop(1, n, give)
    near = gathered(along_cells, gram0, me, n, g0s_sem, g0r_sem)
    corner = lax.broadcasted_iota(jnp.int32, (LANES, LANES), 0)
    across = lax.broadcasted_iota(jnp.int32, (BASIS, LANES), 1)
    el[...] = jnp.where((same > 0) & (corner >= BASIS), 1.0, 0.0)
    el[0:BASIS] = jnp.where(across < SLOTS, near[0:BASIS], 0.0)
    wsum[...] = near[BASIS:]
    live_total = near[BASIS : BASIS + 1, WEIGHT : WEIGHT + 1]
    inverse = 1.0 / live_total
    factor_scale = lax.rsqrt(live_total)
    factor_scale = factor_scale * (1.5 - 0.5 * live_total * factor_scale * factor_scale)
    er[0 : BASIS + BLOCK] = gathered(along_genes, xs0, mine, g, s0s_sem, s0r_sem)

    def turned(column, start):
        return jnp.sum(jnp.where(lane == row + start, column, 0.0), axis=0, keepdims=True)

    def fresh(d):
        chigh, clow = split(chg[...])
        cboth = jnp.concatenate([chigh, clow], axis=0)
        return product(chigh, cboth, bhi[d, cells:], blo[d, cells:], ALONG)

    def emit(d, rows, values):
        @pl.when(d < whole)
        def _():
            right_out[rows, pl.ds(pl.multiple_of(d * width, LANES), width)] = values * scales[1]

        if spare:
            @pl.when(d == whole)
            def _():
                right_out[rows, whole * width : genes] = values[:, :spare] * scales[1]

    def update(j):
        later = pl.multiple_of(cells + BASIS + (j + 1) * BLOCK, BLOCK)
        rows = pl.ds(pl.multiple_of(j * BLOCK, BLOCK), BLOCK)

        def right(d):
            values = fresh(d)
            vhigh, vlow = split(values)
            bhi[d, pl.ds(later, BLOCK)] = vhigh
            blo[d, pl.ds(later, BLOCK)] = vlow
            emit(d, rows, values)

        loop(0, n, right)

    def keep(d, values):
        phigh, plow = split(values)
        bhi[d, cells + SLOTS : cells + SLOTS + BLOCK] = phigh
        blo[d, cells + SLOTS : cells + SLOTS + BLOCK] = plow
        return phigh, jnp.concatenate([phigh, plow], axis=0)

    def begin(j):
        @pl.when(j == 0)
        def _():
            base.third()

            def take(k):
                source = lax.rem(me + n - k, n)
                item = along_cells(tpart.at[source], tfrom.at[source], ts_sem.at[k], tr_sem.at[source], sibling)
                item.wait_send()
                item.wait_recv()
                tpart[me] = tpart[me] + tfrom[source]

            loop(1, n, take)
            stack[WEIGHT : WEIGHT + 1] = tpart[me]
            mr[0:BASIS] = gathered(along_genes, xb0, mine, g, b0s_sem, b0r_sem)

    def step(j, final):
        position = BASIS + j * BLOCK
        position = position if final else pl.multiple_of(position, BLOCK)
        mr[SLOTS : SLOTS + BLOCK] = gathered(along_genes, xg.at[j], mine, g, xs_sem.at[j], xr_sem.at[j])
        vectors = exact(chg[...], mr[...])
        mr[pl.ds(position, BLOCK)] = vectors
        sl[SLOTS : SLOTS + BLOCK] = vectors
        gram[me] = exact_rows(vectors, sl[...])
        spread(along_cells, gram, me, n, gs_sem, gr_sem)
        high, low = split(vectors)
        both = jnp.concatenate([high, low], axis=0)

        def produce(d):
            w[d] = product(high, both, bhi[d, 0:cells], blo[d, 0:cells], ALONG)

        walk.first(produce)
        walk.second(produce)
        if final:
            update(j - 1)
        else:
            begin(j)
            pl.when(j > 0)(lambda: update(j - 1))
        total = gathered(along_cells, gram, me, n, gs_sem, gr_sem)
        held = total[:, WEIGHT : WEIGHT + 1] * inverse
        weighed = wsum[0:1] + turned(total[:, WEIGHT : WEIGHT + 1], SLOTS)
        scale = jnp.where(lane < SLOTS, factor_scale, factor_scale * factor_scale)
        factor, against, change = orthonormal((total - held * weighed) * scale, el[...], tl[...])
        diag_out[j] = factor
        tilt = jnp.sum(jnp.where(lane < SLOTS, change * wsum[0:1], 0.0), axis=1, keepdims=True)
        wsum[0:1] = wsum[0:1] + turned(tilt, position)
        shift = jnp.sum(
            jnp.where((lane >= SLOTS) & (lane < WEIGHT), change * turned(held, SLOTS), 0.0), axis=1, keepdims=True
        )
        blend = jnp.where(
            lane < SLOTS, change,
            jnp.where(lane < WEIGHT, change * factor_scale, jnp.where(lane == WEIGHT, -shift * factor_scale, 0.0)),
        )
        leftvec = exact(blend, sl[...])
        sl[pl.ds(position, BLOCK)] = leftvec
        el[pl.ds(position, BLOCK)] = el[pl.ds(position, BLOCK)] + against
        tl[pl.ds(position, BLOCK)] = against
        left_out[pl.ds(position - BASIS, BLOCK)] = leftvec * scales[0]
        tilt = tilt * inverse
        blend = jnp.where(lane == WEIGHT, blend - tilt, blend) * factor_scale
        walk.third()
        if not final:
            pl.when(j == 0)(lambda: base.fourth(stack, slice(0, BASIS)))
        ground[...] = exact(jnp.where((lane < SLOTS) | (lane >= WEIGHT), blend, 0.0), stack[...])
        walk.fourth(stack, slice(SLOTS, SLOTS + BLOCK))
        columns = [blend[:, SLOTS + k : SLOTS + k + 1] for k in range(BLOCK)]
        for i in range(tiles):
            here = slice(i * LANES, (i + 1) * LANES)
            values = ground[:, here]
            for k in range(BLOCK):
                values = values + columns[k] * stack[SLOTS + k : SLOTS + k + 1, here]
            pb[me, :, here] = values

        def relay(z):
            t = z * b + yi
            d = 2 * t + core

            def to_y(k):
                y = lax.rem(yi + k, b)
                along_cells(pb.at[d], pb.at[d], fs_sem.at[z * b + y], cr_sem.at[d], 2 * (zi * b + y) + core).start()

            loop(1, b, to_y)
            along_cells(pb.at[d], pb.at[d], ds_sem.at[t], cr_sem.at[d], sibling).start()

        def arrived(d):
            along_cells(pb.at[d], pb.at[d], ds_sem.at[0], cr_sem.at[d], sibling).wait_recv()

        def go(k):
            z = lax.rem(zi + k, a)
            along_cells(pb.at[me], pb.at[me], cs_sem.at[z], cr_sem.at[me], 2 * (z * b + yi) + core).start()

        loop(1, a, go)
        relay(zi)
        phigh, pboth = keep(me, pb[me])
        gx[mine] = product(phigh, pboth, bhi[me, cells:], blo[me, cells:], ROWS)
        spread(along_genes, gx, mine, g, gxs_sem, gxr_sem)
        if not final:
            stack[pl.ds(position, BLOCK)] = (
                pb[me] * (live_total * factor_scale) + tilt * stack[WEIGHT : WEIGHT + 1]
            )
            xg[j + 1, mine] = jnp.zeros((BLOCK, LANES), F32)

        def consume(d):
            phigh, pboth = keep(d, pb[d])
            if final:
                emit(d, pl.ds((STEPS - 1) * BLOCK, BLOCK), fresh(d))
            else:
                xg[j + 1, mine] = xg[j + 1, mine] + product(phigh, pboth, bhi[d, 0:cells], blo[d, 0:cells], ROWS)

        def pass_z(k):
            z = lax.rem(zi + a - k, a)
            arrived(2 * (z * b + yi) + core)
            relay(z)

        seat = 2 * yi + core
        loop(1, min(2, a), pass_z)
        gy[seat] = gathered(along_genes, gx, mine, g, gxs_sem, gxr_sem)
        spread(along_plane, gy, seat, 2 * b, gys_sem, gyr_sem)
        loop(min(2, a), min(3, a), pass_z)
        gz[zi] = gathered(along_plane, gy, seat, 2 * b, gys_sem, gyr_sem)
        spread(along_column, gz, zi, a, gzs_sem, gzr_sem)
        loop(min(3, a), a, pass_z)

        def close():
            total = gathered(along_column, gz, zi, a, gzs_sem, gzr_sem)
            factor, against, change = orthonormal(total, er[...], tr[...])
            couple_out[j] = factor
            chg[...] = change
            if not final:
                later = pl.multiple_of(position + BLOCK, BLOCK)
                er[pl.ds(later, BLOCK)] = er[pl.ds(later, BLOCK)] + against
                tr[pl.ds(later, BLOCK)] = against

        if final:
            close()
        consume(me)
        loop(1, a, lambda k: consume(2 * (lax.rem(zi + a - k, a) * b + yi) + core))

        def pass_y(k):
            z = lax.rem(zi + a - lax.rem(k, a), a)
            t = z * b + lax.rem(yi + 1 + k // a, b)
            d = 2 * t + core
            arrived(d)
            along_cells(pb.at[d], pb.at[d], ds_sem.at[t], cr_sem.at[d], sibling).start()
            consume(d)

        loop(0, h - a, pass_y)

        def rest(k):
            z = lax.rem(zi + a - lax.rem(k, a), a)
            t = z * b + lax.rem(yi + k // a, b)
            d = 2 * t + 1 - core
            arrived(d)
            consume(d)

        loop(0, h, rest)
        if not final:
            spread(along_genes, xg.at[j + 1], mine, g, xs_sem.at[j + 1], xr_sem.at[j + 1])
            close()
        walk.ended()

        def ended(t):
            along_cells(pb.at[t], pb.at[t], ds_sem.at[t], cr_sem.at[t], sibling).wait_send()

        loop(0, h, ended)

        def ended_y(k):
            z, y = order(k)
            t = z * b + y
            along_cells(pb.at[t], pb.at[t], fs_sem.at[t], cr_sem.at[t], sibling).wait_send()

        loop(0, h - a, ended_y)

        def ended_z(k):
            z = lax.rem(zi + k, a)
            along_cells(pb.at[z], pb.at[z], cs_sem.at[z], cr_sem.at[z], sibling).wait_send()

        loop(1, a, ended_z)

    loop(0, STEPS - 1, lambda j: step(j, False))
    step(STEPS - 1, True)
    base.ended()


def body(counts, live_rows, left_basis, right_basis, right_start):
    cells, genes = counts.shape
    n = lax.axis_size("cells")
    g = lax.axis_size("genes")
    h = n // 2
    width = -(-(genes // LANES) // n) * LANES
    scales = (math.sqrt(float(cells * n)), math.sqrt(float(genes * g)))
    vmem = pl.BlockSpec(memory_space=pltpu.VMEM)
    anywhere = pl.BlockSpec(memory_space=pl.ANY)
    held = lambda *shape: pltpu.VMEM(shape, F32)
    square = held(LANES, LANES)
    dma = lambda *shape: pltpu.SemaphoreType.DMA(shape)
    out_shape = (
        jax.ShapeDtypeStruct((STEPS * BLOCK, cells), F32),
        jax.ShapeDtypeStruct((STEPS * BLOCK, genes), F32),
        jax.ShapeDtypeStruct((STEPS, BLOCK, BLOCK), F32),
        jax.ShapeDtypeStruct((STEPS, BLOCK, BLOCK), F32),
    )
    buffers = lambda rows: [
        held(n, rows, width), held(h, rows, width), held(h, rows, width), held(h, rows, width),
    ]
    scratch = [
        pltpu.VMEM((n, cells, width), jnp.int32),
        held(n, cells, width),
        pltpu.VMEM((n, cells + LANES, width), BF16),
        pltpu.VMEM((n, cells + LANES, width), BF16),
        held(n, BASIS + BLOCK, width),
        square, square, square, square, square, square,
        *buffers(BLOCK),
        *buffers(BASIS),
        held(n, BLOCK, width),
        held(LANES, width),
        held(BLOCK, width),
        held(n, 1, width),
        held(n, 1, width),
        held(n, 1, width),
        held(8, LANES),
        held(BLOCK, LANES),
        held(n, BASIS + 8, LANES),
        held(n, BLOCK, LANES),
        held(g, BASIS + BLOCK, LANES),
        held(g, BASIS, LANES),
        held(STEPS, g, BLOCK, LANES),
        held(g, BLOCK, LANES),
        held(n, BLOCK, LANES),
        held(h, BLOCK, LANES),
        dma(n, 3),
        *[dma(h)] * 6,
        *[dma(h)] * 6,
        dma(h), dma(n), dma(h), dma(h), dma(n), dma(n),
        *[dma(n)] * 6,
        *[dma(g)] * 4,
        dma(STEPS, g), dma(STEPS, g),
        dma(g), dma(g), dma(n), dma(n), dma(h), dma(h),
    ]
    return pl.pallas_call(
        functools.partial(kernel, n, g, width, scales),
        out_shape=out_shape,
        in_specs=[pl.BlockSpec(memory_space=pltpu.SMEM), anywhere, vmem, anywhere, anywhere],
        out_specs=(vmem, vmem, vmem, vmem),
        scratch_shapes=scratch,
        compiler_params=pltpu.CompilerParams(
            collective_id=0, has_side_effects=True, vmem_limit_bytes=66 * 1000 * 1000
        ),
    )(live_rows, counts, left_basis, right_basis, right_start)


def solution(mesh):
    in_specs = (
        P("cells", "genes"),
        P("cells"),
        P(None, "cells"),
        P(None, "genes"),
        P(None, "genes"),
    )
    out_specs = (P(None, "cells"), P(None, "genes"), P(), P())
    return jax.shard_map(body, mesh=mesh, in_specs=in_specs, out_specs=out_specs, check_vma=False)
```

```python
import functools
import math

import jax
import jax.numpy as jnp
from jax import lax
from jax.experimental import pallas as pl
from jax.experimental.pallas import tpu as pltpu
from jax.sharding import PartitionSpec as P

BASIS = 32
BLOCK = 16
STEPS = 3
SLOTS = BASIS + STEPS * BLOCK
WEIGHT = SLOTS + BLOCK
LAG = 2
LANES = 128
F32 = jnp.float32
BF16 = jnp.bfloat16
HIGHEST = lax.Precision.HIGHEST
MESH = pl.DeviceIdType.MESH


def exact(lhs, rhs):
    return jnp.dot(lhs, rhs, precision=HIGHEST, preferred_element_type=F32)


def exact_rows(lhs, rhs):
    return lax.dot_general(
        lhs, rhs, (((1,), (1,)), ((), ())), precision=HIGHEST, preferred_element_type=F32
    )


def split(values):
    high = values.astype(BF16)
    return high, (values - high.astype(F32)).astype(BF16)


def product(high, both, rhs_high, rhs_low, dims):
    rows = high.shape[0]
    first = lax.dot_general(both, rhs_high, (dims, ((), ())), preferred_element_type=F32)
    second = lax.dot_general(high, rhs_low, (dims, ((), ())), preferred_element_type=F32)
    return first[:rows] + (first[rows:] + second)


ALONG = ((1,), (0,))
ROWS = ((1,), (1,))


def loop(start, stop, step, unroll=1):
    def one(k, carry):
        step(k)
        return carry

    lax.fori_loop(start, stop, one, 0, unroll=unroll if (stop - start) % unroll == 0 else 1)


def both_sides(gram, identity):
    gap = identity - gram
    return identity + gap, exact(gap, gap)


def orthonormal(gram, first, second):
    lane = lax.broadcasted_iota(jnp.int32, (BLOCK, LANES), 1)
    row = lax.broadcasted_iota(jnp.int32, (BLOCK, LANES), 0)
    coeffs = jnp.where(lane < SLOTS, gram, 0.0)
    combined = exact(coeffs, first)
    residue = exact(coeffs, second)
    squares = gram[:, SLOTS : SLOTS + BLOCK] - exact_rows(
        jnp.concatenate([combined, residue], axis=1), jnp.concatenate([coeffs, combined], axis=1)
    )
    change = jnp.where(lane == row + SLOTS, 1.0, -combined)
    columns = [jnp.broadcast_to(squares[:, k : k + 1], (BLOCK, LANES)) for k in range(BLOCK)]
    factor = jnp.zeros((BLOCK, LANES), F32)
    for k in range(BLOCK):
        pivot = jnp.broadcast_to(columns[k][k : k + 1], (BLOCK, LANES))
        root = lax.rsqrt(pivot)
        root = root * (1.5 - 0.5 * pivot * root * root)
        column = columns[k] * root
        factor = jnp.where((lane == k) & (row >= k), column, factor)
        below = jnp.where(row > k, column, 0.0)
        for i in range(k + 1, BLOCK):
            columns[i] = columns[i] - column * jnp.broadcast_to(column[i : i + 1], (BLOCK, LANES))
        scaled = jnp.broadcast_to(residue[k : k + 1], (BLOCK, LANES)) * root
        residue = jnp.where(row == k, scaled, residue - below * scaled)
        scaled = jnp.broadcast_to(change[k : k + 1], (BLOCK, LANES)) * root
        change = jnp.where(row == k, scaled, change - below * scaled)
    return factor[:, :BLOCK], residue, change


def kernel(
    n, g, width, scales,
    live, counts, left_basis, right_basis, right_start,
    left_out, right_out, diag_out, couple_out,
    cnt, logged, lhi, llo, vhi, vlo, rb, sl, mr, el, er, l1, l2, r1, r2,
    w, ra, rt, rz, wb, rab, rtb, rzb, pb, stack, ground, tpart, tfrom,
    mu, wsum, chg, gram0, gram, xs0, xb0, xg, gx, gy, gz,
    in_sem, as_sem, ar_sem, bs_sem, br_sem, zs_sem, zr_sem,
    bas_sem, bar_sem, bbs_sem, bbr_sem, bzs_sem, bzr_sem,
    cs_sem, cr_sem, ds_sem, fs_sem, ts_sem, tr_sem,
    ms_sem, mr_sem, g0s_sem, g0r_sem, gs_sem, gr_sem, s0s_sem, s0r_sem, b0s_sem, b0r_sem,
    xs_sem, xr_sem, gxs_sem, gxr_sem, gys_sem, gyr_sem, gzs_sem, gzr_sem,
):
    cells, genes = counts.shape
    me = lax.axis_index("cells")
    mine = lax.axis_index("genes")
    core = lax.rem(me, 2)
    chip = me // 2
    h = n // 2
    b = 1 << ((h.bit_length() - 1) // 2)
    b = b if h % b == 0 else 1
    a = h // b
    zi, yi = chip // b, lax.rem(chip, b)
    sibling = me + 1 - 2 * core
    tiles = width // LANES
    whole, spare = genes // width, genes % width
    lane = lax.broadcasted_iota(jnp.int32, (BLOCK, LANES), 1)
    row = lax.broadcasted_iota(jnp.int32, (BLOCK, LANES), 0)

    def along_cells(src, dst, send, recv, peer):
        return pltpu.make_async_remote_copy(
            src_ref=src, dst_ref=dst, send_sem=send, recv_sem=recv,
            device_id=(peer, mine), device_id_type=MESH,
        )

    def along_genes(src, dst, send, recv, peer):
        return pltpu.make_async_remote_copy(
            src_ref=src, dst_ref=dst, send_sem=send, recv_sem=recv,
            device_id=(me, peer), device_id_type=MESH,
        )

    def along_plane(src, dst, send, recv, peer):
        return along_cells(src, dst, send, recv, 2 * b * zi + peer)

    def along_column(src, dst, send, recv, peer):
        return along_cells(src, dst, send, recv, 2 * (peer * b + yi) + core)

    loads = []
    for d in range(n):
        cols = max(0, min(width, genes - d * width))
        if cols:
            here = pl.ds(d * width, cols)
            loads.append((d, [
                pltpu.make_async_copy(counts.at[:, here], cnt.at[d, :, pl.ds(0, cols)], in_sem.at[d, 0]),
                pltpu.make_async_copy(right_basis.at[:, here], rb.at[d, pl.ds(0, BASIS), pl.ds(0, cols)], in_sem.at[d, 1]),
                pltpu.make_async_copy(right_start.at[:, here], rb.at[d, pl.ds(BASIS, BLOCK), pl.ds(0, cols)], in_sem.at[d, 2]),
            ]))
        if cols < width:
            cnt[d, :, cols:] = jnp.zeros((cells, width - cols), jnp.int32)
            rb[d, :, cols:] = jnp.zeros((BASIS + BLOCK, width - cols), F32)
    for _, trio in loads:
        trio[0].start()
    for _, trio in loads:
        trio[1].start()
        trio[2].start()

    barrier = pltpu.get_barrier_semaphore()

    def greet_cells(k):
        pl.semaphore_signal(barrier, inc=1, device_id=(lax.rem(me + k, n), mine), device_id_type=MESH)

    def greet_genes(k):
        pl.semaphore_signal(barrier, inc=1, device_id=(me, lax.rem(mine + k, g)), device_id_type=MESH)

    loop(1, n, greet_cells)
    loop(1, g, greet_genes)

    def spread(copy, buf, at, size, send, recv):
        def go(k):
            copy(buf.at[at], buf.at[at], send.at[k], recv.at[at], lax.rem(at + k, size)).start()

        loop(1, size, go)

    def waited(copy, buf, at, size, send, recv):
        def end(k):
            source = lax.rem(at + size - k, size)
            item = copy(buf.at[source], buf.at[source], send.at[k], recv.at[source], lax.rem(at + k, size))
            item.wait_send()
            item.wait_recv()

        loop(1, size, end)

    def gathered(copy, buf, at, size, send, recv):
        waited(copy, buf, at, size, send, recv)
        return lax.fori_loop(
            1, size, lambda k, total: total + buf[k], buf[0]
        )

    def onward(k):
        return lax.rem(zi + k, a)

    def behind(k):
        return lax.rem(zi + a - k, a)

    def order(k):
        return onward(1 + lax.rem(k, a)), lax.rem(yi + 1 + k // a, b)

    class Scatter:
        def __init__(self, part, fromcore, fromy, fromz, sems):
            self.part, self.fromcore, self.fromy, self.fromz = part, fromcore, fromy, fromz
            self.cs, self.cr, self.ys, self.yr, self.zs, self.zr = sems

        def over(self, d, t):
            return along_cells(self.part.at[d], self.fromcore.at[t], self.cs.at[t], self.cr.at[t], sibling)

        def launch(self, produce):
            def other(k):
                z, y = order(k)
                t = z * b + y
                return t, 2 * t + 1 - core

            def own(k):
                z, y = order(k)
                t = z * b + y
                return z, y, t, 2 * t + core

            def join(k):
                z, y, t, d = own(k)
                self.over(d, t).wait_recv()
                self.part[d] = self.part[d] + self.fromcore[t]

                @pl.when(k < h - a)
                def _():
                    to = z * b + yi
                    along_cells(
                        self.part.at[d], self.fromy.at[to], self.ys.at[t], self.yr.at[to],
                        2 * (zi * b + y) + core,
                    ).start()

            def pair(k):
                t, d = other(k)
                produce(d)
                produce(own(k)[3])
                self.over(d, t).start()

            def one(k):
                pair(k)
                join(k - LAG)

            loop(0, LAG, pair)
            loop(LAG, h, one)
            loop(h - LAG, h, join)

        def complete(self, z):
            d = 2 * (z * b + yi) + core

            def add(k):
                source = z * b + lax.rem(yi + k, b)
                along_cells(self.part.at[d], self.fromy.at[source], self.ys.at[source], self.yr.at[source], sibling).wait_recv()
                self.part[d] = self.part[d] + self.fromy[source]

            loop(1, b, add)
            return d

        def third(self, start, stop):
            def one(k):
                z = onward(1 + k)
                d = self.complete(z)
                along_cells(self.part.at[d], self.fromz.at[zi], self.zs.at[z], self.zr.at[zi], d).start()

            loop(min(start, a - 1), min(stop, a - 1), one)
            if stop >= a:
                self.complete(zi)

        def fourth(self, result, rows):
            result[rows] = self.part[me]

            def one(k):
                z = behind(k)
                along_cells(self.part.at[me], self.fromz.at[z], self.zs.at[z], self.zr.at[z], sibling).wait_recv()
                result[rows] = result[rows] + self.fromz[z]

            loop(1, a, one)

        def ended(self):
            loop(0, h, lambda t: self.over(t, t).wait_send())

            def sent_y(k):
                z, y = order(k)
                t = z * b + y
                along_cells(self.part.at[t], self.fromy.at[t], self.ys.at[t], self.yr.at[t], sibling).wait_send()

            loop(0, h - a, sent_y)

            def sent_z(k):
                z = lax.rem(zi + k, a)
                along_cells(self.part.at[z], self.fromz.at[z], self.zs.at[z], self.zr.at[z], sibling).wait_send()

            loop(1, a, sent_z)

    walk = Scatter(w, ra, rt, rz, (as_sem, ar_sem, bs_sem, br_sem, zs_sem, zr_sem))
    base = Scatter(wb, rab, rtb, rzb, (bas_sem, bar_sem, bbs_sem, bbr_sem, bzs_sem, bzr_sem))

    live_here = live[0]
    weights_row = jnp.where(
        lax.broadcasted_iota(jnp.int32, (1, cells), 1) < live_here, 1.0, 0.0
    ).astype(F32)
    weights = jnp.where(
        lax.broadcasted_iota(jnp.int32, (cells, LANES), 0) < live_here, 1.0, 0.0
    ).astype(F32)
    for table in (sl, mr, stack):
        table[...] = jnp.zeros_like(table)
    same = jnp.where(
        lax.broadcasted_iota(jnp.int32, (LANES, LANES), 0)
        == lax.broadcasted_iota(jnp.int32, (LANES, LANES), 1),
        1.0, 0.0,
    ).astype(F32)
    er[...] = same
    chg[...] = jnp.where(lane == row + SLOTS, 1.0, 0.0)

    def extend(table, first, second, position, against):
        here = jnp.where(lane == row + position, 1.0, 0.0).astype(F32)
        turn = lambda lhs, rhs: lax.dot_general(
            lhs, rhs, (((0,), (0,)), ((), ())), precision=HIGHEST, preferred_element_type=F32
        )
        table[...] = table[...] + turn(here, against) + turn(against, here)
        first[...], second[...] = both_sides(table[...], same)
    sl[0:BASIS] = left_basis[...] * weights_row
    sl[WEIGHT : WEIGHT + 8] = jnp.where(
        lax.broadcasted_iota(jnp.int32, (8, cells), 0) == 0, weights_row, 0.0
    )
    gram0[me, 0:BASIS] = exact_rows(sl[0:BASIS], sl[...])
    gram0[me, BASIS:] = exact_rows(sl[WEIGHT : WEIGHT + 8], sl[...])

    def take_log(d):
        for i in range(tiles):
            here = slice(i * LANES, (i + 1) * LANES)
            logged[d, :, here] = jnp.log(1.0 + cnt[d, :, here].astype(F32)) * weights

    for _, trio in loads:
        trio[0].wait()
    take_log(me)
    portion = 1.0 / jnp.maximum(live_here, 1).astype(F32)
    for i in range(tiles):
        here = slice(i * LANES, (i + 1) * LANES)
        mu[me, :, here] = jnp.sum(logged[me, :, here], axis=0, keepdims=True) * portion
    pl.semaphore_wait(barrier, n - 1 + g - 1)
    spread(along_cells, mu, me, n, ms_sem, mr_sem)
    spread(along_cells, gram0, me, n, g0s_sem, g0r_sem)
    loop(1, n, lambda k: take_log(lax.rem(me + k, n)))

    for _, trio in loads:
        trio[1].wait()
        trio[2].wait()
    xs0[mine] = jnp.zeros((BASIS + BLOCK, LANES), F32)
    xb0[mine] = jnp.zeros((BASIS, LANES), F32)
    xg[0, mine] = jnp.zeros((BLOCK, LANES), F32)

    def fill(d):
        high, low = split(rb[d])
        vhi[d, 0 : BASIS + BLOCK] = high
        vlo[d, 0 : BASIS + BLOCK] = low
        blank = jnp.zeros((LANES - BASIS - BLOCK, width), BF16)
        vhi[d, BASIS + BLOCK :] = blank
        vlo[d, BASIS + BLOCK :] = blank

    loop(0, n, fill)
    waited(along_cells, mu, me, n, ms_sem, mr_sem)

    bhigh, blow = split(jnp.concatenate(
        [sl[0:BASIS], sl[WEIGHT : WEIGHT + 8], jnp.zeros((8, cells), F32)], axis=0
    ))
    bboth = jnp.concatenate([bhigh, blow], axis=0)

    def center(d):
        for i in range(tiles):
            here = slice(i * LANES, (i + 1) * LANES)
            high, low = split(logged[d, :, here] - weights * mu[d, :, here])
            lhi[d, :, here] = high
            llo[d, :, here] = low
        made = product(bhigh, bboth, lhi[d], llo[d], ALONG)
        wb[d] = made[0:BASIS]
        tpart[d] = made[BASIS : BASIS + 1]

    base.launch(center)

    def give(k):
        d = lax.rem(me + k, n)
        along_cells(tpart.at[d], tfrom.at[me], ts_sem.at[k], tr_sem.at[me], d).start()

    loop(1, n, give)

    def cross(d):
        high = vhi[d, 0 : BASIS + BLOCK]
        both = jnp.concatenate([high, vlo[d, 0 : BASIS + BLOCK]], axis=0)
        met = product(high, both, lhi[d], llo[d], ROWS)
        xb0[mine] = xb0[mine] + met[0:BASIS]
        xg[0, mine] = xg[0, mine] + met[BASIS:]

    base.third(0, 1)
    loop(0, n, cross, 2)
    spread(along_genes, xg.at[0], mine, g, xs_sem.at[0], xr_sem.at[0])
    spread(along_genes, xb0, mine, g, b0s_sem, b0r_sem)
    base.third(1, 2)

    near = gathered(along_cells, gram0, me, n, g0s_sem, g0r_sem)
    corner = lax.broadcasted_iota(jnp.int32, (LANES, LANES), 0)
    across = lax.broadcasted_iota(jnp.int32, (BASIS, LANES), 1)
    el[...] = jnp.where((same > 0) & (corner >= BASIS), 1.0, 0.0)
    el[0:BASIS] = jnp.where(across < SLOTS, near[0:BASIS], 0.0)
    l1[...], l2[...] = both_sides(el[...], same)
    wsum[...] = near[BASIS:]
    live_total = near[BASIS : BASIS + 1, WEIGHT : WEIGHT + 1]
    inverse = 1.0 / live_total
    factor_scale = lax.rsqrt(live_total)
    factor_scale = factor_scale * (1.5 - 0.5 * live_total * factor_scale * factor_scale)

    def turned(column, start):
        return jnp.sum(jnp.where(lane == row + start, column, 0.0), axis=0, keepdims=True)

    def fresh(d):
        chigh, clow = split(chg[...])
        cboth = jnp.concatenate([chigh, clow], axis=0)
        return product(chigh, cboth, vhi[d], vlo[d], ALONG)

    def emit(d, rows, values):
        @pl.when(d < whole)
        def _():
            right_out[rows, pl.ds(pl.multiple_of(d * width, LANES), width)] = values * scales[1]

        if spare:
            @pl.when(d == whole)
            def _():
                right_out[rows, whole * width : genes] = values[:, :spare] * scales[1]

    def update(j, start, stop):
        later = pl.multiple_of(BASIS + (j + 1) * BLOCK, BLOCK)
        rows = pl.ds(pl.multiple_of(j * BLOCK, BLOCK), BLOCK)

        def right(d):
            values = fresh(d)
            vhigh, vlow = split(values)
            vhi[d, pl.ds(later, BLOCK)] = vhigh
            vlo[d, pl.ds(later, BLOCK)] = vlow
            emit(d, rows, values)

        loop(start, stop, right)

    def keep(d, values):
        phigh, plow = split(values)
        vhi[d, SLOTS : SLOTS + BLOCK] = phigh
        vlo[d, SLOTS : SLOTS + BLOCK] = plow
        return phigh, jnp.concatenate([phigh, plow], axis=0)

    def meet(d):
        high = vhi[d, 0 : BASIS + BLOCK]
        both = jnp.concatenate([high, vlo[d, 0 : BASIS + BLOCK]], axis=0)
        xs0[mine] = xs0[mine] + product(high, both, vhi[d], vlo[d], ROWS)

    def begin(j):
        @pl.when(j == 0)
        def _():
            base.third(2, a)
            walk.third(0, 2)

    def step(j, final):
        position = BASIS + j * BLOCK
        position = position if final else pl.multiple_of(position, BLOCK)
        mr[SLOTS : SLOTS + BLOCK] = gathered(along_genes, xg.at[j], mine, g, xs_sem.at[j], xr_sem.at[j])
        vectors = exact(chg[...], mr[...])
        mr[pl.ds(position, BLOCK)] = vectors
        sl[SLOTS : SLOTS + BLOCK] = vectors
        gram[me] = exact_rows(vectors, sl[...])
        spread(along_cells, gram, me, n, gs_sem, gr_sem)
        high, low = split(vectors)
        both = jnp.concatenate([high, low], axis=0)

        def produce(d):
            w[d] = product(high, both, lhi[d], llo[d], ALONG)

        walk.launch(produce)
        if final:
            update(j - 1, 0, n // 2)
            walk.third(0, 1)
            update(j - 1, n // 2, n)
            walk.third(1, 2)
        else:
            begin(j)

            @pl.when(j > 0)
            def _():
                update(j - 1, 0, n // 2)
                walk.third(0, 1)
                update(j - 1, n // 2, n)
                walk.third(1, 2)

        total = gathered(along_cells, gram, me, n, gs_sem, gr_sem)
        held = total[:, WEIGHT : WEIGHT + 1] * inverse
        weighed = wsum[0:1] + turned(total[:, WEIGHT : WEIGHT + 1], SLOTS)
        scale = jnp.where(lane < SLOTS, factor_scale, factor_scale * factor_scale)
        factor, against, change = orthonormal((total - held * weighed) * scale, l1[...], l2[...])
        diag_out[j] = factor
        tilt = jnp.sum(jnp.where(lane < SLOTS, change * wsum[0:1], 0.0), axis=1, keepdims=True)
        wsum[0:1] = wsum[0:1] + turned(tilt, position)
        shift = jnp.sum(
            jnp.where((lane >= SLOTS) & (lane < WEIGHT), change * turned(held, SLOTS), 0.0), axis=1, keepdims=True
        )
        blend = jnp.where(
            lane < SLOTS, change,
            jnp.where(lane < WEIGHT, change * factor_scale, jnp.where(lane == WEIGHT, -shift * factor_scale, 0.0)),
        )
        leftvec = exact(blend, sl[...])
        sl[pl.ds(position, BLOCK)] = leftvec
        left_out[pl.ds(position - BASIS, BLOCK)] = leftvec * scales[0]
        tilt = tilt * inverse
        blend = jnp.where(lane == WEIGHT, blend - tilt, blend) * factor_scale

        def settle():
            ground[...] = exact(jnp.where((lane < SLOTS) | (lane >= WEIGHT), blend, 0.0), stack[...])

        if final:
            settle()
        else:
            pl.when(j > 0)(settle)
        walk.third(2, a)
        if not final:
            @pl.when(j == 0)
            def _():
                base.fourth(stack, slice(0, BASIS))

                def take(k):
                    source = lax.rem(me + n - k, n)
                    item = along_cells(tpart.at[source], tfrom.at[source], ts_sem.at[k], tr_sem.at[source], sibling)
                    item.wait_send()
                    item.wait_recv()
                    tpart[me] = tpart[me] + tfrom[source]

                loop(1, n, take)
                stack[WEIGHT : WEIGHT + 1] = tpart[me]
                settle()
                mr[0:BASIS] = gathered(along_genes, xb0, mine, g, b0s_sem, b0r_sem)

        walk.fourth(stack, slice(SLOTS, SLOTS + BLOCK))
        columns = [blend[:, SLOTS + k : SLOTS + k + 1] for k in range(BLOCK)]
        for i in range(tiles):
            here = slice(i * LANES, (i + 1) * LANES)
            values = ground[:, here]
            for k in range(BLOCK):
                values = values + columns[k] * stack[SLOTS + k : SLOTS + k + 1, here]
            pb[me, :, here] = values

        def relay(z):
            t = z * b + yi
            d = 2 * t + core

            def to_y(k):
                y = lax.rem(yi + k, b)
                along_cells(pb.at[d], pb.at[d], fs_sem.at[z * b + y], cr_sem.at[d], 2 * (zi * b + y) + core).start()

            loop(1, b, to_y)
            along_cells(pb.at[d], pb.at[d], ds_sem.at[t], cr_sem.at[d], sibling).start()

        def arrived(d):
            along_cells(pb.at[d], pb.at[d], ds_sem.at[0], cr_sem.at[d], sibling).wait_recv()

        def go(k):
            z = onward(k)
            along_cells(pb.at[me], pb.at[me], cs_sem.at[z], cr_sem.at[me], 2 * (z * b + yi) + core).start()

        if not final:
            loop(1, min(2, a), go)
            relay(zi)
        phigh, pboth = keep(me, pb[me])
        gz[zi] = product(phigh, pboth, vhi[me], vlo[me], ROWS)
        spread(along_column, gz, zi, a, gzs_sem, gzr_sem)
        if final:
            loop(1, min(2, a), go)
            relay(zi)
        loop(min(2, a), a, go)
        if not final:
            stack[pl.ds(position, BLOCK)] = (
                pb[me] * (live_total * factor_scale) + tilt * stack[WEIGHT : WEIGHT + 1]
            )
            xg[j + 1, mine] = jnp.zeros((BLOCK, LANES), F32)
            extend(el, l1, l2, position, against)

        def consume(d):
            phigh, pboth = keep(d, pb[d])
            if final:
                emit(d, pl.ds((STEPS - 1) * BLOCK, BLOCK), fresh(d))
            else:
                xg[j + 1, mine] = xg[j + 1, mine] + product(phigh, pboth, lhi[d], llo[d], ROWS)

        def pass_z(k):
            z = behind(k)
            arrived(2 * (z * b + yi) + core)
            relay(z)

        seat = 2 * yi + core
        def quarter(q):
            if not final:
                pl.when(j == 0)(lambda: loop(q * n // 4, (q + 1) * n // 4, meet))

        quarter(0)
        loop(1, min(2, a), pass_z)
        quarter(1)
        if not final:
            loop(min(2, a), min(3, a), pass_z)
        gx[mine] = gathered(along_column, gz, zi, a, gzs_sem, gzr_sem)
        spread(along_genes, gx, mine, g, gxs_sem, gxr_sem)
        if final:
            loop(min(2, a), min(3, a), pass_z)
        quarter(2)
        loop(min(3, a), a, pass_z)
        quarter(3)
        if not final:
            pl.when(j == 0)(lambda: spread(along_genes, xs0, mine, g, s0s_sem, s0r_sem))

        def plane():
            gy[seat] = gathered(along_genes, gx, mine, g, gxs_sem, gxr_sem)
            spread(along_plane, gy, seat, 2 * b, gys_sem, gyr_sem)

        def open_right():
            met = gathered(along_genes, xs0, mine, g, s0s_sem, s0r_sem)
            held = lax.broadcasted_iota(jnp.int32, met.shape, 1) < SLOTS
            er[0 : BASIS + BLOCK] = jnp.where(held, met, 0.0)
            r1[...], r2[...] = both_sides(er[...], same)

        def close():
            if not final:
                pl.when(j == 0)(open_right)
            total = gathered(along_plane, gy, seat, 2 * b, gys_sem, gyr_sem)
            factor, against, change = orthonormal(total, r1[...], r2[...])
            couple_out[j] = factor
            chg[...] = change
            if not final:
                extend(er, r1, r2, position + BLOCK, against)

        if final:
            plane()
            close()
        consume(me)
        loop(1, a, lambda k: consume(2 * (behind(k) * b + yi) + core))

        def pass_y(k):
            z = behind(lax.rem(k, a))
            t = z * b + lax.rem(yi + 1 + k // a, b)
            d = 2 * t + core
            arrived(d)
            along_cells(pb.at[d], pb.at[d], ds_sem.at[t], cr_sem.at[d], sibling).start()
            consume(d)

        def rest(k):
            z = behind(lax.rem(k, a))
            t = z * b + lax.rem(yi + k // a, b)
            d = 2 * t + 1 - core
            arrived(d)
            consume(d)

        if not final:
            plane()
        loop(0, a, rest)
        loop(0, h - a, pass_y)

        loop(a, h, rest)
        if not final:
            spread(along_genes, xg.at[j + 1], mine, g, xs_sem.at[j + 1], xr_sem.at[j + 1])
            close()
        walk.ended()

        def ended(t):
            along_cells(pb.at[t], pb.at[t], ds_sem.at[t], cr_sem.at[t], sibling).wait_send()

        loop(0, h, ended)

        def ended_y(k):
            z, y = order(k)
            t = z * b + y
            along_cells(pb.at[t], pb.at[t], fs_sem.at[t], cr_sem.at[t], sibling).wait_send()

        loop(0, h - a, ended_y)

        def ended_z(k):
            z = lax.rem(zi + k, a)
            along_cells(pb.at[z], pb.at[z], cs_sem.at[z], cr_sem.at[z], sibling).wait_send()

        loop(1, a, ended_z)

    loop(0, STEPS - 1, lambda j: step(j, False))
    step(STEPS - 1, True)
    base.ended()


def body(counts, live_rows, left_basis, right_basis, right_start):
    cells, genes = counts.shape
    n = lax.axis_size("cells")
    g = lax.axis_size("genes")
    h = n // 2
    width = -(-(genes // LANES) // n) * LANES
    scales = (math.sqrt(float(cells * n)), math.sqrt(float(genes * g)))
    vmem = pl.BlockSpec(memory_space=pltpu.VMEM)
    anywhere = pl.BlockSpec(memory_space=pl.ANY)
    held = lambda *shape: pltpu.VMEM(shape, F32)
    square = held(LANES, LANES)
    dma = lambda *shape: pltpu.SemaphoreType.DMA(shape)
    out_shape = (
        jax.ShapeDtypeStruct((STEPS * BLOCK, cells), F32),
        jax.ShapeDtypeStruct((STEPS * BLOCK, genes), F32),
        jax.ShapeDtypeStruct((STEPS, BLOCK, BLOCK), F32),
        jax.ShapeDtypeStruct((STEPS, BLOCK, BLOCK), F32),
    )
    buffers = lambda rows: [
        held(n, rows, width), held(h, rows, width), held(h, rows, width), held(h, rows, width),
    ]
    scratch = [
        pltpu.VMEM((n, cells, width), jnp.int32),
        held(n, cells, width),
        *[pltpu.VMEM((n, cells, width), BF16)] * 2,
        *[pltpu.VMEM((n, LANES, width), BF16)] * 2,
        held(n, BASIS + BLOCK, width),
        *[square] * 8,
        *buffers(BLOCK),
        *buffers(BASIS),
        held(n, BLOCK, width),
        held(LANES, width),
        held(BLOCK, width),
        held(n, 1, width),
        held(n, 1, width),
        held(n, 1, width),
        held(8, LANES),
        held(BLOCK, LANES),
        held(n, BASIS + 8, LANES),
        held(n, BLOCK, LANES),
        held(g, BASIS + BLOCK, LANES),
        held(g, BASIS, LANES),
        held(STEPS, g, BLOCK, LANES),
        held(g, BLOCK, LANES),
        held(n, BLOCK, LANES),
        held(h, BLOCK, LANES),
        dma(n, 3),
        *[dma(h)] * 6,
        *[dma(h)] * 6,
        dma(h), dma(n), dma(h), dma(h), dma(n), dma(n),
        *[dma(n)] * 6,
        *[dma(g)] * 4,
        dma(STEPS, g), dma(STEPS, g),
        dma(g), dma(g), dma(n), dma(n), dma(h), dma(h),
    ]
    return pl.pallas_call(
        functools.partial(kernel, n, g, width, scales),
        out_shape=out_shape,
        in_specs=[pl.BlockSpec(memory_space=pltpu.SMEM), anywhere, vmem, anywhere, anywhere],
        out_specs=(vmem, vmem, vmem, vmem),
        scratch_shapes=scratch,
        compiler_params=pltpu.CompilerParams(
            collective_id=0, has_side_effects=True, vmem_limit_bytes=66 * 1000 * 1000
        ),
    )(live_rows, counts, left_basis, right_basis, right_start)


def solution(mesh):
    in_specs = (
        P("cells", "genes"),
        P("cells"),
        P(None, "cells"),
        P(None, "genes"),
        P(None, "genes"),
    )
    out_specs = (P(None, "cells"), P(None, "genes"), P(), P())
    return jax.shard_map(body, mesh=mesh, in_specs=in_specs, out_specs=out_specs, check_vma=False)
```

```python
import functools
import math

import jax
import jax.numpy as jnp
from jax import lax
from jax.experimental import pallas as pl
from jax.experimental.pallas import tpu as pltpu
from jax.sharding import PartitionSpec as P

BASIS = 32
BLOCK = 16
STEPS = 3
SLOTS = BASIS + STEPS * BLOCK
WEIGHT = SLOTS + BLOCK
LAG = 2
LANES = 128
F32 = jnp.float32
BF16 = jnp.bfloat16
HIGHEST = lax.Precision.HIGHEST
MESH = pl.DeviceIdType.MESH


def exact(lhs, rhs):
    return jnp.dot(lhs, rhs, precision=HIGHEST, preferred_element_type=F32)


def exact_rows(lhs, rhs):
    return lax.dot_general(
        lhs, rhs, (((1,), (1,)), ((), ())), precision=HIGHEST, preferred_element_type=F32
    )


def split(values):
    high = values.astype(BF16)
    return high, (values - high.astype(F32)).astype(BF16)


def product(high, both, rhs_high, rhs_low, dims):
    rows = high.shape[0]
    first = lax.dot_general(both, rhs_high, (dims, ((), ())), preferred_element_type=F32)
    second = lax.dot_general(high, rhs_low, (dims, ((), ())), preferred_element_type=F32)
    return first[:rows] + (first[rows:] + second)


ALONG = ((1,), (0,))
ROWS = ((1,), (1,))


def loop(start, stop, step, unroll=1):
    def one(k, carry):
        step(k)
        return carry

    lax.fori_loop(start, stop, one, 0, unroll=unroll if (stop - start) % unroll == 0 else 1)


def both_sides(gram, identity):
    gap = identity - gram
    return identity + gap, exact(gap, gap)


def orthonormal(gram, first, second):
    lane = lax.broadcasted_iota(jnp.int32, (BLOCK, LANES), 1)
    row = lax.broadcasted_iota(jnp.int32, (BLOCK, LANES), 0)
    coeffs = jnp.where(lane < SLOTS, gram, 0.0)
    combined = exact(coeffs, first)
    residue = exact(coeffs, second)
    squares = gram[:, SLOTS : SLOTS + BLOCK] - exact_rows(
        jnp.concatenate([combined, residue], axis=1), jnp.concatenate([coeffs, combined], axis=1)
    )
    change = jnp.where(lane == row + SLOTS, 1.0, -combined)
    columns = [jnp.broadcast_to(squares[:, k : k + 1], (BLOCK, LANES)) for k in range(BLOCK)]
    factor = jnp.zeros((BLOCK, LANES), F32)
    for k in range(BLOCK):
        pivot = jnp.broadcast_to(columns[k][k : k + 1], (BLOCK, LANES))
        root = lax.rsqrt(pivot)
        root = root * (1.5 - 0.5 * pivot * root * root)
        column = columns[k] * root
        factor = jnp.where((lane == k) & (row >= k), column, factor)
        below = jnp.where(row > k, column, 0.0)
        for i in range(k + 1, BLOCK):
            columns[i] = columns[i] - column * jnp.broadcast_to(column[i : i + 1], (BLOCK, LANES))
        scaled = jnp.broadcast_to(residue[k : k + 1], (BLOCK, LANES)) * root
        residue = jnp.where(row == k, scaled, residue - below * scaled)
        scaled = jnp.broadcast_to(change[k : k + 1], (BLOCK, LANES)) * root
        change = jnp.where(row == k, scaled, change - below * scaled)
    return factor[:, :BLOCK], residue, change


def chunks(n, genes):
    brief, extra = divmod(genes // LANES, n)
    stride = n // extra if extra else n
    return brief, [i * stride + (2 * (i % 2) if stride > 3 else 0) for i in range(extra)]


def kernel(
    n, g, width, scales,
    live, counts, left_basis, right_basis, right_start,
    left_out, right_hbm, diag_out, couple_out,
    right_out, cnt, logged, lhi, llo, vhi, vlo, rb, sl, mr, el, er, l1, l2, r1, r2,
    w, ra, rt, rz, wb, rab, rtb, rzb, pb, stack, ground, tpart, tfrom,
    mu, wsum, chg, gram0, gram, xs0, xb0, xg, gx, gy, gz,
    in_sem, as_sem, ar_sem, bs_sem, br_sem, zs_sem, zr_sem,
    bas_sem, bar_sem, bbs_sem, bbr_sem, bzs_sem, bzr_sem,
    cs_sem, cr_sem, ds_sem, fs_sem, ts_sem, tr_sem,
    ms_sem, mr_sem, g0s_sem, g0r_sem, gs_sem, gr_sem, s0s_sem, s0r_sem, b0s_sem, b0r_sem,
    xs_sem, xr_sem, gxs_sem, gxr_sem, gys_sem, gyr_sem, gzs_sem, gzr_sem, out_sem, tail_sem,
):
    cells, genes = counts.shape
    me = lax.axis_index("cells")
    mine = lax.axis_index("genes")
    core = lax.rem(me, 2)
    chip = me // 2
    h = n // 2
    b = 1 << ((h.bit_length() - 1) // 2)
    b = b if h % b == 0 else 1
    a = h // b
    zi, yi = chip // b, lax.rem(chip, b)
    sibling = me + 1 - 2 * core
    tiles = width // LANES
    brief, longs = chunks(n, genes)
    brief = brief * LANES
    lane = lax.broadcasted_iota(jnp.int32, (BLOCK, LANES), 1)
    row = lax.broadcasted_iota(jnp.int32, (BLOCK, LANES), 0)

    def along_cells(src, dst, send, recv, peer):
        return pltpu.make_async_remote_copy(
            src_ref=src, dst_ref=dst, send_sem=send, recv_sem=recv,
            device_id=(peer, mine), device_id_type=MESH,
        )

    def along_genes(src, dst, send, recv, peer):
        return pltpu.make_async_remote_copy(
            src_ref=src, dst_ref=dst, send_sem=send, recv_sem=recv,
            device_id=(me, peer), device_id_type=MESH,
        )

    def along_plane(src, dst, send, recv, peer):
        return along_cells(src, dst, send, recv, 2 * b * zi + peer)

    def along_column(src, dst, send, recv, peer):
        return along_cells(src, dst, send, recv, 2 * (peer * b + yi) + core)

    def is_long(d):
        found = d == longs[0]
        for other in longs[1:]:
            found = found | (d == other)
        return found

    def first_gene(d):
        at = d * brief
        for other in longs:
            at = at + jnp.where(d > other, LANES, 0)
        return pl.multiple_of(at, LANES)

    def fill_in(d, kind, method):
        here, there, rows = (
            (counts, cnt, pl.ds(0, cells)), (right_basis, rb, pl.ds(0, BASIS)), (right_start, rb, pl.ds(BASIS, BLOCK)),
        )[kind]
        at = first_gene(d)
        getattr(pltpu.make_async_copy(
            here.at[:, pl.ds(at, brief)], there.at[d, rows, pl.ds(0, brief)], in_sem.at[d, kind, 0]
        ), method)()
        if longs:
            @pl.when(is_long(d))
            def _():
                getattr(pltpu.make_async_copy(
                    here.at[:, pl.ds(pl.multiple_of(at + brief, LANES), LANES)],
                    there.at[d, rows, pl.ds(brief, LANES)], in_sem.at[d, kind, 1],
                ), method)()

    def hop(src, dst, send, recv, peer, d):
        def act(method):
            getattr(along_cells(
                src.at[:, pl.ds(0, brief)], dst.at[:, pl.ds(0, brief)],
                send[0].at[0, send[1]], recv[0].at[0, recv[1]], peer,
            ), method)()
            if longs:
                @pl.when(is_long(d))
                def _():
                    getattr(along_cells(
                        src.at[:, pl.ds(brief, LANES)], dst.at[:, pl.ds(brief, LANES)],
                        send[0].at[1, send[1]], recv[0].at[1, recv[1]], peer,
                    ), method)()

        return act

    def around(k):
        return lax.rem(me + k, n)

    loop(0, n, lambda k: fill_in(around(k), 0, "start"))

    def more(k):
        fill_in(around(k), 1, "start")
        fill_in(around(k), 2, "start")

    loop(0, n, more)
    if longs:
        for d in range(n):
            if d not in longs:
                cnt[d, :, brief:] = jnp.zeros((cells, LANES), jnp.int32)
                rb[d, :, brief:] = jnp.zeros((BASIS + BLOCK, LANES), F32)
        for table in (ra, rt, rz, rab, rtb, rzb, pb):
            table[:, :, brief:] = jnp.zeros((table.shape[0], table.shape[1], LANES), F32)

    barrier = pltpu.get_barrier_semaphore()

    def greet_cells(k):
        pl.semaphore_signal(barrier, inc=1, device_id=(lax.rem(me + k, n), mine), device_id_type=MESH)

    def greet_genes(k):
        pl.semaphore_signal(barrier, inc=1, device_id=(me, lax.rem(mine + k, g)), device_id_type=MESH)

    loop(1, n, greet_cells)
    loop(1, g, greet_genes)

    def spread(copy, buf, at, size, send, recv):
        def go(k):
            copy(buf.at[at], buf.at[at], send.at[k], recv.at[at], lax.rem(at + k, size)).start()

        loop(1, size, go)

    def waited(copy, buf, at, size, send, recv):
        def end(k):
            source = lax.rem(at + size - k, size)
            item = copy(buf.at[source], buf.at[source], send.at[k], recv.at[source], lax.rem(at + k, size))
            item.wait_send()
            item.wait_recv()

        loop(1, size, end)

    def gathered(copy, buf, at, size, send, recv):
        waited(copy, buf, at, size, send, recv)
        return lax.fori_loop(
            1, size, lambda k, total: total + buf[k], buf[0]
        )

    def onward(k):
        return lax.rem(zi + k, a)

    def behind(k):
        return lax.rem(zi + a - k, a)

    def order(k):
        return onward(1 + lax.rem(k, a)), lax.rem(yi + 1 + k // a, b)

    class Scatter:
        def __init__(self, part, fromcore, fromy, fromz, sems):
            self.part, self.fromcore, self.fromy, self.fromz = part, fromcore, fromy, fromz
            self.cs, self.cr, self.ys, self.yr, self.zs, self.zr = sems

        def over(self, d, t):
            return hop(self.part.at[d], self.fromcore.at[t], (self.cs, t), (self.cr, t), sibling, d)

        def launch(self, produce):
            def other(k):
                z, y = order(k)
                t = z * b + y
                return t, 2 * t + 1 - core

            def own(k):
                z, y = order(k)
                t = z * b + y
                return z, y, t, 2 * t + core

            def join(k):
                z, y, t, d = own(k)
                self.over(d, t)("wait_recv")
                self.part[d] = self.part[d] + self.fromcore[t]

                @pl.when(k < h - a)
                def _():
                    to = z * b + yi
                    hop(
                        self.part.at[d], self.fromy.at[to], (self.ys, t), (self.yr, to),
                        2 * (zi * b + y) + core, d,
                    )("start")

            def pair(k):
                t, d = other(k)
                produce(d)
                produce(own(k)[3])
                self.over(d, t)("start")

            def one(k):
                pair(k)
                join(k - LAG)

            loop(0, LAG, pair)
            loop(LAG, h, one)
            loop(h - LAG, h, join)

        def complete(self, z):
            d = 2 * (z * b + yi) + core

            def add(k):
                source = z * b + lax.rem(yi + k, b)
                hop(self.part.at[d], self.fromy.at[source], (self.ys, source), (self.yr, source), sibling, d)("wait_recv")
                self.part[d] = self.part[d] + self.fromy[source]

            loop(1, b, add)
            return d

        def third(self, start, stop):
            def one(k):
                z = onward(1 + k)
                d = self.complete(z)
                hop(self.part.at[d], self.fromz.at[zi], (self.zs, z), (self.zr, zi), d, d)("start")

            loop(min(start, a - 1), min(stop, a - 1), one)
            if stop >= a:
                self.complete(zi)

        def fourth(self, result, rows):
            result[rows] = self.part[me]

            def one(k):
                z = behind(k)
                hop(self.part.at[me], self.fromz.at[z], (self.zs, z), (self.zr, z), sibling, me)("wait_recv")
                result[rows] = result[rows] + self.fromz[z]

            loop(1, a, one)

        def ended(self):
            loop(0, h, lambda t: self.over(2 * t + 1 - core, t)("wait_send"))

            def sent_y(k):
                z, y = order(k)
                t = z * b + y
                hop(self.part.at[t], self.fromy.at[t], (self.ys, t), (self.yr, t), sibling, 2 * t + core)("wait_send")

            loop(0, h - a, sent_y)

            def sent_z(k):
                z = lax.rem(zi + k, a)
                d = 2 * (z * b + yi) + core
                hop(self.part.at[z], self.fromz.at[z], (self.zs, z), (self.zr, z), sibling, d)("wait_send")

            loop(1, a, sent_z)

    walk = Scatter(w, ra, rt, rz, (as_sem, ar_sem, bs_sem, br_sem, zs_sem, zr_sem))
    base = Scatter(wb, rab, rtb, rzb, (bas_sem, bar_sem, bbs_sem, bbr_sem, bzs_sem, bzr_sem))

    live_here = live[0]
    weights_row = jnp.where(
        lax.broadcasted_iota(jnp.int32, (1, cells), 1) < live_here, 1.0, 0.0
    ).astype(F32)
    weights = jnp.where(
        lax.broadcasted_iota(jnp.int32, (cells, LANES), 0) < live_here, 1.0, 0.0
    ).astype(F32)
    for table in (sl, mr, stack):
        table[...] = jnp.zeros_like(table)
    same = jnp.where(
        lax.broadcasted_iota(jnp.int32, (LANES, LANES), 0)
        == lax.broadcasted_iota(jnp.int32, (LANES, LANES), 1),
        1.0, 0.0,
    ).astype(F32)
    er[...] = same
    chg[...] = jnp.where(lane == row + SLOTS, 1.0, 0.0)

    def extend(table, first, second, position, against):
        here = jnp.where(lane == row + position, 1.0, 0.0).astype(F32)
        turn = lambda lhs, rhs: lax.dot_general(
            lhs, rhs, (((0,), (0,)), ((), ())), precision=HIGHEST, preferred_element_type=F32
        )
        table[...] = table[...] + turn(here, against) + turn(against, here)
        first[...], second[...] = both_sides(table[...], same)
    sl[0:BASIS] = left_basis[...] * weights_row
    sl[WEIGHT : WEIGHT + 8] = jnp.where(
        lax.broadcasted_iota(jnp.int32, (8, cells), 0) == 0, weights_row, 0.0
    )
    gram0[me, 0:BASIS] = exact_rows(sl[0:BASIS], sl[...])
    gram0[me, BASIS:] = exact_rows(sl[WEIGHT : WEIGHT + 8], sl[...])

    def take_log(d):
        for i in range(tiles):
            here = slice(i * LANES, (i + 1) * LANES)
            logged[d, :, here] = jnp.log(1.0 + cnt[d, :, here].astype(F32)) * weights

    fill_in(me, 0, "wait")
    take_log(me)
    portion = 1.0 / jnp.maximum(live_here, 1).astype(F32)
    for i in range(tiles):
        here = slice(i * LANES, (i + 1) * LANES)
        mu[me, :, here] = jnp.sum(logged[me, :, here], axis=0, keepdims=True) * portion
    pl.semaphore_wait(barrier, n - 1 + g - 1)
    spread(along_cells, mu, me, n, ms_sem, mr_sem)
    spread(along_cells, gram0, me, n, g0s_sem, g0r_sem)

    def next_log(k):
        fill_in(around(k), 0, "wait")
        take_log(around(k))

    loop(1, n, next_log)
    xs0[mine] = jnp.zeros((BASIS + BLOCK, LANES), F32)
    xb0[mine] = jnp.zeros((BASIS, LANES), F32)
    xg[0, mine] = jnp.zeros((BLOCK, LANES), F32)

    def fill(k):
        d = around(k)
        fill_in(d, 1, "wait")
        fill_in(d, 2, "wait")
        high, low = split(rb[d])
        vhi[d, 0 : BASIS + BLOCK] = high
        vlo[d, 0 : BASIS + BLOCK] = low
        blank = jnp.zeros((LANES - BASIS - BLOCK, width), BF16)
        vhi[d, BASIS + BLOCK :] = blank
        vlo[d, BASIS + BLOCK :] = blank

    loop(0, n, fill)
    waited(along_cells, mu, me, n, ms_sem, mr_sem)

    bhigh, blow = split(jnp.concatenate(
        [sl[0:BASIS], sl[WEIGHT : WEIGHT + 8], jnp.zeros((8, cells), F32)], axis=0
    ))
    bboth = jnp.concatenate([bhigh, blow], axis=0)

    def center(d):
        for i in range(tiles):
            here = slice(i * LANES, (i + 1) * LANES)
            high, low = split(logged[d, :, here] - weights * mu[d, :, here])
            lhi[d, :, here] = high
            llo[d, :, here] = low
        made = product(bhigh, bboth, lhi[d], llo[d], ALONG)
        wb[d] = made[0:BASIS]
        tpart[d] = made[BASIS : BASIS + 1]

    base.launch(center)

    def give(k):
        d = lax.rem(me + k, n)
        along_cells(tpart.at[d], tfrom.at[me], ts_sem.at[k], tr_sem.at[me], d).start()

    loop(1, n, give)

    def cross(d):
        high = vhi[d, 0 : BASIS + BLOCK]
        both = jnp.concatenate([high, vlo[d, 0 : BASIS + BLOCK]], axis=0)
        met = product(high, both, lhi[d], llo[d], ROWS)
        xb0[mine] = xb0[mine] + met[0:BASIS]
        xg[0, mine] = xg[0, mine] + met[BASIS:]

    base.third(0, 1)
    loop(0, n, cross, 2)
    spread(along_genes, xg.at[0], mine, g, xs_sem.at[0], xr_sem.at[0])
    spread(along_genes, xb0, mine, g, b0s_sem, b0r_sem)
    base.third(1, 2)

    near = gathered(along_cells, gram0, me, n, g0s_sem, g0r_sem)
    corner = lax.broadcasted_iota(jnp.int32, (LANES, LANES), 0)
    across = lax.broadcasted_iota(jnp.int32, (BASIS, LANES), 1)
    el[...] = jnp.where((same > 0) & (corner >= BASIS), 1.0, 0.0)
    el[0:BASIS] = jnp.where(across < SLOTS, near[0:BASIS], 0.0)
    l1[...], l2[...] = both_sides(el[...], same)
    wsum[...] = near[BASIS:]
    live_total = near[BASIS : BASIS + 1, WEIGHT : WEIGHT + 1]
    inverse = 1.0 / live_total
    factor_scale = lax.rsqrt(live_total)
    factor_scale = factor_scale * (1.5 - 0.5 * live_total * factor_scale * factor_scale)

    def turned(column, start):
        return jnp.sum(jnp.where(lane == row + start, column, 0.0), axis=0, keepdims=True)

    def fresh(d):
        chigh, clow = split(chg[...])
        cboth = jnp.concatenate([chigh, clow], axis=0)
        return product(chigh, cboth, vhi[d], vlo[d], ALONG)

    def emit(d, rows, values):
        values = values * scales[1]
        at = first_gene(d)
        right_out[rows, pl.ds(at, brief)] = values[:, :brief]
        if longs:
            @pl.when(is_long(d))
            def _():
                right_out[rows, pl.ds(pl.multiple_of(at + brief, LANES), LANES)] = values[:, brief:]

    def shipped(d, method):
        rows = pl.ds((STEPS - 1) * BLOCK, BLOCK)
        at = first_gene(d)

        def act(start, size, which):
            here = pl.ds(start, size)
            getattr(pltpu.make_async_copy(
                right_out.at[rows, here], right_hbm.at[rows, here], tail_sem.at[d, which]
            ), method)()

        act(at, brief, 0)
        if longs:
            pl.when(is_long(d))(lambda: act(pl.multiple_of(at + brief, LANES), LANES, 1))

    def block(j):
        rows = pl.ds(j * BLOCK if isinstance(j, int) else pl.multiple_of(j * BLOCK, BLOCK), BLOCK)
        return pltpu.make_async_copy(right_out.at[rows], right_hbm.at[rows], out_sem.at[j])

    def update(j, start, stop):
        later = pl.multiple_of(BASIS + (j + 1) * BLOCK, BLOCK)
        rows = pl.ds(pl.multiple_of(j * BLOCK, BLOCK), BLOCK)

        def right(d):
            values = fresh(d)
            vhigh, vlow = split(values)
            vhi[d, pl.ds(later, BLOCK)] = vhigh
            vlo[d, pl.ds(later, BLOCK)] = vlow
            emit(d, rows, values)

        loop(start, stop, right)

    def keep(d, values):
        phigh, plow = split(values)
        vhi[d, SLOTS : SLOTS + BLOCK] = phigh
        vlo[d, SLOTS : SLOTS + BLOCK] = plow
        return phigh, jnp.concatenate([phigh, plow], axis=0)

    def meet(d):
        high = vhi[d, 0 : BASIS + BLOCK]
        both = jnp.concatenate([high, vlo[d, 0 : BASIS + BLOCK]], axis=0)
        xs0[mine] = xs0[mine] + product(high, both, vhi[d], vlo[d], ROWS)

    def begin(j):
        @pl.when(j == 0)
        def _():
            base.third(2, a)
            walk.third(0, 2)

    def step(j, final):
        position = BASIS + j * BLOCK
        position = position if final else pl.multiple_of(position, BLOCK)
        mr[SLOTS : SLOTS + BLOCK] = gathered(along_genes, xg.at[j], mine, g, xs_sem.at[j], xr_sem.at[j])
        vectors = exact(chg[...], mr[...])
        mr[pl.ds(position, BLOCK)] = vectors
        sl[SLOTS : SLOTS + BLOCK] = vectors
        gram[me] = exact_rows(vectors, sl[...])
        spread(along_cells, gram, me, n, gs_sem, gr_sem)
        high, low = split(vectors)
        both = jnp.concatenate([high, low], axis=0)

        def produce(d):
            w[d] = product(high, both, lhi[d], llo[d], ALONG)

        walk.launch(produce)
        if final:
            update(j - 1, 0, n // 2)
            walk.third(0, 1)
            update(j - 1, n // 2, n)
            block(j - 1).start()
            walk.third(1, 2)
        else:
            begin(j)

            @pl.when(j > 0)
            def _():
                update(j - 1, 0, n // 2)
                walk.third(0, 1)
                update(j - 1, n // 2, n)
                block(j - 1).start()
                walk.third(1, 2)

        total = gathered(along_cells, gram, me, n, gs_sem, gr_sem)
        held = total[:, WEIGHT : WEIGHT + 1] * inverse
        weighed = wsum[0:1] + turned(total[:, WEIGHT : WEIGHT + 1], SLOTS)
        scale = jnp.where(lane < SLOTS, factor_scale, factor_scale * factor_scale)
        factor, against, change = orthonormal((total - held * weighed) * scale, l1[...], l2[...])
        walk.third(2, a - 1)
        diag_out[j] = factor
        tilt = jnp.sum(jnp.where(lane < SLOTS, change * wsum[0:1], 0.0), axis=1, keepdims=True)
        wsum[0:1] = wsum[0:1] + turned(tilt, position)
        shift = jnp.sum(
            jnp.where((lane >= SLOTS) & (lane < WEIGHT), change * turned(held, SLOTS), 0.0), axis=1, keepdims=True
        )
        blend = jnp.where(
            lane < SLOTS, change,
            jnp.where(lane < WEIGHT, change * factor_scale, jnp.where(lane == WEIGHT, -shift * factor_scale, 0.0)),
        )
        leftvec = exact(blend, sl[...])
        sl[pl.ds(position, BLOCK)] = leftvec
        left_out[pl.ds(position - BASIS, BLOCK)] = leftvec * scales[0]
        tilt = tilt * inverse
        blend = jnp.where(lane == WEIGHT, blend - tilt, blend) * factor_scale

        def settle():
            ground[...] = exact(jnp.where((lane < SLOTS) | (lane >= WEIGHT), blend, 0.0), stack[...])

        if final:
            settle()
        else:
            pl.when(j > 0)(settle)
        walk.third(a - 1, a)
        if not final:
            @pl.when(j == 0)
            def _():
                base.fourth(stack, slice(0, BASIS))

                def take(k):
                    source = lax.rem(me + n - k, n)
                    item = along_cells(tpart.at[source], tfrom.at[source], ts_sem.at[k], tr_sem.at[source], sibling)
                    item.wait_send()
                    item.wait_recv()
                    tpart[me] = tpart[me] + tfrom[source]

                loop(1, n, take)
                stack[WEIGHT : WEIGHT + 1] = tpart[me]
                settle()
                mr[0:BASIS] = gathered(along_genes, xb0, mine, g, b0s_sem, b0r_sem)

        walk.fourth(stack, slice(SLOTS, SLOTS + BLOCK))
        columns = [blend[:, SLOTS + k : SLOTS + k + 1] for k in range(BLOCK)]
        for i in range(tiles):
            here = slice(i * LANES, (i + 1) * LANES)
            values = ground[:, here]
            for k in range(BLOCK):
                values = values + columns[k] * stack[SLOTS + k : SLOTS + k + 1, here]
            pb[me, :, here] = values

        def relay(z):
            t = z * b + yi
            d = 2 * t + core

            def to_y(k):
                y = lax.rem(yi + k, b)
                hop(pb.at[d], pb.at[d], (fs_sem, z * b + y), (cr_sem, d), 2 * (zi * b + y) + core, d)("start")

            loop(1, b, to_y)
            hop(pb.at[d], pb.at[d], (ds_sem, t), (cr_sem, d), sibling, d)("start")

        def arrived(d):
            hop(pb.at[d], pb.at[d], (ds_sem, 0), (cr_sem, d), sibling, d)("wait_recv")

        def go(k):
            z = onward(k)
            hop(pb.at[me], pb.at[me], (cs_sem, z), (cr_sem, me), 2 * (z * b + yi) + core, me)("start")

        seat = 2 * yi + core
        late = max(a - 1, 1)
        if not final:
            loop(1, a, go)
            relay(zi)
        phigh, pboth = keep(me, pb[me])
        gy[seat] = product(phigh, pboth, vhi[me], vlo[me], ROWS)
        spread(along_plane, gy, seat, 2 * b, gys_sem, gyr_sem)
        if final:
            relay(zi)
            loop(1, late, go)
        else:
            stack[pl.ds(position, BLOCK)] = (
                pb[me] * (live_total * factor_scale) + tilt * stack[WEIGHT : WEIGHT + 1]
            )
            xg[j + 1, mine] = jnp.zeros((BLOCK, LANES), F32)
            extend(el, l1, l2, position, against)

        def consume(d):
            phigh, pboth = keep(d, pb[d])
            if final:
                emit(d, pl.ds((STEPS - 1) * BLOCK, BLOCK), fresh(d))
                shipped(d, "start")
            else:
                xg[j + 1, mine] = xg[j + 1, mine] + product(phigh, pboth, lhi[d], llo[d], ROWS)

        def pass_z(k):
            z = behind(k)
            arrived(2 * (z * b + yi) + core)
            relay(z)

        def quarter(q):
            if not final:
                pl.when(j == 0)(lambda: loop(q * n // 4, (q + 1) * n // 4, meet))

        def own(k):
            consume(2 * (behind(k) * b + yi) + core)

        def pass_y(k):
            z = behind(lax.rem(k, a))
            t = z * b + lax.rem(yi + 1 + k // a, b)
            d = 2 * t + core
            arrived(d)
            hop(pb.at[d], pb.at[d], (ds_sem, t), (cr_sem, d), sibling, d)("start")
            consume(d)

        def rest(k):
            z = behind(lax.rem(k, a))
            t = z * b + lax.rem(yi + k // a, b)
            d = 2 * t + 1 - core
            arrived(d)
            consume(d)

        def early(k):
            if not final:
                own(k)
                rest(k - 1)

        def ahead():
            gx[mine] = gathered(along_plane, gy, seat, 2 * b, gys_sem, gyr_sem)
            spread(along_genes, gx, mine, g, gxs_sem, gxr_sem)

        if final:
            ahead()
        else:
            consume(me)
        quarter(0)
        loop(1, min(2, a), pass_z)
        if not final:
            ahead()
        loop(1, min(2, a), early)
        quarter(1)
        if not final:
            loop(min(2, a), min(3, a), pass_z)
        gz[zi] = gathered(along_genes, gx, mine, g, gxs_sem, gxr_sem)
        spread(along_column, gz, zi, a, gzs_sem, gzr_sem)
        if final:
            loop(late, a, go)
            loop(min(2, a), min(3, a), pass_z)
        loop(min(2, a), min(3, a), early)
        met = min(1, h - a)
        if not final:
            loop(0, met, pass_y)
        quarter(2)

        def follow(k):
            pass_z(k)
            early(k)

        loop(min(3, a), a, follow)
        quarter(3)
        if not final:
            pl.when(j == 0)(lambda: spread(along_genes, xs0, mine, g, s0s_sem, s0r_sem))

        def open_right():
            met = gathered(along_genes, xs0, mine, g, s0s_sem, s0r_sem)
            held = lax.broadcasted_iota(jnp.int32, met.shape, 1) < SLOTS
            er[0 : BASIS + BLOCK] = jnp.where(held, met, 0.0)
            r1[...], r2[...] = both_sides(er[...], same)

        def close():
            if not final:
                pl.when(j == 0)(open_right)
            total = gathered(along_column, gz, zi, a, gzs_sem, gzr_sem)
            factor, against, change = orthonormal(total, r1[...], r2[...])
            couple_out[j] = factor
            chg[...] = change
            if not final:
                extend(er, r1, r2, position + BLOCK, against)

        if final:
            close()
            consume(me)
            loop(1, a, own)
            loop(0, a, rest)
            loop(0, h - a, pass_y)
        else:
            rest(a - 1)
            loop(met, h - a, pass_y)
        loop(a, h, rest)
        if not final:
            spread(along_genes, xg.at[j + 1], mine, g, xs_sem.at[j + 1], xr_sem.at[j + 1])
            close()
        walk.ended()

        def ended(t):
            hop(pb.at[t], pb.at[t], (ds_sem, t), (cr_sem, t), sibling, 2 * t + core)("wait_send")

        loop(0, h, ended)

        def ended_y(k):
            z, y = order(k)
            t = z * b + y
            hop(pb.at[t], pb.at[t], (fs_sem, t), (cr_sem, t), sibling, 2 * (z * b + yi) + core)("wait_send")

        loop(0, h - a, ended_y)

        def ended_z(k):
            z = lax.rem(zi + k, a)
            hop(pb.at[z], pb.at[z], (cs_sem, z), (cr_sem, z), sibling, me)("wait_send")

        loop(1, a, ended_z)

    loop(0, STEPS - 1, lambda j: step(j, False))
    step(STEPS - 1, True)
    base.ended()
    loop(0, n, lambda d: shipped(d, "wait"))
    loop(0, STEPS - 1, lambda j: block(j).wait())


def settle_outputs(left, right, diag, couple, left_out, right_out, diag_out, couple_out, lv, rv, dv, cv, came, went):
    routes = [(left, lv, left_out), (diag, dv, diag_out), (couple, cv, couple_out)]
    for i in range(right.shape[0] // 8):
        rows = pl.ds(i * 8, 8)
        routes.append((right.at[rows], rv.at[rows], right_out.at[rows]))
    fetch = [pltpu.make_async_copy(src, mid, came.at[i]) for i, (src, mid, _) in enumerate(routes)]
    store = [pltpu.make_async_copy(mid, dst, went.at[i]) for i, (_, mid, dst) in enumerate(routes)]
    for item in fetch:
        item.start()
    for item, onward in zip(fetch, store):
        item.wait()
        onward.start()
    for item in store:
        item.wait()


def body(counts, live_rows, left_basis, right_basis, right_start):
    cells, genes = counts.shape
    n = lax.axis_size("cells")
    g = lax.axis_size("genes")
    h = n // 2
    brief, longs = chunks(n, genes)
    width = (brief + (1 if longs else 0)) * LANES
    scales = (math.sqrt(float(cells * n)), math.sqrt(float(genes * g)))
    vmem = pl.BlockSpec(memory_space=pltpu.VMEM)
    anywhere = pl.BlockSpec(memory_space=pl.ANY)
    held = lambda *shape: pltpu.VMEM(shape, F32)
    square = held(LANES, LANES)
    dma = lambda *shape: pltpu.SemaphoreType.DMA(shape)
    out_shape = (
        jax.ShapeDtypeStruct((STEPS * BLOCK, cells), F32),
        jax.ShapeDtypeStruct((STEPS * BLOCK, genes), F32),
        jax.ShapeDtypeStruct((STEPS, BLOCK, BLOCK), F32),
        jax.ShapeDtypeStruct((STEPS, BLOCK, BLOCK), F32),
    )
    buffers = lambda rows: [
        held(n, rows, width), held(h, rows, width), held(h, rows, width), held(h, rows, width),
    ]
    scratch = [
        held(STEPS * BLOCK, genes),
        pltpu.VMEM((n, cells, width), jnp.int32),
        held(n, cells, width),
        *[pltpu.VMEM((n, cells, width), BF16)] * 2,
        *[pltpu.VMEM((n, LANES, width), BF16)] * 2,
        held(n, BASIS + BLOCK, width),
        *[square] * 8,
        *buffers(BLOCK),
        *buffers(BASIS),
        held(n, BLOCK, width),
        held(LANES, width),
        held(BLOCK, width),
        held(n, 1, width),
        held(n, 1, width),
        held(n, 1, width),
        held(8, LANES),
        held(BLOCK, LANES),
        held(n, BASIS + 8, LANES),
        held(n, BLOCK, LANES),
        held(g, BASIS + BLOCK, LANES),
        held(g, BASIS, LANES),
        held(STEPS, g, BLOCK, LANES),
        held(g, BLOCK, LANES),
        held(n, BLOCK, LANES),
        held(h, BLOCK, LANES),
        dma(n, 3, 2),
        *[dma(2, h)] * 12,
        dma(2, h), dma(2, n), dma(2, h), dma(2, h), dma(n), dma(n),
        *[dma(n)] * 6,
        *[dma(g)] * 4,
        dma(STEPS, g), dma(STEPS, g),
        dma(g), dma(g), dma(n), dma(n), dma(h), dma(h), dma(STEPS), dma(n, 2),
    ]
    results = pl.pallas_call(
        functools.partial(kernel, n, g, width, scales),
        out_shape=out_shape,
        in_specs=[pl.BlockSpec(memory_space=pltpu.SMEM), anywhere, vmem, anywhere, anywhere],
        out_specs=(vmem, anywhere, vmem, vmem),
        scratch_shapes=scratch,
        compiler_params=pltpu.CompilerParams(
            collective_id=0, has_side_effects=True, vmem_limit_bytes=66 * 1000 * 1000
        ),
    )(live_rows, counts, left_basis, right_basis, right_start)
    moves = 3 + STEPS * BLOCK // 8
    return pl.pallas_call(
        settle_outputs,
        out_shape=out_shape,
        in_specs=[anywhere] * 4,
        out_specs=(anywhere,) * 4,
        scratch_shapes=[pltpu.VMEM(item.shape, F32) for item in out_shape] + [dma(moves), dma(moves)],
    )(*results)


def solution(mesh):
    in_specs = (
        P("cells", "genes"),
        P("cells"),
        P(None, "cells"),
        P(None, "genes"),
        P(None, "genes"),
    )
    out_specs = (P(None, "cells"), P(None, "genes"), P(), P())
    return jax.shard_map(body, mesh=mesh, in_specs=in_specs, out_specs=out_specs, check_vma=False)
```

```python
import functools
import math

import jax
import jax.numpy as jnp
from jax import lax
from jax.experimental import pallas as pl
from jax.experimental.pallas import tpu as pltpu
from jax.sharding import PartitionSpec as P

BASIS = 32
BLOCK = 16
STEPS = 3
SLOTS = BASIS + STEPS * BLOCK
WEIGHT = SLOTS + BLOCK
LAG = 2
LANES = 128
F32 = jnp.float32
BF16 = jnp.bfloat16
HIGHEST = lax.Precision.HIGHEST
MESH = pl.DeviceIdType.MESH


def exact(lhs, rhs):
    return jnp.dot(lhs, rhs, precision=HIGHEST, preferred_element_type=F32)


def exact_rows(lhs, rhs):
    return lax.dot_general(
        lhs, rhs, (((1,), (1,)), ((), ())), precision=HIGHEST, preferred_element_type=F32
    )


def split(values):
    high = values.astype(BF16)
    return high, (values - high.astype(F32)).astype(BF16)


def product(high, both, rhs_high, rhs_low, dims):
    rows = high.shape[0]
    first = lax.dot_general(both, rhs_high, (dims, ((), ())), preferred_element_type=F32)
    second = lax.dot_general(high, rhs_low, (dims, ((), ())), preferred_element_type=F32)
    return first[:rows] + (first[rows:] + second)


ALONG = ((1,), (0,))
ROWS = ((1,), (1,))


def loop(start, stop, step, unroll=1):
    def one(k, carry):
        step(k)
        return carry

    lax.fori_loop(start, stop, one, 0, unroll=unroll if (stop - start) % unroll == 0 else 1)


def both_sides(gram, identity):
    gap = identity - gram
    return identity + gap, exact(gap, gap)


def orthonormal(gram, first, second):
    lane = lax.broadcasted_iota(jnp.int32, (BLOCK, LANES), 1)
    row = lax.broadcasted_iota(jnp.int32, (BLOCK, LANES), 0)
    coeffs = jnp.where(lane < SLOTS, gram, 0.0)
    combined = exact(coeffs, first)
    residue = exact(coeffs, second)
    squares = gram[:, SLOTS : SLOTS + BLOCK] - exact_rows(
        jnp.concatenate([combined, residue], axis=1), jnp.concatenate([coeffs, combined], axis=1)
    )
    change = jnp.where(lane == row + SLOTS, 1.0, -combined)
    columns = [jnp.broadcast_to(squares[:, k : k + 1], (BLOCK, LANES)) for k in range(BLOCK)]
    factor = jnp.zeros((BLOCK, LANES), F32)
    for k in range(BLOCK):
        pivot = jnp.broadcast_to(columns[k][k : k + 1], (BLOCK, LANES))
        root = lax.rsqrt(pivot)
        root = root * (1.5 - 0.5 * pivot * root * root)
        column = columns[k] * root
        factor = jnp.where((lane == k) & (row >= k), column, factor)
        below = jnp.where(row > k, column, 0.0)
        for i in range(k + 1, BLOCK):
            columns[i] = columns[i] - column * jnp.broadcast_to(column[i : i + 1], (BLOCK, LANES))
        scaled = jnp.broadcast_to(residue[k : k + 1], (BLOCK, LANES)) * root
        residue = jnp.where(row == k, scaled, residue - below * scaled)
        scaled = jnp.broadcast_to(change[k : k + 1], (BLOCK, LANES)) * root
        change = jnp.where(row == k, scaled, change - below * scaled)
    return factor[:, :BLOCK], residue, change


def grid(h):
    b = 1 << ((h.bit_length() - 1) // 2)
    b = b if h % b == 0 else 1
    return h // b, b


def chunks(n, genes):
    brief, extra = divmod(genes // LANES, n)
    stride = n // extra if extra else n
    return brief, [i * stride + (2 * (i % 2) if stride > 3 else 0) for i in range(extra)]


def kernel(
    n, g, width, scales,
    live, counts, left_basis, right_basis, right_start,
    left_out, right_hbm, diag_out, couple_out,
    right_out, cnt, logged, lhi, llo, vhi, vlo, rb, sl, mr, el, er, l1, l2, r1, r2,
    w, ra, rt, rz, wb, rab, rtb, rzb, pb, stack, ground, tpart, tfrom,
    mu, wsum, chg, gram0, gramz, gram, gramc, xs0, xb0, xg, gx, gy, gz,
    in_sem, as_sem, ar_sem, bs_sem, br_sem, zs_sem, zr_sem,
    bas_sem, bar_sem, bbs_sem, bbr_sem, bzs_sem, bzr_sem,
    cs_sem, cr_sem, ds_sem, fs_sem, ts_sem, tr_sem,
    ms_sem, mr_sem, g0s_sem, g0r_sem, g0zs_sem, g0zr_sem, gs_sem, gr_sem, gcs_sem, gcr_sem, s0s_sem, s0r_sem, b0s_sem, b0r_sem,
    xs_sem, xr_sem, gxs_sem, gxr_sem, gys_sem, gyr_sem, gzs_sem, gzr_sem, out_sem, tail_sem,
):
    cells, genes = counts.shape
    me = lax.axis_index("cells")
    mine = lax.axis_index("genes")
    core = lax.rem(me, 2)
    chip = me // 2
    h = n // 2
    a, b = grid(h)
    zi, yi = chip // b, lax.rem(chip, b)
    sibling = me + 1 - 2 * core
    seat = 2 * yi + core
    tiles = width // LANES
    brief, longs = chunks(n, genes)
    brief = brief * LANES
    lane = lax.broadcasted_iota(jnp.int32, (BLOCK, LANES), 1)
    row = lax.broadcasted_iota(jnp.int32, (BLOCK, LANES), 0)

    def along_cells(src, dst, send, recv, peer):
        return pltpu.make_async_remote_copy(
            src_ref=src, dst_ref=dst, send_sem=send, recv_sem=recv,
            device_id=(peer, mine), device_id_type=MESH,
        )

    def along_genes(src, dst, send, recv, peer):
        return pltpu.make_async_remote_copy(
            src_ref=src, dst_ref=dst, send_sem=send, recv_sem=recv,
            device_id=(me, peer), device_id_type=MESH,
        )

    def along_plane(src, dst, send, recv, peer):
        return along_cells(src, dst, send, recv, 2 * b * zi + peer)

    def along_column(src, dst, send, recv, peer):
        return along_cells(src, dst, send, recv, 2 * (peer * b + yi) + core)

    def is_long(d):
        found = d == longs[0]
        for other in longs[1:]:
            found = found | (d == other)
        return found

    def first_gene(d):
        at = d * brief
        for other in longs:
            at = at + jnp.where(d > other, LANES, 0)
        return pl.multiple_of(at, LANES)

    def fill_in(d, kind, method):
        here, there, rows = (
            (counts, cnt, pl.ds(0, cells)), (right_basis, rb, pl.ds(0, BASIS)), (right_start, rb, pl.ds(BASIS, BLOCK)),
        )[kind]
        at = first_gene(d)
        getattr(pltpu.make_async_copy(
            here.at[:, pl.ds(at, brief)], there.at[d, rows, pl.ds(0, brief)], in_sem.at[d, kind, 0]
        ), method)()
        if longs:
            @pl.when(is_long(d))
            def _():
                getattr(pltpu.make_async_copy(
                    here.at[:, pl.ds(pl.multiple_of(at + brief, LANES), LANES)],
                    there.at[d, rows, pl.ds(brief, LANES)], in_sem.at[d, kind, 1],
                ), method)()

    def hop(src, dst, send, recv, peer, d):
        def act(method):
            getattr(along_cells(
                src.at[:, pl.ds(0, brief)], dst.at[:, pl.ds(0, brief)],
                send[0].at[0, send[1]], recv[0].at[0, recv[1]], peer,
            ), method)()
            if longs:
                @pl.when(is_long(d))
                def _():
                    getattr(along_cells(
                        src.at[:, pl.ds(brief, LANES)], dst.at[:, pl.ds(brief, LANES)],
                        send[0].at[1, send[1]], recv[0].at[1, recv[1]], peer,
                    ), method)()

        return act

    def around(k):
        return lax.rem(me + k, n)

    loop(0, n, lambda k: fill_in(around(k), 0, "start"))

    def more(k):
        fill_in(around(k), 1, "start")
        fill_in(around(k), 2, "start")

    loop(0, n, more)
    if longs:
        for d in range(n):
            if d not in longs:
                cnt[d, :, brief:] = jnp.zeros((cells, LANES), jnp.int32)
                rb[d, :, brief:] = jnp.zeros((BASIS + BLOCK, LANES), F32)
        for table in (ra, rt, rz, rab, rtb, rzb, pb):
            table[:, :, brief:] = jnp.zeros((table.shape[0], table.shape[1], LANES), F32)

    barrier = pltpu.get_barrier_semaphore()

    def greet_cells(k):
        pl.semaphore_signal(barrier, inc=1, device_id=(lax.rem(me + k, n), mine), device_id_type=MESH)

    def greet_genes(k):
        pl.semaphore_signal(barrier, inc=1, device_id=(me, lax.rem(mine + k, g)), device_id_type=MESH)

    loop(1, n, greet_cells)
    loop(1, g, greet_genes)

    def spread(copy, buf, at, size, send, recv):
        def go(k):
            copy(buf.at[at], buf.at[at], send.at[k], recv.at[at], lax.rem(at + k, size)).start()

        loop(1, size, go)

    def waited(copy, buf, at, size, send, recv):
        def end(k):
            source = lax.rem(at + size - k, size)
            item = copy(buf.at[source], buf.at[source], send.at[k], recv.at[source], lax.rem(at + k, size))
            item.wait_send()
            item.wait_recv()

        loop(1, size, end)

    def gathered(copy, buf, at, size, send, recv):
        waited(copy, buf, at, size, send, recv)
        return lax.fori_loop(
            1, size, lambda k, total: total + buf[k], buf[0]
        )

    def onward(k):
        return lax.rem(zi + k, a)

    def behind(k):
        return lax.rem(zi + a - k, a)

    def order(k):
        return onward(1 + lax.rem(k, a)), lax.rem(yi + 1 + k // a, b)

    class Scatter:
        def __init__(self, part, fromcore, fromy, fromz, sems):
            self.part, self.fromcore, self.fromy, self.fromz = part, fromcore, fromy, fromz
            self.cs, self.cr, self.ys, self.yr, self.zs, self.zr = sems

        def over(self, d, t):
            return hop(self.part.at[d], self.fromcore.at[t], (self.cs, t), (self.cr, t), sibling, d)

        def launch(self, produce):
            def other(k):
                z, y = order(k)
                t = z * b + y
                return t, 2 * t + 1 - core

            def own(k):
                z, y = order(k)
                t = z * b + y
                return z, y, t, 2 * t + core

            def join(k):
                z, y, t, d = own(k)
                self.over(d, t)("wait_recv")
                self.part[d] = self.part[d] + self.fromcore[t]

                @pl.when(k < h - a)
                def _():
                    to = z * b + yi
                    hop(
                        self.part.at[d], self.fromy.at[to], (self.ys, t), (self.yr, to),
                        2 * (zi * b + y) + core, d,
                    )("start")

            def pair(k):
                t, d = other(k)
                produce(d)
                produce(own(k)[3])
                self.over(d, t)("start")

            def one(k):
                pair(k)
                join(k - LAG)

            loop(0, LAG, pair)
            loop(LAG, h, one)
            loop(h - LAG, h, join)

        def complete(self, z):
            d = 2 * (z * b + yi) + core

            def add(k):
                source = z * b + lax.rem(yi + k, b)
                hop(self.part.at[d], self.fromy.at[source], (self.ys, source), (self.yr, source), sibling, d)("wait_recv")
                self.part[d] = self.part[d] + self.fromy[source]

            loop(1, b, add)
            return d

        def third(self, start, stop):
            def one(k):
                z = onward(1 + k)
                d = self.complete(z)
                hop(self.part.at[d], self.fromz.at[zi], (self.zs, z), (self.zr, zi), d, d)("start")

            loop(min(start, a - 1), min(stop, a - 1), one)
            if stop >= a:
                self.complete(zi)

        def fourth(self, result, rows):
            result[rows] = self.part[me]

            def one(k):
                z = behind(k)
                hop(self.part.at[me], self.fromz.at[z], (self.zs, z), (self.zr, z), sibling, me)("wait_recv")
                result[rows] = result[rows] + self.fromz[z]

            loop(1, a, one)

        def ended(self):
            loop(0, h, lambda t: self.over(2 * t + 1 - core, t)("wait_send"))

            def sent_y(k):
                z, y = order(k)
                t = z * b + y
                hop(self.part.at[t], self.fromy.at[t], (self.ys, t), (self.yr, t), sibling, 2 * t + core)("wait_send")

            loop(0, h - a, sent_y)

            def sent_z(k):
                z = lax.rem(zi + k, a)
                d = 2 * (z * b + yi) + core
                hop(self.part.at[z], self.fromz.at[z], (self.zs, z), (self.zr, z), sibling, d)("wait_send")

            loop(1, a, sent_z)

    walk = Scatter(w, ra, rt, rz, (as_sem, ar_sem, bs_sem, br_sem, zs_sem, zr_sem))
    base = Scatter(wb, rab, rtb, rzb, (bas_sem, bar_sem, bbs_sem, bbr_sem, bzs_sem, bzr_sem))

    live_here = live[0]
    weights_row = jnp.where(
        lax.broadcasted_iota(jnp.int32, (1, cells), 1) < live_here, 1.0, 0.0
    ).astype(F32)
    weights = jnp.where(
        lax.broadcasted_iota(jnp.int32, (cells, LANES), 0) < live_here, 1.0, 0.0
    ).astype(F32)
    for table in (sl, mr, stack):
        table[...] = jnp.zeros_like(table)
    same = jnp.where(
        lax.broadcasted_iota(jnp.int32, (LANES, LANES), 0)
        == lax.broadcasted_iota(jnp.int32, (LANES, LANES), 1),
        1.0, 0.0,
    ).astype(F32)
    er[...] = same
    chg[...] = jnp.where(lane == row + SLOTS, 1.0, 0.0)

    def extend(table, first, second, position, against):
        here = jnp.where(lane == row + position, 1.0, 0.0).astype(F32)
        turn = lambda lhs, rhs: lax.dot_general(
            lhs, rhs, (((0,), (0,)), ((), ())), precision=HIGHEST, preferred_element_type=F32
        )
        table[...] = table[...] + turn(here, against) + turn(against, here)
        first[...], second[...] = both_sides(table[...], same)
    sl[0:BASIS] = left_basis[...] * weights_row
    sl[WEIGHT : WEIGHT + 8] = jnp.where(
        lax.broadcasted_iota(jnp.int32, (8, cells), 0) == 0, weights_row, 0.0
    )
    gram0[seat, 0:BASIS] = exact_rows(sl[0:BASIS], sl[...])
    gram0[seat, BASIS:] = exact_rows(sl[WEIGHT : WEIGHT + 8], sl[...])

    def take_log(d):
        for i in range(tiles):
            here = slice(i * LANES, (i + 1) * LANES)
            logged[d, :, here] = jnp.log(1.0 + cnt[d, :, here].astype(F32))

    fill_in(me, 0, "wait")
    take_log(me)
    portion = 1.0 / jnp.maximum(live_here, 1).astype(F32)
    for i in range(tiles):
        here = slice(i * LANES, (i + 1) * LANES)
        mu[me, :, here] = jnp.sum(logged[me, :, here] * weights, axis=0, keepdims=True) * portion
    pl.semaphore_wait(barrier, n - 1 + g - 1)
    spread(along_cells, mu, me, n, ms_sem, mr_sem)
    spread(along_plane, gram0, seat, 2 * b, g0s_sem, g0r_sem)

    def next_log(k):
        fill_in(around(k), 0, "wait")
        take_log(around(k))

    loop(1, n, next_log)
    xs0[mine] = jnp.zeros((BASIS + BLOCK, LANES), F32)
    xb0[mine] = jnp.zeros((BASIS, LANES), F32)
    xg[0, mine] = jnp.zeros((BLOCK, LANES), F32)

    def fill(k):
        d = around(k)
        fill_in(d, 1, "wait")
        fill_in(d, 2, "wait")
        high, low = split(rb[d])
        vhi[d, 0 : BASIS + BLOCK] = high
        vlo[d, 0 : BASIS + BLOCK] = low
        blank = jnp.zeros((LANES - BASIS - BLOCK, width), BF16)
        vhi[d, BASIS + BLOCK :] = blank
        vlo[d, BASIS + BLOCK :] = blank

    loop(0, n, fill)
    def meet(d):
        high = vhi[d, 0 : BASIS + BLOCK]
        both = jnp.concatenate([high, vlo[d, 0 : BASIS + BLOCK]], axis=0)
        xs0[mine] = xs0[mine] + product(high, both, vhi[d], vlo[d], ROWS)

    loop(0, n // 2, meet, 2)
    gramz[zi] = gathered(along_plane, gram0, seat, 2 * b, g0s_sem, g0r_sem)
    spread(along_column, gramz, zi, a, g0zs_sem, g0zr_sem)
    waited(along_cells, mu, me, n, ms_sem, mr_sem)

    bhigh, blow = split(jnp.concatenate(
        [sl[0:BASIS], sl[WEIGHT : WEIGHT + 8], jnp.zeros((8, cells), F32)], axis=0
    ))
    bboth = jnp.concatenate([bhigh, blow], axis=0)

    def center(d):
        for i in range(tiles):
            here = slice(i * LANES, (i + 1) * LANES)
            high, low = split(logged[d, :, here] - mu[d, :, here])
            lhi[d, :, here] = high
            llo[d, :, here] = low
        made = product(bhigh, bboth, lhi[d], llo[d], ALONG)
        wb[d] = made[0:BASIS]
        tpart[d] = made[BASIS : BASIS + 1]

    base.launch(center)

    def give(k):
        d = lax.rem(me + k, n)
        along_cells(tpart.at[d], tfrom.at[me], ts_sem.at[k], tr_sem.at[me], d).start()

    loop(1, n, give)

    def cross(d):
        high = vhi[d, 0 : BASIS + BLOCK]
        both = jnp.concatenate([high, vlo[d, 0 : BASIS + BLOCK]], axis=0)
        met = product(high, both, lhi[d], llo[d], ROWS)
        xb0[mine] = xb0[mine] + met[0:BASIS]
        xg[0, mine] = xg[0, mine] + met[BASIS:]

    loop(0, n // 2, cross, 2)
    base.third(0, 1)
    loop(n // 2, n, cross, 2)
    spread(along_genes, xg.at[0], mine, g, xs_sem.at[0], xr_sem.at[0])
    spread(along_genes, xb0, mine, g, b0s_sem, b0r_sem)
    base.third(1, 2)

    near = gathered(along_column, gramz, zi, a, g0zs_sem, g0zr_sem)
    corner = lax.broadcasted_iota(jnp.int32, (LANES, LANES), 0)
    across = lax.broadcasted_iota(jnp.int32, (BASIS, LANES), 1)
    el[...] = jnp.where((same > 0) & (corner >= BASIS), 1.0, 0.0)
    el[0:BASIS] = jnp.where(across < SLOTS, near[0:BASIS], 0.0)
    l1[...], l2[...] = both_sides(el[...], same)
    wsum[...] = near[BASIS:]
    live_total = near[BASIS : BASIS + 1, WEIGHT : WEIGHT + 1]
    inverse = 1.0 / live_total
    factor_scale = lax.rsqrt(live_total)
    factor_scale = factor_scale * (1.5 - 0.5 * live_total * factor_scale * factor_scale)

    def turned(column, start):
        return jnp.sum(jnp.where(lane == row + start, column, 0.0), axis=0, keepdims=True)

    def fresh(d):
        chigh, clow = split(chg[...])
        cboth = jnp.concatenate([chigh, clow], axis=0)
        return product(chigh, cboth, vhi[d], vlo[d], ALONG)

    def emit(d, rows, values):
        values = values * scales[1]
        at = first_gene(d)
        right_out[rows, pl.ds(at, brief)] = values[:, :brief]
        if longs:
            @pl.when(is_long(d))
            def _():
                right_out[rows, pl.ds(pl.multiple_of(at + brief, LANES), LANES)] = values[:, brief:]

    def shipped(d, method):
        rows = pl.ds((STEPS - 1) * BLOCK, BLOCK)
        at = first_gene(d)

        def act(start, size, which):
            here = pl.ds(start, size)
            getattr(pltpu.make_async_copy(
                right_out.at[rows, here], right_hbm.at[rows, here], tail_sem.at[d, which]
            ), method)()

        act(at, brief, 0)
        if longs:
            pl.when(is_long(d))(lambda: act(pl.multiple_of(at + brief, LANES), LANES, 1))

    def block(j):
        rows = pl.ds(j * BLOCK if isinstance(j, int) else pl.multiple_of(j * BLOCK, BLOCK), BLOCK)
        return pltpu.make_async_copy(right_out.at[rows], right_hbm.at[rows], out_sem.at[j])

    def update(j, start, stop):
        later = pl.multiple_of(BASIS + (j + 1) * BLOCK, BLOCK)
        rows = pl.ds(pl.multiple_of(j * BLOCK, BLOCK), BLOCK)

        def right(d):
            values = fresh(d)
            vhigh, vlow = split(values)
            vhi[d, pl.ds(later, BLOCK)] = vhigh
            vlo[d, pl.ds(later, BLOCK)] = vlow
            emit(d, rows, values)

        loop(start, stop, right)

    def keep(d, values):
        phigh, plow = split(values)
        vhi[d, SLOTS : SLOTS + BLOCK] = phigh
        vlo[d, SLOTS : SLOTS + BLOCK] = plow
        return phigh, jnp.concatenate([phigh, plow], axis=0)

    def begin(j):
        @pl.when(j == 0)
        def _():
            base.third(2, a)
            walk.third(0, 2)

    def step(j, final):
        position = BASIS + j * BLOCK
        position = position if final else pl.multiple_of(position, BLOCK)
        mr[SLOTS : SLOTS + BLOCK] = gathered(along_genes, xg.at[j], mine, g, xs_sem.at[j], xr_sem.at[j]) * weights_row
        vectors = exact(chg[...], mr[...])
        mr[pl.ds(position, BLOCK)] = vectors
        sl[SLOTS : SLOTS + BLOCK] = vectors
        gram[seat] = exact_rows(vectors, sl[...])
        spread(along_plane, gram, seat, 2 * b, gs_sem, gr_sem)
        high, low = split(vectors)
        both = jnp.concatenate([high, low], axis=0)

        def produce(d):
            w[d] = product(high, both, lhi[d], llo[d], ALONG)

        walk.launch(produce)
        gramc[zi] = gathered(along_plane, gram, seat, 2 * b, gs_sem, gr_sem)
        spread(along_column, gramc, zi, a, gcs_sem, gcr_sem)
        if final:
            update(j - 1, 0, n // 4)
            walk.third(0, 1)
            update(j - 1, n // 4, n // 2)
            walk.third(1, 2)
            update(j - 1, n // 2, n)
            block(j - 1).start()
        else:
            begin(j)

            @pl.when(j > 0)
            def _():
                update(j - 1, 0, n // 4)
                walk.third(0, 1)
                update(j - 1, n // 4, n // 2)
                walk.third(1, 2)
                update(j - 1, n // 2, n)
                block(j - 1).start()

        total = gathered(along_column, gramc, zi, a, gcs_sem, gcr_sem)
        held = total[:, WEIGHT : WEIGHT + 1] * inverse
        weighed = wsum[0:1] + turned(total[:, WEIGHT : WEIGHT + 1], SLOTS)
        scale = jnp.where(lane < SLOTS, factor_scale, factor_scale * factor_scale)
        factor, against, change = orthonormal((total - held * weighed) * scale, l1[...], l2[...])
        walk.third(2, a - 1)
        diag_out[j] = factor
        tilt = jnp.sum(jnp.where(lane < SLOTS, change * wsum[0:1], 0.0), axis=1, keepdims=True)
        wsum[0:1] = wsum[0:1] + turned(tilt, position)
        shift = jnp.sum(
            jnp.where((lane >= SLOTS) & (lane < WEIGHT), change * turned(held, SLOTS), 0.0), axis=1, keepdims=True
        )
        blend = jnp.where(
            lane < SLOTS, change,
            jnp.where(lane < WEIGHT, change * factor_scale, jnp.where(lane == WEIGHT, -shift * factor_scale, 0.0)),
        )
        leftvec = exact(blend, sl[...])
        sl[pl.ds(position, BLOCK)] = leftvec
        left_out[pl.ds(position - BASIS, BLOCK)] = leftvec * scales[0]
        tilt = tilt * inverse
        blend = jnp.where(lane == WEIGHT, blend - tilt, blend) * factor_scale

        def settle():
            ground[...] = exact(jnp.where((lane < SLOTS) | (lane >= WEIGHT), blend, 0.0), stack[...])

        if final:
            settle()
        else:
            pl.when(j > 0)(settle)
        walk.third(a - 1, a)
        if not final:
            @pl.when(j == 0)
            def _():
                base.fourth(stack, slice(0, BASIS))

                def take(k):
                    source = lax.rem(me + n - k, n)
                    item = along_cells(tpart.at[source], tfrom.at[source], ts_sem.at[k], tr_sem.at[source], sibling)
                    item.wait_send()
                    item.wait_recv()
                    tpart[me] = tpart[me] + tfrom[source]

                loop(1, n, take)
                stack[WEIGHT : WEIGHT + 1] = tpart[me]
                settle()
                mr[0:BASIS] = gathered(along_genes, xb0, mine, g, b0s_sem, b0r_sem) * weights_row

        walk.fourth(stack, slice(SLOTS, SLOTS + BLOCK))
        columns = [blend[:, SLOTS + k : SLOTS + k + 1] for k in range(BLOCK)]
        for i in range(tiles):
            here = slice(i * LANES, (i + 1) * LANES)
            values = ground[:, here]
            for k in range(BLOCK):
                values = values + columns[k] * stack[SLOTS + k : SLOTS + k + 1, here]
            pb[me, :, here] = values

        def relay(z):
            t = z * b + yi
            d = 2 * t + core

            def to_y(k):
                y = lax.rem(yi + k, b)
                hop(pb.at[d], pb.at[d], (fs_sem, z * b + y), (cr_sem, d), 2 * (zi * b + y) + core, d)("start")

            loop(1, b, to_y)
            hop(pb.at[d], pb.at[d], (ds_sem, t), (cr_sem, d), sibling, d)("start")

        def arrived(d):
            hop(pb.at[d], pb.at[d], (ds_sem, 0), (cr_sem, d), sibling, d)("wait_recv")

        def go(k):
            z = onward(k)
            hop(pb.at[me], pb.at[me], (cs_sem, z), (cr_sem, me), 2 * (z * b + yi) + core, me)("start")

        if not final:
            loop(1, a, go)
            relay(zi)
        phigh, pboth = keep(me, pb[me])
        square = product(phigh, pboth, vhi[me], vlo[me], ROWS)
        plane = (along_plane, gy, seat, 2 * b, gys_sem, gyr_sem)
        line = (along_genes, gx, mine, g, gxs_sem, gxr_sem)
        column = (along_column, gz, zi, a, gzs_sem, gzr_sem)
        stages = (column, line, plane) if final else (plane, line, column)

        def advance(i):
            copy, buf, at = stages[i][:3]
            buf[at] = gathered(*stages[i - 1]) if i else square
            spread(*stages[i])

        advance(0)
        if final:
            relay(zi)
            loop(1, a, go)
        else:
            stack[pl.ds(position, BLOCK)] = (
                pb[me] * (live_total * factor_scale) + tilt * stack[WEIGHT : WEIGHT + 1]
            )
            xg[j + 1, mine] = jnp.zeros((BLOCK, LANES), F32)
            extend(el, l1, l2, position, against)

        def consume(d):
            phigh, pboth = keep(d, pb[d])
            if final:
                emit(d, pl.ds((STEPS - 1) * BLOCK, BLOCK), fresh(d))
                shipped(d, "start")
            else:
                xg[j + 1, mine] = xg[j + 1, mine] + product(phigh, pboth, lhi[d], llo[d], ROWS)

        def pass_z(k):
            z = behind(k)
            arrived(2 * (z * b + yi) + core)
            relay(z)

        def quarter(q):
            if not final:
                pl.when(j == 0)(lambda: loop(n // 2 + q * n // 8, n // 2 + (q + 1) * n // 8, meet))

        def own(k):
            consume(2 * (behind(k) * b + yi) + core)

        def pass_y(k):
            z = behind(lax.rem(k, a))
            t = z * b + lax.rem(yi + 1 + k // a, b)
            d = 2 * t + core
            arrived(d)
            hop(pb.at[d], pb.at[d], (ds_sem, t), (cr_sem, d), sibling, d)("start")
            consume(d)

        def rest(k):
            z = behind(lax.rem(k, a))
            t = z * b + lax.rem(yi + k // a, b)
            d = 2 * t + 1 - core
            arrived(d)
            consume(d)

        def early(k):
            if not final:
                own(k)
                rest(k - 1)

        def follow(k):
            pass_z(k)
            early(k)

        met = min(1, h - a)
        if final:
            advance(1)
            loop(1, min(2, a), pass_z)
            advance(2)
            loop(min(2, a), a, pass_z)
        else:
            consume(me)
            quarter(0)
            loop(1, min(2, a), pass_z)
            loop(1, min(2, a), early)
            advance(1)
            quarter(1)
            loop(min(2, a), min(3, a), pass_z)
            loop(min(2, a), min(3, a), early)
            loop(0, met, pass_y)
            advance(2)
            quarter(2)
            loop(min(3, a), a, follow)
            quarter(3)
            pl.when(j == 0)(lambda: spread(along_genes, xs0, mine, g, s0s_sem, s0r_sem))

        def open_right():
            met = gathered(along_genes, xs0, mine, g, s0s_sem, s0r_sem)
            held = lax.broadcasted_iota(jnp.int32, met.shape, 1) < SLOTS
            er[0 : BASIS + BLOCK] = jnp.where(held, met, 0.0)
            r1[...], r2[...] = both_sides(er[...], same)

        def close():
            if not final:
                pl.when(j == 0)(open_right)
            total = gathered(*stages[2])
            factor, against, change = orthonormal(total, r1[...], r2[...])
            couple_out[j] = factor
            chg[...] = change
            if not final:
                extend(er, r1, r2, position + BLOCK, against)

        if final:
            close()
            consume(me)
            loop(1, a, own)
            loop(0, a, rest)
            loop(0, h - a, pass_y)
        else:
            rest(a - 1)
            loop(met, h - a, pass_y)
        loop(a, h, rest)
        if not final:
            spread(along_genes, xg.at[j + 1], mine, g, xs_sem.at[j + 1], xr_sem.at[j + 1])
            close()
        walk.ended()

        def ended(t):
            hop(pb.at[t], pb.at[t], (ds_sem, t), (cr_sem, t), sibling, 2 * t + core)("wait_send")

        loop(0, h, ended)

        def ended_y(k):
            z, y = order(k)
            t = z * b + y
            hop(pb.at[t], pb.at[t], (fs_sem, t), (cr_sem, t), sibling, 2 * (z * b + yi) + core)("wait_send")

        loop(0, h - a, ended_y)

        def ended_z(k):
            z = lax.rem(zi + k, a)
            hop(pb.at[z], pb.at[z], (cs_sem, z), (cr_sem, z), sibling, me)("wait_send")

        loop(1, a, ended_z)

    loop(0, STEPS - 1, lambda j: step(j, False))
    step(STEPS - 1, True)
    base.ended()
    loop(0, n, lambda d: shipped(d, "wait"))
    loop(0, STEPS - 1, lambda j: block(j).wait())


def settle_outputs(left, right, diag, couple, left_out, right_out, diag_out, couple_out, lv, rv, dv, cv, came, went):
    routes = [(left, lv, left_out), (diag, dv, diag_out), (couple, cv, couple_out)]
    for i in range(right.shape[0] // 8):
        rows = pl.ds(i * 8, 8)
        routes.append((right.at[rows], rv.at[rows], right_out.at[rows]))
    fetch = [pltpu.make_async_copy(src, mid, came.at[i]) for i, (src, mid, _) in enumerate(routes)]
    store = [pltpu.make_async_copy(mid, dst, went.at[i]) for i, (_, mid, dst) in enumerate(routes)]
    for item in fetch:
        item.start()
    for item, onward in zip(fetch, store):
        item.wait()
        onward.start()
    for item in store:
        item.wait()


def body(counts, live_rows, left_basis, right_basis, right_start):
    cells, genes = counts.shape
    n = lax.axis_size("cells")
    g = lax.axis_size("genes")
    h = n // 2
    a, b = grid(h)
    brief, longs = chunks(n, genes)
    width = (brief + (1 if longs else 0)) * LANES
    scales = (math.sqrt(float(cells * n)), math.sqrt(float(genes * g)))
    vmem = pl.BlockSpec(memory_space=pltpu.VMEM)
    anywhere = pl.BlockSpec(memory_space=pl.ANY)
    held = lambda *shape: pltpu.VMEM(shape, F32)
    square = held(LANES, LANES)
    dma = lambda *shape: pltpu.SemaphoreType.DMA(shape)
    out_shape = (
        jax.ShapeDtypeStruct((STEPS * BLOCK, cells), F32),
        jax.ShapeDtypeStruct((STEPS * BLOCK, genes), F32),
        jax.ShapeDtypeStruct((STEPS, BLOCK, BLOCK), F32),
        jax.ShapeDtypeStruct((STEPS, BLOCK, BLOCK), F32),
    )
    buffers = lambda rows: [
        held(n, rows, width), held(h, rows, width), held(h, rows, width), held(h, rows, width),
    ]
    scratch = [
        held(STEPS * BLOCK, genes),
        pltpu.VMEM((n, cells, width), jnp.int32),
        held(n, cells, width),
        *[pltpu.VMEM((n, cells, width), BF16)] * 2,
        *[pltpu.VMEM((n, LANES, width), BF16)] * 2,
        held(n, BASIS + BLOCK, width),
        *[square] * 8,
        *buffers(BLOCK),
        *buffers(BASIS),
        held(n, BLOCK, width),
        held(LANES, width),
        held(BLOCK, width),
        held(n, 1, width),
        held(n, 1, width),
        held(n, 1, width),
        held(8, LANES),
        held(BLOCK, LANES),
        held(2 * b, BASIS + 8, LANES),
        held(a, BASIS + 8, LANES),
        held(2 * b, BLOCK, LANES),
        held(a, BLOCK, LANES),
        held(g, BASIS + BLOCK, LANES),
        held(g, BASIS, LANES),
        held(STEPS, g, BLOCK, LANES),
        held(g, BLOCK, LANES),
        held(2 * b, BLOCK, LANES),
        held(a, BLOCK, LANES),
        dma(n, 3, 2),
        *[dma(2, h)] * 12,
        dma(2, h), dma(2, n), dma(2, h), dma(2, h), dma(n), dma(n),
        dma(n), dma(n),
        *[dma(2 * b), dma(2 * b), dma(a), dma(a)] * 2,
        *[dma(g)] * 4,
        dma(STEPS, g), dma(STEPS, g),
        dma(g), dma(g), dma(2 * b), dma(2 * b), dma(a), dma(a), dma(STEPS), dma(n, 2),
    ]
    results = pl.pallas_call(
        functools.partial(kernel, n, g, width, scales),
        out_shape=out_shape,
        in_specs=[pl.BlockSpec(memory_space=pltpu.SMEM), anywhere, vmem, anywhere, anywhere],
        out_specs=(vmem, anywhere, vmem, vmem),
        scratch_shapes=scratch,
        compiler_params=pltpu.CompilerParams(
            collective_id=0, has_side_effects=True, vmem_limit_bytes=66 * 1000 * 1000
        ),
    )(live_rows, counts, left_basis, right_basis, right_start)
    moves = 3 + STEPS * BLOCK // 8
    return pl.pallas_call(
        settle_outputs,
        out_shape=out_shape,
        in_specs=[anywhere] * 4,
        out_specs=(anywhere,) * 4,
        scratch_shapes=[pltpu.VMEM(item.shape, F32) for item in out_shape] + [dma(moves), dma(moves)],
    )(*results)


def solution(mesh):
    in_specs = (
        P("cells", "genes"),
        P("cells"),
        P(None, "cells"),
        P(None, "genes"),
        P(None, "genes"),
    )
    out_specs = (P(None, "cells"), P(None, "genes"), P(), P())
    return jax.shard_map(body, mesh=mesh, in_specs=in_specs, out_specs=out_specs, check_vma=False)
```

```python
import functools
import math

import jax
import jax.numpy as jnp
from jax import lax
from jax.experimental import pallas as pl
from jax.experimental.pallas import tpu as pltpu
from jax.sharding import PartitionSpec as P

BASIS = 32
BLOCK = 16
STEPS = 3
SLOTS = BASIS + STEPS * BLOCK
WEIGHT = SLOTS + BLOCK
LAG = 2
LANES = 128
F32 = jnp.float32
BF16 = jnp.bfloat16
HIGHEST = lax.Precision.HIGHEST
MESH = pl.DeviceIdType.MESH


def exact(lhs, rhs):
    return jnp.dot(lhs, rhs, precision=HIGHEST, preferred_element_type=F32)


def exact_rows(lhs, rhs):
    return lax.dot_general(
        lhs, rhs, (((1,), (1,)), ((), ())), precision=HIGHEST, preferred_element_type=F32
    )


def split(values):
    high = values.astype(BF16)
    return high, (values - high.astype(F32)).astype(BF16)


def product(high, both, rhs_high, rhs_low, dims):
    rows = high.shape[0]
    first = lax.dot_general(both, rhs_high, (dims, ((), ())), preferred_element_type=F32)
    second = lax.dot_general(high, rhs_low, (dims, ((), ())), preferred_element_type=F32)
    return first[:rows] + (first[rows:] + second)


ALONG = ((1,), (0,))
ROWS = ((1,), (1,))


def loop(start, stop, step, unroll=1):
    def one(k, carry):
        step(k)
        return carry

    lax.fori_loop(start, stop, one, 0, unroll=unroll if (stop - start) % unroll == 0 else 1)


def both_sides(gram, identity):
    gap = identity - gram
    return identity + gap, exact(gap, gap)


def orthonormal(gram, first, second):
    lane = lax.broadcasted_iota(jnp.int32, (BLOCK, LANES), 1)
    row = lax.broadcasted_iota(jnp.int32, (BLOCK, LANES), 0)
    coeffs = jnp.where(lane < SLOTS, gram, 0.0)
    combined = exact(coeffs, first)
    residue = exact(coeffs, second)
    squares = gram[:, SLOTS : SLOTS + BLOCK] - exact_rows(
        jnp.concatenate([combined, residue], axis=1), jnp.concatenate([coeffs, combined], axis=1)
    )
    change = jnp.where(lane == row + SLOTS, 1.0, -combined)
    columns = [jnp.broadcast_to(squares[:, k : k + 1], (BLOCK, LANES)) for k in range(BLOCK)]
    factor = jnp.zeros((BLOCK, LANES), F32)
    for k in range(BLOCK):
        pivot = jnp.broadcast_to(columns[k][k : k + 1], (BLOCK, LANES))
        root = lax.rsqrt(pivot)
        root = root * (1.5 - 0.5 * pivot * root * root)
        column = columns[k] * root
        factor = jnp.where((lane == k) & (row >= k), column, factor)
        below = jnp.where(row > k, column, 0.0)
        for i in range(k + 1, BLOCK):
            columns[i] = columns[i] - column * jnp.broadcast_to(column[i : i + 1], (BLOCK, LANES))
        scaled = jnp.broadcast_to(residue[k : k + 1], (BLOCK, LANES)) * root
        residue = jnp.where(row == k, scaled, residue - below * scaled)
        scaled = jnp.broadcast_to(change[k : k + 1], (BLOCK, LANES)) * root
        change = jnp.where(row == k, scaled, change - below * scaled)
    return factor[:, :BLOCK], residue, change


def grid(h):
    b = 1 << ((h.bit_length() - 1) // 2)
    b = b if h % b == 0 else 1
    return h // b, b


def chunks(n, genes):
    brief, extra = divmod(genes // LANES, n)
    stride = n // extra if extra else n
    return brief, [i * stride + (2 * (i % 2) if stride > 3 else 0) for i in range(extra)]


def kernel(
    n, g, width, scales,
    live, counts, left_basis, right_basis, right_start,
    left_out, right_out, diag_out, couple_out,
    cnt, logged, lhi, llo, vhi, vlo, rb, sl, mr, el, er, l1, l2, r1, r2,
    w, ra, rt, rz, wb, rab, rtb, rzb, pb, stack, ground, tpart, tfrom,
    mu, wsum, chg, gram0, gramz, gram, gramc, xs0, xb0, xg, gx, gy, gz,
    in_sem, as_sem, ar_sem, bs_sem, br_sem, zs_sem, zr_sem,
    bas_sem, bar_sem, bbs_sem, bbr_sem, bzs_sem, bzr_sem,
    cs_sem, cr_sem, ds_sem, fs_sem, ts_sem, tr_sem,
    ms_sem, mr_sem, g0s_sem, g0r_sem, g0zs_sem, g0zr_sem, gs_sem, gr_sem, gcs_sem, gcr_sem, s0s_sem, s0r_sem, b0s_sem, b0r_sem,
    xs_sem, xr_sem, gxs_sem, gxr_sem, gys_sem, gyr_sem, gzs_sem, gzr_sem,
):
    cells, genes = counts.shape
    me = lax.axis_index("cells")
    mine = lax.axis_index("genes")
    core = lax.rem(me, 2)
    chip = me // 2
    h = n // 2
    a, b = grid(h)
    zi, yi = chip // b, lax.rem(chip, b)
    sibling = me + 1 - 2 * core
    seat = 2 * yi + core
    tiles = width // LANES
    brief, longs = chunks(n, genes)
    brief = brief * LANES
    lane = lax.broadcasted_iota(jnp.int32, (BLOCK, LANES), 1)
    row = lax.broadcasted_iota(jnp.int32, (BLOCK, LANES), 0)

    def along_cells(src, dst, send, recv, peer):
        return pltpu.make_async_remote_copy(
            src_ref=src, dst_ref=dst, send_sem=send, recv_sem=recv,
            device_id=(peer, mine), device_id_type=MESH,
        )

    def along_genes(src, dst, send, recv, peer):
        return pltpu.make_async_remote_copy(
            src_ref=src, dst_ref=dst, send_sem=send, recv_sem=recv,
            device_id=(me, peer), device_id_type=MESH,
        )

    def along_plane(src, dst, send, recv, peer):
        return along_cells(src, dst, send, recv, 2 * b * zi + peer)

    def along_column(src, dst, send, recv, peer):
        return along_cells(src, dst, send, recv, 2 * (peer * b + yi) + core)

    def is_long(d):
        found = d == longs[0]
        for other in longs[1:]:
            found = found | (d == other)
        return found

    def first_gene(d):
        at = d * brief
        for other in longs:
            at = at + jnp.where(d > other, LANES, 0)
        return pl.multiple_of(at, LANES)

    def fill_in(d, kind, method):
        here, there, rows = (
            (counts, cnt, pl.ds(0, cells)), (right_basis, rb, pl.ds(0, BASIS)), (right_start, rb, pl.ds(BASIS, BLOCK)),
        )[kind]
        at = first_gene(d)
        getattr(pltpu.make_async_copy(
            here.at[:, pl.ds(at, brief)], there.at[d, rows, pl.ds(0, brief)], in_sem.at[d, kind, 0]
        ), method)()
        if longs:
            @pl.when(is_long(d))
            def _():
                getattr(pltpu.make_async_copy(
                    here.at[:, pl.ds(pl.multiple_of(at + brief, LANES), LANES)],
                    there.at[d, rows, pl.ds(brief, LANES)], in_sem.at[d, kind, 1],
                ), method)()

    def hop(src, dst, send, recv, peer, d):
        def act(method):
            getattr(along_cells(
                src.at[:, pl.ds(0, brief)], dst.at[:, pl.ds(0, brief)],
                send[0].at[0, send[1]], recv[0].at[0, recv[1]], peer,
            ), method)()
            if longs:
                @pl.when(is_long(d))
                def _():
                    getattr(along_cells(
                        src.at[:, pl.ds(brief, LANES)], dst.at[:, pl.ds(brief, LANES)],
                        send[0].at[1, send[1]], recv[0].at[1, recv[1]], peer,
                    ), method)()

        return act

    def around(k):
        return lax.rem(me + k, n)

    loop(0, n, lambda k: fill_in(around(k), 0, "start"))

    def more(k):
        fill_in(around(k), 1, "start")
        fill_in(around(k), 2, "start")

    loop(0, n, more)
    if longs:
        for d in range(n):
            if d not in longs:
                cnt[d, :, brief:] = jnp.zeros((cells, LANES), jnp.int32)
                rb[d, :, brief:] = jnp.zeros((BASIS + BLOCK, LANES), F32)
        for table in (ra, rt, rz, rab, rtb, rzb, pb):
            table[:, :, brief:] = jnp.zeros((table.shape[0], table.shape[1], LANES), F32)

    barrier = pltpu.get_barrier_semaphore()

    def greet_cells(k):
        pl.semaphore_signal(barrier, inc=1, device_id=(lax.rem(me + k, n), mine), device_id_type=MESH)

    def greet_genes(k):
        pl.semaphore_signal(barrier, inc=1, device_id=(me, lax.rem(mine + k, g)), device_id_type=MESH)

    loop(1, n, greet_cells)
    loop(1, g, greet_genes)

    def spread(copy, buf, at, size, send, recv):
        def go(k):
            copy(buf.at[at], buf.at[at], send.at[k], recv.at[at], lax.rem(at + k, size)).start()

        loop(1, size, go)

    def waited(copy, buf, at, size, send, recv):
        def end(k):
            source = lax.rem(at + size - k, size)
            item = copy(buf.at[source], buf.at[source], send.at[k], recv.at[source], lax.rem(at + k, size))
            item.wait_send()
            item.wait_recv()

        loop(1, size, end)

    def gathered(copy, buf, at, size, send, recv):
        waited(copy, buf, at, size, send, recv)
        return lax.fori_loop(
            1, size, lambda k, total: total + buf[k], buf[0]
        )

    def onward(k):
        return lax.rem(zi + k, a)

    def behind(k):
        return lax.rem(zi + a - k, a)

    def order(k):
        return onward(1 + lax.rem(k, a)), lax.rem(yi + 1 + k // a, b)

    class Scatter:
        def __init__(self, part, fromcore, fromy, fromz, sems):
            self.part, self.fromcore, self.fromy, self.fromz = part, fromcore, fromy, fromz
            self.cs, self.cr, self.ys, self.yr, self.zs, self.zr = sems

        def over(self, d, t):
            return hop(self.part.at[d], self.fromcore.at[t], (self.cs, t), (self.cr, t), sibling, d)

        def launch(self, produce):
            def other(k):
                z, y = order(k)
                t = z * b + y
                return t, 2 * t + 1 - core

            def own(k):
                z, y = order(k)
                t = z * b + y
                return z, y, t, 2 * t + core

            def join(k):
                z, y, t, d = own(k)
                self.over(d, t)("wait_recv")
                self.part[d] = self.part[d] + self.fromcore[t]

                @pl.when(k < h - a)
                def _():
                    to = z * b + yi
                    hop(
                        self.part.at[d], self.fromy.at[to], (self.ys, t), (self.yr, to),
                        2 * (zi * b + y) + core, d,
                    )("start")

            def pair(k):
                t, d = other(k)
                produce(d)
                produce(own(k)[3])
                self.over(d, t)("start")

            def one(k):
                pair(k)
                join(k - LAG)

            loop(0, LAG, pair)
            loop(LAG, h, one)
            loop(h - LAG, h, join)

        def complete(self, z):
            d = 2 * (z * b + yi) + core

            def add(k):
                source = z * b + lax.rem(yi + k, b)
                hop(self.part.at[d], self.fromy.at[source], (self.ys, source), (self.yr, source), sibling, d)("wait_recv")
                self.part[d] = self.part[d] + self.fromy[source]

            loop(1, b, add)
            return d

        def third(self, start, stop):
            def one(k):
                z = onward(1 + k)
                d = self.complete(z)
                hop(self.part.at[d], self.fromz.at[zi], (self.zs, z), (self.zr, zi), d, d)("start")

            loop(min(start, a - 1), min(stop, a - 1), one)
            if stop >= a:
                self.complete(zi)

        def fourth(self, result, rows):
            result[rows] = self.part[me]

            def one(k):
                z = behind(k)
                hop(self.part.at[me], self.fromz.at[z], (self.zs, z), (self.zr, z), sibling, me)("wait_recv")
                result[rows] = result[rows] + self.fromz[z]

            loop(1, a, one)

        def ended(self):
            loop(0, h, lambda t: self.over(2 * t + 1 - core, t)("wait_send"))

            def sent_y(k):
                z, y = order(k)
                t = z * b + y
                hop(self.part.at[t], self.fromy.at[t], (self.ys, t), (self.yr, t), sibling, 2 * t + core)("wait_send")

            loop(0, h - a, sent_y)

            def sent_z(k):
                z = lax.rem(zi + k, a)
                d = 2 * (z * b + yi) + core
                hop(self.part.at[z], self.fromz.at[z], (self.zs, z), (self.zr, z), sibling, d)("wait_send")

            loop(1, a, sent_z)

    walk = Scatter(w, ra, rt, rz, (as_sem, ar_sem, bs_sem, br_sem, zs_sem, zr_sem))
    base = Scatter(wb, rab, rtb, rzb, (bas_sem, bar_sem, bbs_sem, bbr_sem, bzs_sem, bzr_sem))

    live_here = live[0]
    weights_row = jnp.where(
        lax.broadcasted_iota(jnp.int32, (1, cells), 1) < live_here, 1.0, 0.0
    ).astype(F32)
    weights = jnp.where(
        lax.broadcasted_iota(jnp.int32, (cells, LANES), 0) < live_here, 1.0, 0.0
    ).astype(F32)
    for table in (sl, mr, stack):
        table[...] = jnp.zeros_like(table)
    same = jnp.where(
        lax.broadcasted_iota(jnp.int32, (LANES, LANES), 0)
        == lax.broadcasted_iota(jnp.int32, (LANES, LANES), 1),
        1.0, 0.0,
    ).astype(F32)
    er[...] = same
    chg[...] = jnp.where(lane == row + SLOTS, 1.0, 0.0)

    def extend(table, first, second, position, against):
        here = jnp.where(lane == row + position, 1.0, 0.0).astype(F32)
        turn = lambda lhs, rhs: lax.dot_general(
            lhs, rhs, (((0,), (0,)), ((), ())), precision=HIGHEST, preferred_element_type=F32
        )
        table[...] = table[...] + turn(here, against) + turn(against, here)
        first[...], second[...] = both_sides(table[...], same)
    sl[0:BASIS] = left_basis[...] * weights_row
    sl[WEIGHT : WEIGHT + 8] = jnp.where(
        lax.broadcasted_iota(jnp.int32, (8, cells), 0) == 0, weights_row, 0.0
    )
    gram0[seat, 0:BASIS] = exact_rows(sl[0:BASIS], sl[...])
    gram0[seat, BASIS:] = exact_rows(sl[WEIGHT : WEIGHT + 8], sl[...])

    def take_log(d):
        for i in range(tiles):
            here = slice(i * LANES, (i + 1) * LANES)
            logged[d, :, here] = jnp.log(1.0 + cnt[d, :, here].astype(F32))

    fill_in(me, 0, "wait")
    take_log(me)
    portion = 1.0 / jnp.maximum(live_here, 1).astype(F32)
    for i in range(tiles):
        here = slice(i * LANES, (i + 1) * LANES)
        mu[me, :, here] = jnp.sum(logged[me, :, here] * weights, axis=0, keepdims=True) * portion
    def next_log(k):
        fill_in(around(k), 0, "wait")
        take_log(around(k))

    loop(1, n, next_log)
    pl.semaphore_wait(barrier, n - 1 + g - 1)
    spread(along_cells, mu, me, n, ms_sem, mr_sem)
    spread(along_plane, gram0, seat, 2 * b, g0s_sem, g0r_sem)

    xs0[mine] = jnp.zeros((BASIS + BLOCK, LANES), F32)
    xb0[mine] = jnp.zeros((BASIS, LANES), F32)
    xg[0, mine] = jnp.zeros((BLOCK, LANES), F32)

    def fill(k):
        d = around(k)
        fill_in(d, 1, "wait")
        fill_in(d, 2, "wait")
        high, low = split(rb[d])
        vhi[d, 0 : BASIS + BLOCK] = high
        vlo[d, 0 : BASIS + BLOCK] = low
        blank = jnp.zeros((LANES - BASIS - BLOCK, width), BF16)
        vhi[d, BASIS + BLOCK :] = blank
        vlo[d, BASIS + BLOCK :] = blank

    loop(0, n, fill)
    def meet(d):
        high = vhi[d, 0 : BASIS + BLOCK]
        both = jnp.concatenate([high, vlo[d, 0 : BASIS + BLOCK]], axis=0)
        xs0[mine] = xs0[mine] + product(high, both, vhi[d], vlo[d], ROWS)

    loop(0, n // 2, meet, 2)
    gramz[zi] = gathered(along_plane, gram0, seat, 2 * b, g0s_sem, g0r_sem)
    spread(along_column, gramz, zi, a, g0zs_sem, g0zr_sem)
    waited(along_cells, mu, me, n, ms_sem, mr_sem)

    bhigh, blow = split(jnp.concatenate(
        [sl[0:BASIS], sl[WEIGHT : WEIGHT + 8], jnp.zeros((8, cells), F32)], axis=0
    ))
    bboth = jnp.concatenate([bhigh, blow], axis=0)

    def center(d):
        for i in range(tiles):
            here = slice(i * LANES, (i + 1) * LANES)
            high, low = split(logged[d, :, here] - mu[d, :, here])
            lhi[d, :, here] = high
            llo[d, :, here] = low
        made = product(bhigh, bboth, lhi[d], llo[d], ALONG)
        wb[d] = made[0:BASIS]
        tpart[d] = made[BASIS : BASIS + 1]

    base.launch(center)

    def give(k):
        d = lax.rem(me + k, n)
        along_cells(tpart.at[d], tfrom.at[me], ts_sem.at[k], tr_sem.at[me], d).start()

    loop(1, n, give)

    def cross(d):
        high = vhi[d, 0 : BASIS + BLOCK]
        both = jnp.concatenate([high, vlo[d, 0 : BASIS + BLOCK]], axis=0)
        met = product(high, both, lhi[d], llo[d], ROWS)
        xb0[mine] = xb0[mine] + met[0:BASIS]
        xg[0, mine] = xg[0, mine] + met[BASIS:]

    loop(0, n // 2, cross, 2)
    base.third(0, 1)
    loop(n // 2, n, cross, 2)
    spread(along_genes, xg.at[0], mine, g, xs_sem.at[0], xr_sem.at[0])
    spread(along_genes, xb0, mine, g, b0s_sem, b0r_sem)
    base.third(1, 2)

    loop(n // 2, n, meet, 2)
    spread(along_genes, xs0, mine, g, s0s_sem, s0r_sem)
    near = gathered(along_column, gramz, zi, a, g0zs_sem, g0zr_sem)
    corner = lax.broadcasted_iota(jnp.int32, (LANES, LANES), 0)
    across = lax.broadcasted_iota(jnp.int32, (BASIS, LANES), 1)
    el[...] = jnp.where((same > 0) & (corner >= BASIS), 1.0, 0.0)
    el[0:BASIS] = jnp.where(across < SLOTS, near[0:BASIS], 0.0)
    l1[...], l2[...] = both_sides(el[...], same)
    wsum[...] = near[BASIS:]
    live_total = near[BASIS : BASIS + 1, WEIGHT : WEIGHT + 1]
    inverse = 1.0 / live_total
    factor_scale = lax.rsqrt(live_total)
    factor_scale = factor_scale * (1.5 - 0.5 * live_total * factor_scale * factor_scale)

    def turned(column, start):
        return jnp.sum(jnp.where(lane == row + start, column, 0.0), axis=0, keepdims=True)

    def fresh(d):
        chigh, clow = split(chg[...])
        cboth = jnp.concatenate([chigh, clow], axis=0)
        return product(chigh, cboth, vhi[d], vlo[d], ALONG)

    def emit(d, rows, values):
        values = values * scales[1]
        at = first_gene(d)
        right_out[rows, pl.ds(at, brief)] = values[:, :brief]
        if longs:
            @pl.when(is_long(d))
            def _():
                right_out[rows, pl.ds(pl.multiple_of(at + brief, LANES), LANES)] = values[:, brief:]

    def update(j, start, stop):
        later = pl.multiple_of(BASIS + (j + 1) * BLOCK, BLOCK)
        rows = pl.ds(pl.multiple_of(j * BLOCK, BLOCK), BLOCK)

        def right(d):
            values = fresh(d)
            vhigh, vlow = split(values)
            vhi[d, pl.ds(later, BLOCK)] = vhigh
            vlo[d, pl.ds(later, BLOCK)] = vlow
            emit(d, rows, values)

        loop(start, stop, right)

    def keep(d, values):
        phigh, plow = split(values)
        vhi[d, SLOTS : SLOTS + BLOCK] = phigh
        vlo[d, SLOTS : SLOTS + BLOCK] = plow
        return phigh, jnp.concatenate([phigh, plow], axis=0)

    def begin(j):
        @pl.when(j == 0)
        def _():
            base.third(2, a)
            walk.third(0, 2)

    def step(j, final):
        position = BASIS + j * BLOCK
        position = position if final else pl.multiple_of(position, BLOCK)
        mr[SLOTS : SLOTS + BLOCK] = gathered(along_genes, xg.at[j], mine, g, xs_sem.at[j], xr_sem.at[j]) * weights_row
        vectors = exact(chg[...], mr[...])
        mr[pl.ds(position, BLOCK)] = vectors
        sl[SLOTS : SLOTS + BLOCK] = vectors
        gram[seat] = exact_rows(vectors, sl[...])
        spread(along_plane, gram, seat, 2 * b, gs_sem, gr_sem)
        high, low = split(vectors)
        both = jnp.concatenate([high, low], axis=0)

        def produce(d):
            w[d] = product(high, both, lhi[d], llo[d], ALONG)

        walk.launch(produce)
        gramc[zi] = gathered(along_plane, gram, seat, 2 * b, gs_sem, gr_sem)
        spread(along_column, gramc, zi, a, gcs_sem, gcr_sem)
        if final:
            update(j - 1, 0, n // 4)
            walk.third(0, 1)
            update(j - 1, n // 4, n // 2)
            walk.third(1, 2)
            update(j - 1, n // 2, n)
        else:
            begin(j)

            @pl.when(j > 0)
            def _():
                update(j - 1, 0, n // 4)
                walk.third(0, 1)
                update(j - 1, n // 4, n // 2)
                walk.third(1, 2)
                update(j - 1, n // 2, n)

        total = gathered(along_column, gramc, zi, a, gcs_sem, gcr_sem)
        held = total[:, WEIGHT : WEIGHT + 1] * inverse
        weighed = wsum[0:1] + turned(total[:, WEIGHT : WEIGHT + 1], SLOTS)
        scale = jnp.where(lane < SLOTS, factor_scale, factor_scale * factor_scale)
        factor, against, change = orthonormal((total - held * weighed) * scale, l1[...], l2[...])
        walk.third(2, a - 1)
        diag_out[j] = factor
        tilt = jnp.sum(jnp.where(lane < SLOTS, change * wsum[0:1], 0.0), axis=1, keepdims=True)
        wsum[0:1] = wsum[0:1] + turned(tilt, position)
        shift = jnp.sum(
            jnp.where((lane >= SLOTS) & (lane < WEIGHT), change * turned(held, SLOTS), 0.0), axis=1, keepdims=True
        )
        blend = jnp.where(
            lane < SLOTS, change,
            jnp.where(lane < WEIGHT, change * factor_scale, jnp.where(lane == WEIGHT, -shift * factor_scale, 0.0)),
        )
        leftvec = exact(blend, sl[...])
        sl[pl.ds(position, BLOCK)] = leftvec
        left_out[pl.ds(position - BASIS, BLOCK)] = leftvec * scales[0]
        tilt = tilt * inverse
        blend = jnp.where(lane == WEIGHT, blend - tilt, blend) * factor_scale

        def settle():
            ground[...] = exact(jnp.where((lane < SLOTS) | (lane >= WEIGHT), blend, 0.0), stack[...])

        if final:
            settle()
        else:
            pl.when(j > 0)(settle)
        walk.third(a - 1, a)
        if not final:
            @pl.when(j == 0)
            def _():
                base.fourth(stack, slice(0, BASIS))

                def take(k):
                    source = lax.rem(me + n - k, n)
                    item = along_cells(tpart.at[source], tfrom.at[source], ts_sem.at[k], tr_sem.at[source], sibling)
                    item.wait_send()
                    item.wait_recv()
                    tpart[me] = tpart[me] + tfrom[source]

                loop(1, n, take)
                stack[WEIGHT : WEIGHT + 1] = tpart[me]
                settle()
                mr[0:BASIS] = gathered(along_genes, xb0, mine, g, b0s_sem, b0r_sem) * weights_row

        columns = [jnp.broadcast_to(blend[:, SLOTS + k : SLOTS + k + 1], (BLOCK, LANES)) for k in range(BLOCK)]
        walk.fourth(stack, slice(SLOTS, SLOTS + BLOCK))
        for i in range(tiles):
            here = slice(i * LANES, (i + 1) * LANES)
            values = ground[:, here]
            for k in range(BLOCK):
                values = values + columns[k] * stack[SLOTS + k : SLOTS + k + 1, here]
            pb[me, :, here] = values

        def relay(z):
            t = z * b + yi
            d = 2 * t + core

            def to_y(k):
                y = lax.rem(yi + k, b)
                hop(pb.at[d], pb.at[d], (fs_sem, z * b + y), (cr_sem, d), 2 * (zi * b + y) + core, d)("start")

            loop(1, b, to_y)
            hop(pb.at[d], pb.at[d], (ds_sem, t), (cr_sem, d), sibling, d)("start")

        def arrived(d):
            hop(pb.at[d], pb.at[d], (ds_sem, 0), (cr_sem, d), sibling, d)("wait_recv")

        def go(k):
            z = onward(k)
            hop(pb.at[me], pb.at[me], (cs_sem, z), (cr_sem, me), 2 * (z * b + yi) + core, me)("start")

        if not final:
            loop(1, a, go)
            relay(zi)
        phigh, pboth = keep(me, pb[me])
        square = product(phigh, pboth, vhi[me], vlo[me], ROWS)
        plane = (along_plane, gy, seat, 2 * b, gys_sem, gyr_sem)
        line = (along_genes, gx, mine, g, gxs_sem, gxr_sem)
        column = (along_column, gz, zi, a, gzs_sem, gzr_sem)
        stages = (column, line, plane) if final else (plane, line, column)

        def advance(i):
            copy, buf, at = stages[i][:3]
            buf[at] = gathered(*stages[i - 1]) if i else square
            spread(*stages[i])

        advance(0)
        if final:
            relay(zi)
            loop(1, a, go)
        else:
            stack[pl.ds(position, BLOCK)] = (
                pb[me] * (live_total * factor_scale) + tilt * stack[WEIGHT : WEIGHT + 1]
            )
            xg[j + 1, mine] = jnp.zeros((BLOCK, LANES), F32)
            extend(el, l1, l2, position, against)

        def consume(d):
            phigh, pboth = keep(d, pb[d])
            if final:
                emit(d, pl.ds((STEPS - 1) * BLOCK, BLOCK), fresh(d))
            else:
                xg[j + 1, mine] = xg[j + 1, mine] + product(phigh, pboth, lhi[d], llo[d], ROWS)

        def pass_z(k):
            z = behind(k)
            arrived(2 * (z * b + yi) + core)
            relay(z)

        def own(k):
            consume(2 * (behind(k) * b + yi) + core)

        def pass_y(k):
            z = behind(lax.rem(k, a))
            t = z * b + lax.rem(yi + 1 + k // a, b)
            d = 2 * t + core
            arrived(d)
            hop(pb.at[d], pb.at[d], (ds_sem, t), (cr_sem, d), sibling, d)("start")
            consume(d)

        def rest(k):
            z = behind(lax.rem(k, a))
            t = z * b + lax.rem(yi + k // a, b)
            d = 2 * t + 1 - core
            arrived(d)
            consume(d)

        def early(k):
            if not final:
                own(k)
                rest(k - 1)

        def follow(k):
            pass_z(k)
            early(k)

        met = min(1, h - a)
        if final:
            advance(1)
            loop(1, min(2, a), pass_z)
            advance(2)
            loop(min(2, a), a, pass_z)
        else:
            consume(me)
            loop(1, min(2, a), pass_z)
            loop(1, min(2, a), early)
            advance(1)
            loop(min(2, a), min(3, a), pass_z)
            loop(min(2, a), min(3, a), early)
            loop(0, met, pass_y)
            advance(2)
            loop(min(3, a), a, follow)

        def open_right():
            met = gathered(along_genes, xs0, mine, g, s0s_sem, s0r_sem)
            held = lax.broadcasted_iota(jnp.int32, met.shape, 1) < SLOTS
            er[0 : BASIS + BLOCK] = jnp.where(held, met, 0.0)
            r1[...], r2[...] = both_sides(er[...], same)

        def close():
            if not final:
                pl.when(j == 0)(open_right)
            total = gathered(*stages[2])
            factor, against, change = orthonormal(total, r1[...], r2[...])
            couple_out[j] = factor
            chg[...] = change
            if not final:
                extend(er, r1, r2, position + BLOCK, against)

        if final:
            close()
            consume(me)
            loop(1, a, own)
            loop(0, a, rest)
            loop(0, h - a, pass_y)
        else:
            rest(a - 1)
            loop(met, h - a, pass_y)
        loop(a, h, rest)
        if not final:
            spread(along_genes, xg.at[j + 1], mine, g, xs_sem.at[j + 1], xr_sem.at[j + 1])
            close()
        walk.ended()

        def ended(t):
            hop(pb.at[t], pb.at[t], (ds_sem, t), (cr_sem, t), sibling, 2 * t + core)("wait_send")

        loop(0, h, ended)

        def ended_y(k):
            z, y = order(k)
            t = z * b + y
            hop(pb.at[t], pb.at[t], (fs_sem, t), (cr_sem, t), sibling, 2 * (z * b + yi) + core)("wait_send")

        loop(0, h - a, ended_y)

        def ended_z(k):
            z = lax.rem(zi + k, a)
            hop(pb.at[z], pb.at[z], (cs_sem, z), (cr_sem, z), sibling, me)("wait_send")

        loop(1, a, ended_z)

    loop(0, STEPS - 1, lambda j: step(j, False))
    step(STEPS - 1, True)
    base.ended()


def settle_outputs(left, right, diag, couple, left_out, right_out, diag_out, couple_out, went):
    items = [
        pltpu.make_async_copy(src, dst, went.at[i])
        for i, (src, dst) in enumerate(
            [(right, right_out), (left, left_out), (diag, diag_out), (couple, couple_out)]
        )
    ]
    for item in items:
        item.start()
    for item in items:
        item.wait()


def body(counts, live_rows, left_basis, right_basis, right_start):
    cells, genes = counts.shape
    n = lax.axis_size("cells")
    g = lax.axis_size("genes")
    h = n // 2
    a, b = grid(h)
    brief, longs = chunks(n, genes)
    width = (brief + (1 if longs else 0)) * LANES
    scales = (math.sqrt(float(cells * n)), math.sqrt(float(genes * g)))
    vmem = pl.BlockSpec(memory_space=pltpu.VMEM)
    anywhere = pl.BlockSpec(memory_space=pl.ANY)
    held = lambda *shape: pltpu.VMEM(shape, F32)
    square = held(LANES, LANES)
    dma = lambda *shape: pltpu.SemaphoreType.DMA(shape)
    out_shape = (
        jax.ShapeDtypeStruct((STEPS * BLOCK, cells), F32),
        jax.ShapeDtypeStruct((STEPS * BLOCK, genes), F32),
        jax.ShapeDtypeStruct((STEPS, BLOCK, BLOCK), F32),
        jax.ShapeDtypeStruct((STEPS, BLOCK, BLOCK), F32),
    )
    buffers = lambda rows: [
        held(n, rows, width), held(h, rows, width), held(h, rows, width), held(h, rows, width),
    ]
    scratch = [
        pltpu.VMEM((n, cells, width), jnp.int32),
        held(n, cells, width),
        *[pltpu.VMEM((n, cells, width), BF16)] * 2,
        *[pltpu.VMEM((n, LANES, width), BF16)] * 2,
        held(n, BASIS + BLOCK, width),
        *[square] * 8,
        *buffers(BLOCK),
        *buffers(BASIS),
        held(n, BLOCK, width),
        held(LANES, width),
        held(BLOCK, width),
        held(n, 1, width),
        held(n, 1, width),
        held(n, 1, width),
        held(8, LANES),
        held(BLOCK, LANES),
        held(2 * b, BASIS + 8, LANES),
        held(a, BASIS + 8, LANES),
        held(2 * b, BLOCK, LANES),
        held(a, BLOCK, LANES),
        held(g, BASIS + BLOCK, LANES),
        held(g, BASIS, LANES),
        held(STEPS, g, BLOCK, LANES),
        held(g, BLOCK, LANES),
        held(2 * b, BLOCK, LANES),
        held(a, BLOCK, LANES),
        dma(n, 3, 2),
        *[dma(2, h)] * 12,
        dma(2, h), dma(2, n), dma(2, h), dma(2, h), dma(n), dma(n),
        dma(n), dma(n),
        *[dma(2 * b), dma(2 * b), dma(a), dma(a)] * 2,
        *[dma(g)] * 4,
        dma(STEPS, g), dma(STEPS, g),
        dma(g), dma(g), dma(2 * b), dma(2 * b), dma(a), dma(a),
    ]
    results = pl.pallas_call(
        functools.partial(kernel, n, g, width, scales),
        out_shape=tuple(pltpu.VMEM(item.shape, F32) for item in out_shape),
        in_specs=[pl.BlockSpec(memory_space=pltpu.SMEM), anywhere, vmem, anywhere, anywhere],
        out_specs=(vmem, vmem, vmem, vmem),
        scratch_shapes=scratch,
        compiler_params=pltpu.CompilerParams(
            collective_id=0, has_side_effects=True, vmem_limit_bytes=60 * 1000 * 1000
        ),
    )(live_rows, counts, left_basis, right_basis, right_start)
    return pl.pallas_call(
        settle_outputs,
        out_shape=out_shape,
        in_specs=[vmem] * 4,
        out_specs=(anywhere,) * 4,
        scratch_shapes=[dma(4)],
    )(*[pltpu.with_memory_space_constraint(item, pltpu.VMEM) for item in results])


def solution(mesh):
    in_specs = (
        P("cells", "genes"),
        P("cells"),
        P(None, "cells"),
        P(None, "genes"),
        P(None, "genes"),
    )
    out_specs = (P(None, "cells"), P(None, "genes"), P(), P())
    return jax.shard_map(body, mesh=mesh, in_specs=in_specs, out_specs=out_specs, check_vma=False)
```

```python
import functools
import math

import jax
import jax.numpy as jnp
from jax import lax
from jax.experimental import pallas as pl
from jax.experimental.pallas import tpu as pltpu
from jax.sharding import PartitionSpec as P

BASIS = 32
BLOCK = 16
STEPS = 3
SLOTS = BASIS + STEPS * BLOCK
WEIGHT = SLOTS + BLOCK
LAG = 3
LANES = 128
F32 = jnp.float32
BF16 = jnp.bfloat16
HIGHEST = lax.Precision.HIGHEST
MESH = pl.DeviceIdType.MESH


def exact(lhs, rhs):
    return jnp.dot(lhs, rhs, precision=HIGHEST, preferred_element_type=F32)


def exact_rows(lhs, rhs):
    return lax.dot_general(
        lhs, rhs, (((1,), (1,)), ((), ())), precision=HIGHEST, preferred_element_type=F32
    )


def split(values):
    high = values.astype(BF16)
    return high, (values - high.astype(F32)).astype(BF16)


def product(high, both, rhs_high, rhs_low, dims):
    rows = high.shape[0]
    first = lax.dot_general(both, rhs_high, (dims, ((), ())), preferred_element_type=F32)
    second = lax.dot_general(high, rhs_low, (dims, ((), ())), preferred_element_type=F32)
    return first[:rows] + (first[rows:] + second)


ALONG = ((1,), (0,))
ROWS = ((1,), (1,))


def loop(start, stop, step, unroll=1):
    def one(k, carry):
        step(k)
        return carry

    lax.fori_loop(start, stop, one, 0, unroll=unroll if (stop - start) % unroll == 0 else 1)


def both_sides(gram, identity):
    gap = identity - gram
    return identity + gap, exact(gap, gap)


def orthonormal(gram, first, second):
    lane = lax.broadcasted_iota(jnp.int32, (BLOCK, LANES), 1)
    row = lax.broadcasted_iota(jnp.int32, (BLOCK, LANES), 0)
    coeffs = jnp.where(lane < SLOTS, gram, 0.0)
    combined = exact(coeffs, first)
    residue = exact(coeffs, second)
    squares = gram[:, SLOTS : SLOTS + BLOCK] - exact_rows(
        jnp.concatenate([combined, residue], axis=1), jnp.concatenate([coeffs, combined], axis=1)
    )
    change = jnp.where(lane == row + SLOTS, 1.0, -combined)
    columns = [jnp.broadcast_to(squares[:, k : k + 1], (BLOCK, LANES)) for k in range(BLOCK)]
    factor = jnp.zeros((BLOCK, LANES), F32)
    for k in range(BLOCK):
        pivot = jnp.broadcast_to(columns[k][k : k + 1], (BLOCK, LANES))
        root = lax.rsqrt(pivot)
        root = root * (1.5 - 0.5 * pivot * root * root)
        column = columns[k] * root
        factor = jnp.where((lane == k) & (row >= k), column, factor)
        below = jnp.where(row > k, column, 0.0)
        for i in range(k + 1, BLOCK):
            columns[i] = columns[i] - column * jnp.broadcast_to(column[i : i + 1], (BLOCK, LANES))
        scaled = jnp.broadcast_to(residue[k : k + 1], (BLOCK, LANES)) * root
        residue = jnp.where(row == k, scaled, residue - below * scaled)
        scaled = jnp.broadcast_to(change[k : k + 1], (BLOCK, LANES)) * root
        change = jnp.where(row == k, scaled, change - below * scaled)
    return factor[:, :BLOCK], residue, change


def grid(h):
    b = 1 << ((h.bit_length() - 1) // 2)
    b = b if h % b == 0 else 1
    return h // b, b


def chunks(n, genes):
    brief, extra = divmod(genes // LANES, n)
    stride = n // extra if extra else n
    return brief, [i * stride + (2 * (i % 2) if stride > 3 else 0) for i in range(extra)]


def kernel(
    n, g, width, scales,
    live, counts, left_basis, right_basis, right_start,
    left_out, right_out, diag_out, couple_out,
    cnt, logged, lhi, llo, vhi, vlo, rb, sl, mr, el, er, l1, l2, r1, r2,
    w, ra, rt, rz, wb, rab, rtb, rzb, pb, stack, ground, tpart, tfrom,
    mu, wsum, chg, gram0, gramz, gram, gramc, xs0, xb0, xg, gx, gy, gz,
    in_sem, as_sem, ar_sem, bs_sem, br_sem, zs_sem, zr_sem,
    bas_sem, bar_sem, bbs_sem, bbr_sem, bzs_sem, bzr_sem,
    cs_sem, cr_sem, ds_sem, fs_sem, ts_sem, tr_sem,
    ms_sem, mr_sem, g0s_sem, g0r_sem, g0zs_sem, g0zr_sem, gs_sem, gr_sem, gcs_sem, gcr_sem, s0s_sem, s0r_sem, b0s_sem, b0r_sem,
    xs_sem, xr_sem, gxs_sem, gxr_sem, gys_sem, gyr_sem, gzs_sem, gzr_sem,
):
    cells, genes = counts.shape
    me = lax.axis_index("cells")
    mine = lax.axis_index("genes")
    core = lax.rem(me, 2)
    chip = me // 2
    h = n // 2
    a, b = grid(h)
    zi, yi = chip // b, lax.rem(chip, b)
    sibling = me + 1 - 2 * core
    seat = 2 * yi + core
    tiles = width // LANES
    brief, longs = chunks(n, genes)
    brief = brief * LANES
    lane = lax.broadcasted_iota(jnp.int32, (BLOCK, LANES), 1)
    row = lax.broadcasted_iota(jnp.int32, (BLOCK, LANES), 0)

    def along_cells(src, dst, send, recv, peer):
        return pltpu.make_async_remote_copy(
            src_ref=src, dst_ref=dst, send_sem=send, recv_sem=recv,
            device_id=(peer, mine), device_id_type=MESH,
        )

    def along_genes(src, dst, send, recv, peer):
        return pltpu.make_async_remote_copy(
            src_ref=src, dst_ref=dst, send_sem=send, recv_sem=recv,
            device_id=(me, peer), device_id_type=MESH,
        )

    def along_plane(src, dst, send, recv, peer):
        return along_cells(src, dst, send, recv, 2 * b * zi + peer)

    def along_column(src, dst, send, recv, peer):
        return along_cells(src, dst, send, recv, 2 * (peer * b + yi) + core)

    def is_long(d):
        found = d == longs[0]
        for other in longs[1:]:
            found = found | (d == other)
        return found

    def first_gene(d):
        at = d * brief
        for other in longs:
            at = at + jnp.where(d > other, LANES, 0)
        return pl.multiple_of(at, LANES)

    def fill_in(d, kind, method):
        here, there, rows = (
            (counts, cnt, pl.ds(0, cells)), (right_basis, rb, pl.ds(0, BASIS)), (right_start, rb, pl.ds(BASIS, BLOCK)),
        )[kind]
        at = first_gene(d)
        getattr(pltpu.make_async_copy(
            here.at[:, pl.ds(at, brief)], there.at[d, rows, pl.ds(0, brief)], in_sem.at[d, kind, 0]
        ), method)()
        if longs:
            @pl.when(is_long(d))
            def _():
                getattr(pltpu.make_async_copy(
                    here.at[:, pl.ds(pl.multiple_of(at + brief, LANES), LANES)],
                    there.at[d, rows, pl.ds(brief, LANES)], in_sem.at[d, kind, 1],
                ), method)()

    def hop(src, dst, send, recv, peer, d):
        def act(method):
            getattr(along_cells(
                src.at[:, pl.ds(0, brief)], dst.at[:, pl.ds(0, brief)],
                send[0].at[0, send[1]], recv[0].at[0, recv[1]], peer,
            ), method)()
            if longs:
                @pl.when(is_long(d))
                def _():
                    getattr(along_cells(
                        src.at[:, pl.ds(brief, LANES)], dst.at[:, pl.ds(brief, LANES)],
                        send[0].at[1, send[1]], recv[0].at[1, recv[1]], peer,
                    ), method)()

        return act

    def around(k):
        return lax.rem(me + k, n)

    loop(0, n, lambda k: fill_in(around(k), 0, "start"))

    def more(k):
        fill_in(around(k), 1, "start")
        fill_in(around(k), 2, "start")

    loop(0, n, more)
    if longs:
        for d in range(n):
            if d not in longs:
                cnt[d, :, brief:] = jnp.zeros((cells, LANES), jnp.int32)
                rb[d, :, brief:] = jnp.zeros((BASIS + BLOCK, LANES), F32)
        for table in (ra, rt, rz, rab, rtb, rzb, pb):
            table[:, :, brief:] = jnp.zeros((table.shape[0], table.shape[1], LANES), F32)

    barrier = pltpu.get_barrier_semaphore()

    def greet_cells(k):
        pl.semaphore_signal(barrier, inc=1, device_id=(lax.rem(me + k, n), mine), device_id_type=MESH)

    def greet_genes(k):
        pl.semaphore_signal(barrier, inc=1, device_id=(me, lax.rem(mine + k, g)), device_id_type=MESH)

    loop(1, n, greet_cells)
    loop(1, g, greet_genes)

    def spread(copy, buf, at, size, send, recv):
        def go(k):
            copy(buf.at[at], buf.at[at], send.at[k], recv.at[at], lax.rem(at + k, size)).start()

        loop(1, size, go)

    def waited(copy, buf, at, size, send, recv):
        def end(k):
            source = lax.rem(at + size - k, size)
            item = copy(buf.at[source], buf.at[source], send.at[k], recv.at[source], lax.rem(at + k, size))
            item.wait_send()
            item.wait_recv()

        loop(1, size, end)

    def gathered(copy, buf, at, size, send, recv):
        waited(copy, buf, at, size, send, recv)
        return lax.fori_loop(
            1, size, lambda k, total: total + buf[k], buf[0]
        )

    def onward(k):
        return lax.rem(zi + k, a)

    def behind(k):
        return lax.rem(zi + a - k, a)

    def order(k):
        return onward(1 + lax.rem(k, a)), lax.rem(yi + 1 + k // a, b)

    class Scatter:
        def __init__(self, part, fromcore, fromy, fromz, sems):
            self.part, self.fromcore, self.fromy, self.fromz = part, fromcore, fromy, fromz
            self.cs, self.cr, self.ys, self.yr, self.zs, self.zr = sems

        def over(self, d, t):
            return hop(self.part.at[d], self.fromcore.at[t], (self.cs, t), (self.cr, t), sibling, d)

        def launch(self, produce):
            def other(k):
                z, y = order(k)
                t = z * b + y
                return t, 2 * t + 1 - core

            def own(k):
                z, y = order(k)
                t = z * b + y
                return z, y, t, 2 * t + core

            def join(k):
                z, y, t, d = own(k)
                self.over(d, t)("wait_recv")
                self.part[d] = self.part[d] + self.fromcore[t]

                @pl.when(k < h - a)
                def _():
                    to = z * b + yi
                    hop(
                        self.part.at[d], self.fromy.at[to], (self.ys, t), (self.yr, to),
                        2 * (zi * b + y) + core, d,
                    )("start")

            def pair(k):
                t, d = other(k)
                produce(d)
                produce(own(k)[3])
                self.over(d, t)("start")

            def one(k):
                pair(k)
                join(k - lag)

            lag = min(LAG, h)
            loop(0, lag, pair)
            loop(lag, h, one)
            loop(h - lag, h, join)

        def complete(self, z):
            d = 2 * (z * b + yi) + core

            def add(k):
                source = z * b + lax.rem(yi + k, b)
                hop(self.part.at[d], self.fromy.at[source], (self.ys, source), (self.yr, source), sibling, d)("wait_recv")
                self.part[d] = self.part[d] + self.fromy[source]

            loop(1, b, add)
            return d

        def third(self, start, stop):
            def one(k):
                z = onward(1 + k)
                d = self.complete(z)
                hop(self.part.at[d], self.fromz.at[zi], (self.zs, z), (self.zr, zi), d, d)("start")

            loop(min(start, a - 1), min(stop, a - 1), one)
            if stop >= a:
                self.complete(zi)

        def fourth(self, result, rows):
            result[rows] = self.part[me]

            def one(k):
                z = behind(k)
                hop(self.part.at[me], self.fromz.at[z], (self.zs, z), (self.zr, z), sibling, me)("wait_recv")
                result[rows] = result[rows] + self.fromz[z]

            loop(1, a, one)

        def ended(self):
            loop(0, h, lambda t: self.over(2 * t + 1 - core, t)("wait_send"))

            def sent_y(k):
                z, y = order(k)
                t = z * b + y
                hop(self.part.at[t], self.fromy.at[t], (self.ys, t), (self.yr, t), sibling, 2 * t + core)("wait_send")

            loop(0, h - a, sent_y)

            def sent_z(k):
                z = lax.rem(zi + k, a)
                d = 2 * (z * b + yi) + core
                hop(self.part.at[z], self.fromz.at[z], (self.zs, z), (self.zr, z), sibling, d)("wait_send")

            loop(1, a, sent_z)

    walk = Scatter(w, ra, rt, rz, (as_sem, ar_sem, bs_sem, br_sem, zs_sem, zr_sem))
    base = Scatter(wb, rab, rtb, rzb, (bas_sem, bar_sem, bbs_sem, bbr_sem, bzs_sem, bzr_sem))

    live_here = live[0]
    weights_row = jnp.where(
        lax.broadcasted_iota(jnp.int32, (1, cells), 1) < live_here, 1.0, 0.0
    ).astype(F32)
    weights = jnp.where(
        lax.broadcasted_iota(jnp.int32, (cells, LANES), 0) < live_here, 1.0, 0.0
    ).astype(F32)
    for table in (sl, mr, stack):
        table[...] = jnp.zeros_like(table)
    same = jnp.where(
        lax.broadcasted_iota(jnp.int32, (LANES, LANES), 0)
        == lax.broadcasted_iota(jnp.int32, (LANES, LANES), 1),
        1.0, 0.0,
    ).astype(F32)
    er[...] = same
    chg[...] = jnp.where(lane == row + SLOTS, 1.0, 0.0)

    def extend(table, first, second, position, against):
        here = jnp.where(lane == row + position, 1.0, 0.0).astype(F32)
        turn = lambda lhs, rhs: lax.dot_general(
            lhs, rhs, (((0,), (0,)), ((), ())), precision=HIGHEST, preferred_element_type=F32
        )
        table[...] = table[...] + turn(here, against) + turn(against, here)
        first[...], second[...] = both_sides(table[...], same)
    sl[0:BASIS] = left_basis[...] * weights_row
    sl[WEIGHT : WEIGHT + 8] = jnp.where(
        lax.broadcasted_iota(jnp.int32, (8, cells), 0) == 0, weights_row, 0.0
    )
    gram0[seat, 0:BASIS] = exact_rows(sl[0:BASIS], sl[...])
    gram0[seat, BASIS:] = exact_rows(sl[WEIGHT : WEIGHT + 8], sl[...])

    def take_log(d):
        for i in range(tiles):
            here = slice(i * LANES, (i + 1) * LANES)
            logged[d, :, here] = jnp.log(1.0 + cnt[d, :, here].astype(F32))

    fill_in(me, 0, "wait")
    take_log(me)
    portion = 1.0 / jnp.maximum(live_here, 1).astype(F32)
    for i in range(tiles):
        here = slice(i * LANES, (i + 1) * LANES)
        mu[me, :, here] = jnp.sum(logged[me, :, here] * weights, axis=0, keepdims=True) * portion
    def next_log(k):
        fill_in(around(k), 0, "wait")
        take_log(around(k))

    loop(1, n, next_log)
    pl.semaphore_wait(barrier, n - 1 + g - 1)
    spread(along_cells, mu, me, n, ms_sem, mr_sem)
    spread(along_plane, gram0, seat, 2 * b, g0s_sem, g0r_sem)

    xs0[mine] = jnp.zeros((BASIS + BLOCK, LANES), F32)
    xb0[mine] = jnp.zeros((BASIS, LANES), F32)
    xg[0, mine] = jnp.zeros((BLOCK, LANES), F32)

    def fill(k):
        d = around(k)
        fill_in(d, 1, "wait")
        fill_in(d, 2, "wait")
        high, low = split(rb[d])
        vhi[d, 0 : BASIS + BLOCK] = high
        vlo[d, 0 : BASIS + BLOCK] = low
        blank = jnp.zeros((LANES - BASIS - BLOCK, width), BF16)
        vhi[d, BASIS + BLOCK :] = blank
        vlo[d, BASIS + BLOCK :] = blank

    loop(0, n, fill)
    def meet(d):
        high = vhi[d, 0 : BASIS + BLOCK]
        both = jnp.concatenate([high, vlo[d, 0 : BASIS + BLOCK]], axis=0)
        xs0[mine] = xs0[mine] + product(high, both, vhi[d], vlo[d], ROWS)

    loop(0, n // 2, meet, 4)
    gramz[zi] = gathered(along_plane, gram0, seat, 2 * b, g0s_sem, g0r_sem)
    spread(along_column, gramz, zi, a, g0zs_sem, g0zr_sem)
    waited(along_cells, mu, me, n, ms_sem, mr_sem)

    bhigh, blow = split(jnp.concatenate(
        [sl[0:BASIS], sl[WEIGHT : WEIGHT + 8], jnp.zeros((8, cells), F32)], axis=0
    ))
    bboth = jnp.concatenate([bhigh, blow], axis=0)

    def center(d):
        for i in range(tiles):
            here = slice(i * LANES, (i + 1) * LANES)
            high, low = split(logged[d, :, here] - mu[d, :, here])
            lhi[d, :, here] = high
            llo[d, :, here] = low
        made = product(bhigh, bboth, lhi[d], llo[d], ALONG)
        wb[d] = made[0:BASIS]
        tpart[d] = made[BASIS : BASIS + 1]

    base.launch(center)

    def give(k):
        d = lax.rem(me + k, n)
        along_cells(tpart.at[d], tfrom.at[me], ts_sem.at[k], tr_sem.at[me], d).start()

    loop(1, n, give)

    def cross(d):
        high = vhi[d, 0 : BASIS + BLOCK]
        both = jnp.concatenate([high, vlo[d, 0 : BASIS + BLOCK]], axis=0)
        met = product(high, both, lhi[d], llo[d], ROWS)
        xb0[mine] = xb0[mine] + met[0:BASIS]
        xg[0, mine] = xg[0, mine] + met[BASIS:]

    loop(0, n // 2, cross, 4)
    base.third(0, 1)
    loop(n // 2, n, cross, 4)
    spread(along_genes, xg.at[0], mine, g, xs_sem.at[0], xr_sem.at[0])
    spread(along_genes, xb0, mine, g, b0s_sem, b0r_sem)
    base.third(1, 2)

    loop(n // 2, n, meet, 4)
    spread(along_genes, xs0, mine, g, s0s_sem, s0r_sem)
    near = gathered(along_column, gramz, zi, a, g0zs_sem, g0zr_sem)
    corner = lax.broadcasted_iota(jnp.int32, (LANES, LANES), 0)
    across = lax.broadcasted_iota(jnp.int32, (BASIS, LANES), 1)
    el[...] = jnp.where((same > 0) & (corner >= BASIS), 1.0, 0.0)
    el[0:BASIS] = jnp.where(across < SLOTS, near[0:BASIS], 0.0)
    l1[...], l2[...] = both_sides(el[...], same)
    wsum[...] = near[BASIS:]
    live_total = near[BASIS : BASIS + 1, WEIGHT : WEIGHT + 1]
    inverse = 1.0 / live_total
    factor_scale = lax.rsqrt(live_total)
    factor_scale = factor_scale * (1.5 - 0.5 * live_total * factor_scale * factor_scale)

    def turned(column, start):
        return jnp.sum(jnp.where(lane == row + start, column, 0.0), axis=0, keepdims=True)

    def fresh(d):
        chigh, clow = split(chg[...])
        cboth = jnp.concatenate([chigh, clow], axis=0)
        return product(chigh, cboth, vhi[d], vlo[d], ALONG)

    def emit(d, rows, values):
        values = values * scales[1]
        at = first_gene(d)
        right_out[rows, pl.ds(at, brief)] = values[:, :brief]
        if longs:
            @pl.when(is_long(d))
            def _():
                right_out[rows, pl.ds(pl.multiple_of(at + brief, LANES), LANES)] = values[:, brief:]

    def update(j, start, stop):
        later = pl.multiple_of(BASIS + (j + 1) * BLOCK, BLOCK)
        rows = pl.ds(pl.multiple_of(j * BLOCK, BLOCK), BLOCK)

        def right(d):
            values = fresh(d)
            vhigh, vlow = split(values)
            vhi[d, pl.ds(later, BLOCK)] = vhigh
            vlo[d, pl.ds(later, BLOCK)] = vlow
            emit(d, rows, values)

        loop(start, stop, right)

    def keep(d, values):
        phigh, plow = split(values)
        vhi[d, SLOTS : SLOTS + BLOCK] = phigh
        vlo[d, SLOTS : SLOTS + BLOCK] = plow
        return phigh, jnp.concatenate([phigh, plow], axis=0)

    def begin(j):
        @pl.when(j == 0)
        def _():
            base.third(2, a)
            walk.third(0, 2)

    def step(j, final):
        position = BASIS + j * BLOCK
        position = position if final else pl.multiple_of(position, BLOCK)
        mr[SLOTS : SLOTS + BLOCK] = gathered(along_genes, xg.at[j], mine, g, xs_sem.at[j], xr_sem.at[j]) * weights_row
        vectors = exact(chg[...], mr[...])
        mr[pl.ds(position, BLOCK)] = vectors
        sl[SLOTS : SLOTS + BLOCK] = vectors
        gram[seat] = exact_rows(vectors, sl[...])
        spread(along_plane, gram, seat, 2 * b, gs_sem, gr_sem)
        high, low = split(vectors)
        both = jnp.concatenate([high, low], axis=0)

        def produce(d):
            w[d] = product(high, both, lhi[d], llo[d], ALONG)

        walk.launch(produce)
        gramc[zi] = gathered(along_plane, gram, seat, 2 * b, gs_sem, gr_sem)
        spread(along_column, gramc, zi, a, gcs_sem, gcr_sem)
        if final:
            update(j - 1, 0, n // 4)
            walk.third(0, 1)
            update(j - 1, n // 4, n // 2)
            walk.third(1, 2)
            update(j - 1, n // 2, n)
        else:
            begin(j)

            @pl.when(j > 0)
            def _():
                update(j - 1, 0, n // 4)
                walk.third(0, 1)
                update(j - 1, n // 4, n // 2)
                walk.third(1, 2)
                update(j - 1, n // 2, n)

        total = gathered(along_column, gramc, zi, a, gcs_sem, gcr_sem)
        held = total[:, WEIGHT : WEIGHT + 1] * inverse
        weighed = wsum[0:1] + turned(total[:, WEIGHT : WEIGHT + 1], SLOTS)
        scale = jnp.where(lane < SLOTS, factor_scale, factor_scale * factor_scale)
        factor, against, change = orthonormal((total - held * weighed) * scale, l1[...], l2[...])
        walk.third(2, a - 1)
        diag_out[j] = factor
        tilt = jnp.sum(jnp.where(lane < SLOTS, change * wsum[0:1], 0.0), axis=1, keepdims=True)
        wsum[0:1] = wsum[0:1] + turned(tilt, position)
        shift = jnp.sum(
            jnp.where((lane >= SLOTS) & (lane < WEIGHT), change * turned(held, SLOTS), 0.0), axis=1, keepdims=True
        )
        blend = jnp.where(
            lane < SLOTS, change,
            jnp.where(lane < WEIGHT, change * factor_scale, jnp.where(lane == WEIGHT, -shift * factor_scale, 0.0)),
        )
        leftvec = exact(blend, sl[...])
        sl[pl.ds(position, BLOCK)] = leftvec
        left_out[pl.ds(position - BASIS, BLOCK)] = leftvec * scales[0]
        tilt = tilt * inverse
        blend = jnp.where(lane == WEIGHT, blend - tilt, blend) * factor_scale

        def settle():
            ground[...] = exact(jnp.where((lane < SLOTS) | (lane >= WEIGHT), blend, 0.0), stack[...])

        if final:
            settle()
        else:
            pl.when(j > 0)(settle)
        walk.third(a - 1, a)
        if not final:
            @pl.when(j == 0)
            def _():
                base.fourth(stack, slice(0, BASIS))

                def take(k):
                    source = lax.rem(me + n - k, n)
                    item = along_cells(tpart.at[source], tfrom.at[source], ts_sem.at[k], tr_sem.at[source], sibling)
                    item.wait_send()
                    item.wait_recv()
                    tpart[me] = tpart[me] + tfrom[source]

                loop(1, n, take)
                stack[WEIGHT : WEIGHT + 1] = tpart[me]
                settle()
                mr[0:BASIS] = gathered(along_genes, xb0, mine, g, b0s_sem, b0r_sem) * weights_row

        columns = [jnp.broadcast_to(blend[:, SLOTS + k : SLOTS + k + 1], (BLOCK, LANES)) for k in range(BLOCK)]
        walk.fourth(stack, slice(SLOTS, SLOTS + BLOCK))
        for i in range(tiles):
            here = slice(i * LANES, (i + 1) * LANES)
            values = ground[:, here]
            for k in range(BLOCK):
                values = values + columns[k] * stack[SLOTS + k : SLOTS + k + 1, here]
            pb[me, :, here] = values

        def relay(z):
            t = z * b + yi
            d = 2 * t + core

            def to_y(k):
                y = lax.rem(yi + k, b)
                hop(pb.at[d], pb.at[d], (fs_sem, z * b + y), (cr_sem, d), 2 * (zi * b + y) + core, d)("start")

            loop(1, b, to_y)
            hop(pb.at[d], pb.at[d], (ds_sem, t), (cr_sem, d), sibling, d)("start")

        def arrived(d):
            hop(pb.at[d], pb.at[d], (ds_sem, 0), (cr_sem, d), sibling, d)("wait_recv")

        def go(k):
            z = onward(k)
            hop(pb.at[me], pb.at[me], (cs_sem, z), (cr_sem, me), 2 * (z * b + yi) + core, me)("start")

        if not final:
            loop(1, a, go)
            relay(zi)
        phigh, pboth = keep(me, pb[me])
        square = product(phigh, pboth, vhi[me], vlo[me], ROWS)
        plane = (along_plane, gy, seat, 2 * b, gys_sem, gyr_sem)
        line = (along_genes, gx, mine, g, gxs_sem, gxr_sem)
        column = (along_column, gz, zi, a, gzs_sem, gzr_sem)
        stages = (column, line, plane) if final else (plane, line, column)

        def advance(i):
            copy, buf, at = stages[i][:3]
            buf[at] = gathered(*stages[i - 1]) if i else square
            spread(*stages[i])

        advance(0)
        if final:
            relay(zi)
            loop(1, a, go)
        else:
            stack[pl.ds(position, BLOCK)] = (
                pb[me] * (live_total * factor_scale) + tilt * stack[WEIGHT : WEIGHT + 1]
            )
            xg[j + 1, mine] = jnp.zeros((BLOCK, LANES), F32)
            extend(el, l1, l2, position, against)

        def consume(d):
            phigh, pboth = keep(d, pb[d])
            if final:
                emit(d, pl.ds((STEPS - 1) * BLOCK, BLOCK), fresh(d))
            else:
                xg[j + 1, mine] = xg[j + 1, mine] + product(phigh, pboth, lhi[d], llo[d], ROWS)

        def pass_z(k):
            z = behind(k)
            arrived(2 * (z * b + yi) + core)
            relay(z)

        def own(k):
            consume(2 * (behind(k) * b + yi) + core)

        def pass_y(k):
            z = behind(lax.rem(k, a))
            t = z * b + lax.rem(yi + 1 + k // a, b)
            d = 2 * t + core
            arrived(d)
            hop(pb.at[d], pb.at[d], (ds_sem, t), (cr_sem, d), sibling, d)("start")
            consume(d)

        def rest(k):
            z = behind(lax.rem(k, a))
            t = z * b + lax.rem(yi + k // a, b)
            d = 2 * t + 1 - core
            arrived(d)
            consume(d)

        def early(k):
            if not final:
                own(k)
                rest(k - 1)

        def follow(k):
            pass_z(k)
            early(k)

        met = min(1, h - a)
        if final:
            advance(1)
            loop(1, min(2, a), pass_z)
            advance(2)
            loop(min(2, a), a, pass_z)
        else:
            consume(me)
            loop(1, min(2, a), pass_z)
            loop(1, min(2, a), early)
            advance(1)
            loop(min(2, a), min(3, a), pass_z)
            loop(min(2, a), min(3, a), early)
            loop(0, met, pass_y)
            advance(2)
            loop(min(3, a), a, follow)

        def open_right():
            met = gathered(along_genes, xs0, mine, g, s0s_sem, s0r_sem)
            held = lax.broadcasted_iota(jnp.int32, met.shape, 1) < SLOTS
            er[0 : BASIS + BLOCK] = jnp.where(held, met, 0.0)
            r1[...], r2[...] = both_sides(er[...], same)

        def close():
            if not final:
                pl.when(j == 0)(open_right)
            total = gathered(*stages[2])
            factor, against, change = orthonormal(total, r1[...], r2[...])
            couple_out[j] = factor
            chg[...] = change
            if not final:
                extend(er, r1, r2, position + BLOCK, against)

        if final:
            close()
            consume(me)
            loop(1, a, own)
            loop(0, a, rest)
            loop(0, h - a, pass_y)
        else:
            rest(a - 1)
            loop(met, h - a, pass_y)
        loop(a, h, rest)
        if not final:
            spread(along_genes, xg.at[j + 1], mine, g, xs_sem.at[j + 1], xr_sem.at[j + 1])
            close()
        walk.ended()

        def ended(t):
            hop(pb.at[t], pb.at[t], (ds_sem, t), (cr_sem, t), sibling, 2 * t + core)("wait_send")

        loop(0, h, ended)

        def ended_y(k):
            z, y = order(k)
            t = z * b + y
            hop(pb.at[t], pb.at[t], (fs_sem, t), (cr_sem, t), sibling, 2 * (z * b + yi) + core)("wait_send")

        loop(0, h - a, ended_y)

        def ended_z(k):
            z = lax.rem(zi + k, a)
            hop(pb.at[z], pb.at[z], (cs_sem, z), (cr_sem, z), sibling, me)("wait_send")

        loop(1, a, ended_z)

    loop(0, STEPS - 1, lambda j: step(j, False))
    step(STEPS - 1, True)
    base.ended()


def settle_outputs(left, right, diag, couple, left_out, right_out, diag_out, couple_out, went):
    items = [
        pltpu.make_async_copy(src, dst, went.at[i])
        for i, (src, dst) in enumerate(
            [(right, right_out), (left, left_out), (diag, diag_out), (couple, couple_out)]
        )
    ]
    for item in items:
        item.start()
    for item in items:
        item.wait()


def body(counts, live_rows, left_basis, right_basis, right_start):
    cells, genes = counts.shape
    n = lax.axis_size("cells")
    g = lax.axis_size("genes")
    h = n // 2
    a, b = grid(h)
    brief, longs = chunks(n, genes)
    width = (brief + (1 if longs else 0)) * LANES
    scales = (math.sqrt(float(cells * n)), math.sqrt(float(genes * g)))
    vmem = pl.BlockSpec(memory_space=pltpu.VMEM)
    anywhere = pl.BlockSpec(memory_space=pl.ANY)
    held = lambda *shape: pltpu.VMEM(shape, F32)
    square = held(LANES, LANES)
    dma = lambda *shape: pltpu.SemaphoreType.DMA(shape)
    out_shape = (
        jax.ShapeDtypeStruct((STEPS * BLOCK, cells), F32),
        jax.ShapeDtypeStruct((STEPS * BLOCK, genes), F32),
        jax.ShapeDtypeStruct((STEPS, BLOCK, BLOCK), F32),
        jax.ShapeDtypeStruct((STEPS, BLOCK, BLOCK), F32),
    )
    buffers = lambda rows: [
        held(n, rows, width), held(h, rows, width), held(h, rows, width), held(h, rows, width),
    ]
    scratch = [
        pltpu.VMEM((n, cells, width), jnp.int32),
        held(n, cells, width),
        *[pltpu.VMEM((n, cells, width), BF16)] * 2,
        *[pltpu.VMEM((n, LANES, width), BF16)] * 2,
        held(n, BASIS + BLOCK, width),
        *[square] * 8,
        *buffers(BLOCK),
        *buffers(BASIS),
        held(n, BLOCK, width),
        held(LANES, width),
        held(BLOCK, width),
        held(n, 1, width),
        held(n, 1, width),
        held(n, 1, width),
        held(8, LANES),
        held(BLOCK, LANES),
        held(2 * b, BASIS + 8, LANES),
        held(a, BASIS + 8, LANES),
        held(2 * b, BLOCK, LANES),
        held(a, BLOCK, LANES),
        held(g, BASIS + BLOCK, LANES),
        held(g, BASIS, LANES),
        held(STEPS, g, BLOCK, LANES),
        held(g, BLOCK, LANES),
        held(2 * b, BLOCK, LANES),
        held(a, BLOCK, LANES),
        dma(n, 3, 2),
        *[dma(2, h)] * 12,
        dma(2, h), dma(2, n), dma(2, h), dma(2, h), dma(n), dma(n),
        dma(n), dma(n),
        *[dma(2 * b), dma(2 * b), dma(a), dma(a)] * 2,
        *[dma(g)] * 4,
        dma(STEPS, g), dma(STEPS, g),
        dma(g), dma(g), dma(2 * b), dma(2 * b), dma(a), dma(a),
    ]
    results = pl.pallas_call(
        functools.partial(kernel, n, g, width, scales),
        out_shape=tuple(pltpu.VMEM(item.shape, F32) for item in out_shape),
        in_specs=[pl.BlockSpec(memory_space=pltpu.SMEM), anywhere, vmem, anywhere, anywhere],
        out_specs=(vmem, vmem, vmem, vmem),
        scratch_shapes=scratch,
        compiler_params=pltpu.CompilerParams(
            collective_id=0, has_side_effects=True, vmem_limit_bytes=60 * 1000 * 1000
        ),
    )(live_rows, counts, left_basis, right_basis, right_start)
    return pl.pallas_call(
        settle_outputs,
        out_shape=out_shape,
        in_specs=[vmem] * 4,
        out_specs=(anywhere,) * 4,
        scratch_shapes=[dma(4)],
    )(*[pltpu.with_memory_space_constraint(item, pltpu.VMEM) for item in results])


def solution(mesh):
    in_specs = (
        P("cells", "genes"),
        P("cells"),
        P(None, "cells"),
        P(None, "genes"),
        P(None, "genes"),
    )
    out_specs = (P(None, "cells"), P(None, "genes"), P(), P())
    return jax.shard_map(body, mesh=mesh, in_specs=in_specs, out_specs=out_specs, check_vma=False)
```
